8 devices in a mesh: dp: 2 (over z, y), tp: 4 (over x, core).
Axes of the slice: x: 2, y: 2, z: 1, core: 2. Of those that a mesh axis runs over, the one named last changes fastest.
Arguments:
- ids: int32 [4, 256], P('dp'), parts along dimension 0
- emb: bfloat16 [32768, 2304], P('tp')
- g: bfloat16 [2304], replicated
- w: bfloat16 [2304, 4096], P(None, 'tp')
- du: bfloat16 [4, 256, 4096], P('dp', None, 'tp'), parts along dimension 0
- dres: bfloat16 [4, 256, 2304], P('dp', 'tp'), parts along dimension 0
Outputs:
- output 1: bfloat16 [4, 256, 4096], P('dp', None, 'tp'), parts along dimension 0
- output 2: bfloat16 [4, 256, 2304], P('dp', 'tp'), parts along dimension 0
- output 3: float32 [65536, 2304], P(('dp', 'tp')), parts along dimension 0
- output 4: float32 [2304, 8192], P(None, ('dp', 'tp')), parts along dimension 1
- output 5: float32 [4608], P('dp'), parts along dimension 0
There are 2 independent parts. The reference program is written for one: setup_inputs(seed, part) draws one part's arguments, and reference() takes and returns one part's arrays. A program takes and returns all parts, laid end to end along the dimension named above; an argument that names none is the same for every part.
All inputs are finite; a program needn't handle non-finite values.
Results may differ from the reference program's by a relative error of at most 0.001.
Values are sent between devices in bfloat16 or wider.
A program may use at most 1 GiB of HBM per device.

```python
import jax
import jax.numpy as jnp
from jax import lax

K = 2
T = 256
V = 32768
D = 2304
FC = 4096
GROUP = 4
EPS = 1e-6
NPOOL = K * T // 16
FCG = FC // GROUP


def setup_inputs(seed: int = 0, part: int = 0) -> dict:
    key = jax.random.key(seed)
    kp = jax.random.fold_in(key, part)
    ke, kg, kw = jax.random.split(key, 3)
    k1, k2, k3, k4, k5, k6 = jax.random.split(kp, 6)
    ka, kb, kc = jax.random.split(jax.random.fold_in(kp, 7), 3)
    a = jax.random.randint(ka, (K, T), 0, V)
    b = jax.random.randint(kb, (K, T), 0, V)
    coin = jax.random.bernoulli(kc, 0.4, (K, T))
    ids = jnp.where(coin, a, jnp.minimum(a, b)).astype(jnp.int32)
    emb = jax.random.normal(ke, (V, D), jnp.float32).astype(jnp.bfloat16)
    g = (1.0 + 0.5 * jax.random.normal(kg, (D,), jnp.float32)).astype(jnp.bfloat16)
    w = (jax.random.normal(kw, (D, FC), jnp.float32) * D ** -0.5).astype(jnp.bfloat16)
    du = (jax.random.normal(k5, (K, T, FC), jnp.float32) * (D / FC) ** 0.5).astype(jnp.bfloat16)
    dres = jax.random.normal(k6, (K, T, D), jnp.float32).astype(jnp.bfloat16)
    return {"ids": ids, "emb": emb, "g": g, "w": w, "du": du, "dres": dres}


def reference(ids, emb, g, w, du, dres):
    gf = g.astype(jnp.float32)

    def micro(carry, inp):
        de, dw, dg = carry
        idm, dum, drm = inp
        x = emb[idm]
        xf = x.astype(jnp.float32)
        rs = lax.rsqrt(jnp.mean(xf * xf, axis=-1, keepdims=True) + EPS)
        nh = xf * rs
        n = (nh * gf).astype(jnp.bfloat16)
        u = jnp.dot(n, w, preferred_element_type=jnp.float32).astype(jnp.bfloat16)
        dn = jnp.zeros((T, D), jnp.float32)
        for j in range(GROUP):
            pb = jnp.dot(dum[:, j * FCG:(j + 1) * FCG], w[:, j * FCG:(j + 1) * FCG].T, preferred_element_type=jnp.float32)
            dn = dn + pb.astype(jnp.bfloat16).astype(jnp.float32)
        gdn = gf * dn
        dxn = rs * (gdn - nh * jnp.mean(nh * gdn, axis=-1, keepdims=True))
        dx = (drm.astype(jnp.float32) + dxn).astype(jnp.bfloat16)
        de = de.at[idm].add(dx.astype(jnp.float32))
        dw = dw + jnp.dot(n.T, dum, preferred_element_type=jnp.float32)
        dg = dg + jnp.sum(dn * nh, axis=0)
        return (de, dw, dg), (u, x)

    init = (jnp.zeros((V, D), jnp.float32), jnp.zeros((D, FC), jnp.float32), jnp.zeros((D,), jnp.float32))
    (de, dw, dg), (u, x) = lax.scan(micro, init, (ids, du, dres))
    return u, x, de, dw, dg
```

```python
import functools

import jax
import jax.numpy as jnp
from jax import lax
from jax.experimental import pallas as pl
from jax.experimental.pallas import tpu as pltpu
from jax.sharding import PartitionSpec as P

EPS = 1e-6
F32 = jnp.float32
BF16 = jnp.bfloat16
ANY = pl.BlockSpec(memory_space=pl.ANY)
VMEM = pl.BlockSpec(memory_space=pltpu.VMEM)
SMEM = pl.BlockSpec(memory_space=pltpu.SMEM)
VLIM = 60 * 1024 * 1024


def call(body, name, outs, ins, out_specs, scratch, flops, nbytes, aliases=None):
    return pl.pallas_call(
        body,
        name=name,
        out_shape=outs,
        in_specs=ins,
        out_specs=out_specs,
        scratch_shapes=scratch,
        input_output_aliases=aliases or {},
        cost_estimate=pl.CostEstimate(flops=flops, bytes_accessed=nbytes, transcendentals=0),
        compiler_params=pltpu.CompilerParams(vmem_limit_bytes=VLIM),
    )


def pdn_kernel(du_ref, w_ref, *refs):
    outs, dup = refs[:4], refs[4]
    r = lax.axis_index("tp")
    k, tl = du_ref.shape[0], du_ref.shape[1] // 4
    d = w_ref.shape[0]
    n = k * tl
    for j in range(4):
        q = r ^ j
        for m in range(k):
            dup[pl.ds(j * n + m * tl, tl), :] = du_ref[m, pl.ds(q * tl, tl), :]
    blk = 256

    def step(i, c):
        wt = w_ref[pl.ds(pl.multiple_of(i * blk, blk), blk), :]
        p = lax.dot_general(dup[...], wt, (((1,), (1,)), ((), ())), preferred_element_type=F32)
        for j in range(4):
            outs[j][:, pl.ds(pl.multiple_of(i * blk, blk), blk)] = p[j * n:(j + 1) * n].astype(BF16)
        return c

    lax.fori_loop(0, d // blk, step, 0)


def gather_kernel(loc_ref, nxt_ref, emb_ref, keep_ref, send_ref, last_ref, dup_ref, cnt_ref, buf, tmp, xf, lst, sem):
    t = loc_ref.shape[0]
    vl = emb_ref.shape[0]
    h = keep_ref.shape[0]

    def scan(i, c):
        n, nl, nd = c
        v = loc_ref[i]
        own = jnp.logical_and(v >= 0, v < vl)
        lst[n] = i
        has = nxt_ref[i] < t
        last_ref[nl] = i
        dup_ref[nd] = i
        o = own.astype(jnp.int32)
        hi = has.astype(jnp.int32)
        return n + o, nl + o * (1 - hi), nd + o * hi

    n, nl, nd = lax.fori_loop(0, t, scan, (0, 0, 0), unroll=4)
    cnt_ref[0] = nl
    cnt_ref[1] = nd
    lst[n] = 0
    for a in range(1, 8):
        lst[n + a] = 0

    def start(i, c):
        v = loc_ref[lst[i]]
        b = pl.multiple_of((v >> 3) << 3, 8)
        pltpu.make_async_copy(emb_ref.at[pl.ds(b, 8), :], buf.at[i], sem).start()
        return c

    lax.fori_loop(0, n, start, 0)
    xf[...] = jnp.zeros_like(xf)

    def wait(i, c):
        pltpu.make_async_copy(emb_ref.at[pl.ds(0, 8), :], buf.at[0], sem).wait()
        return c

    lax.fori_loop(0, n, wait, 0)

    def take(g, c):
        for a in range(8):
            i = g * 8 + a
            tmp[a] = buf[i].astype(F32)
        for a in range(8):
            i = g * 8 + a
            dst = jnp.where(i < n, lst[i], t)
            sub = loc_ref[lst[i]] & 7
            xf[pl.ds(dst, 1), :] = tmp[a, pl.ds(sub, 1), :]
        return c

    lax.fori_loop(0, (n + 7) // 8, take, 0)
    keep_ref[...] = xf[0:h, :].astype(BF16)
    send_ref[...] = xf[h:2 * h, :].astype(BF16)


def zero_kernel(tok_ref, de_ref, z, sem):
    rows = z.shape[0]
    z[...] = jnp.zeros_like(z)
    n = de_ref.shape[0] // rows
    for i in range(n):
        pltpu.make_async_copy(z, de_ref.at[pl.ds(i * rows, rows), :], sem).start()
    for i in range(n):
        pltpu.make_async_copy(z, de_ref.at[pl.ds(0, rows), :], sem).wait()


def dx_kernel(x_ref, p0, p1, p2, p3, dres_ref, g_ref, de_ref, dx_ref, dg_ref):
    x = x_ref[...].astype(F32)
    g = g_ref[...].astype(F32)
    rs = lax.rsqrt(jnp.mean(x * x, axis=-1, keepdims=True) + EPS)
    nh = x * rs
    dn = (p0[...].astype(F32) + p1[...].astype(F32)) + (p2[...].astype(F32) + p3[...].astype(F32))
    gdn = g * dn
    mean = jnp.mean(nh * gdn, axis=-1, keepdims=True)
    dxn = rs * (gdn - nh * mean)
    dx_ref[...] = (dres_ref[...].astype(F32) + dxn).astype(BF16)
    dg_ref[...] = jnp.sum(dn * nh, axis=0, keepdims=True)


def proj_kernel(xm_ref, xo_ref, g_ref, w_ref, du_ref, u_ref, dw_ref, n_ref, du2, ub, dwb, usem, wsem):
    r = lax.axis_index("tp")
    k, t = du_ref.shape[0], du_ref.shape[1]
    tl = t // 4
    d, fc = w_ref.shape
    g = g_ref[...].astype(F32)
    par = r & 1
    for side, ref in ((0, xm_ref), (1, xo_ref)):
        for c in range(2):
            q = 2 * c + (par ^ side)
            for m in range(k):
                x = ref[(c * k + m) * tl:(c * k + m + 1) * tl, :].astype(F32)
                rs = lax.rsqrt(jnp.mean(x * x, axis=-1, keepdims=True) + EPS)
                n_ref[pl.ds(pl.multiple_of(m * t + q * tl, tl), tl), :] = ((x * rs) * g).astype(BF16)
    for m in range(k):
        du2[m * t:(m + 1) * t, :] = du_ref[m]
    ublk = 256
    ucopies = []
    for i in range(fc // ublk):
        ub[:, i * ublk:(i + 1) * ublk] = jnp.dot(
            n_ref[...], w_ref[:, i * ublk:(i + 1) * ublk], preferred_element_type=F32).astype(BF16)
    for m in range(k):
        c = pltpu.make_async_copy(ub.at[pl.ds(m * t, t), :], u_ref.at[m], usem)
        c.start()
        ucopies.append(c)
    blk = 256
    nb = d // blk
    copies = []
    for i in range(nb):
        dwb[i] = lax.dot_general(n_ref[:, i * blk:(i + 1) * blk], du2[...], (((0,), (0,)), ((), ())),
                                 preferred_element_type=F32)
        c = pltpu.make_async_copy(dwb.at[i], dw_ref.at[pl.ds(i * blk, blk), :], wsem)
        c.start()
        copies.append(c)
    for c in ucopies + copies:
        c.wait()


def scatter_kernel(loc_ref, nxt_ref, last_ref, dup_ref, cnt_ref, d0, d1, de_in, de_ref, xf, sem):
    h = d0.shape[0]
    xf[0:h, :] = d0[...].astype(F32)
    xf[h:2 * h, :] = d1[...].astype(F32)
    nl = cnt_ref[0]

    def add(i, c):
        a = dup_ref[i]
        b = nxt_ref[a]
        xf[pl.ds(b, 1), :] = xf[pl.ds(b, 1), :] + xf[pl.ds(a, 1), :]
        return c

    lax.fori_loop(0, cnt_ref[1], add, 0)

    def put(i, c):
        a = last_ref[i]
        pltpu.make_async_copy(xf.at[pl.ds(a, 1), :], de_ref.at[pl.ds(loc_ref[a], 1), :], sem).start()
        return c

    lax.fori_loop(0, nl, put, 0)

    def wait(i, c):
        pltpu.make_async_copy(xf.at[pl.ds(0, 1), :], de_ref.at[pl.ds(0, 1), :], sem).wait()
        return c

    lax.fori_loop(0, nl, wait, 0)


def solution(mesh):
    groups = mesh.shape["tp"]
    sib = [(i, i ^ 1) for i in range(groups)]
    cross = [(i, i ^ 2) for i in range(groups)]
    diag = [(i, i ^ 3) for i in range(groups)]

    def local(ids, emb, g, w, du, dres):
        r = lax.axis_index("tp")
        par = r & 1
        k, t = ids.shape
        vl, d = emb.shape
        fc = w.shape[1]
        tl = t // groups
        n = k * tl
        h = 2 * n
        g2 = g.reshape(1, d)
        S = jax.ShapeDtypeStruct
        o = ids.reshape(k, 2, 2, tl).transpose(2, 1, 0, 3).reshape(2, h)
        o = jnp.where(par == 0, o, o[::-1]).reshape(-1)
        loc = o - r * vl
        pos = jnp.arange(2 * h, dtype=jnp.int32)
        nxt = jnp.min(jnp.where((o[:, None] == o[None, :]) & (pos[None, :] > pos[:, None]), pos[None, :], 2 * h), axis=1)

        p0, p1, p2, p3 = call(
            pdn_kernel, "pdn", [S((n, d), BF16)] * 4, [VMEM, VMEM], [VMEM] * 4,
            [pltpu.VMEM((4 * n, fc), BF16)], 2 * 4 * n * fc * d, 2 * d * fc + 8 * n * (fc + d))(du, w)
        q2 = lax.ppermute(p2, "tp", cross)
        q3 = lax.ppermute(p3, "tp", diag)
        q1 = lax.ppermute(p1, "tp", sib)

        keep, send, last, dup, cnt = call(
            gather_kernel, "gather",
            [S((h, d), BF16), S((h, d), BF16), S((2 * h,), jnp.int32), S((2 * h,), jnp.int32), S((8,), jnp.int32)],
            [SMEM, SMEM, ANY], [VMEM, VMEM, SMEM, SMEM, SMEM],
            [pltpu.VMEM((2 * h, 8, d), BF16), pltpu.VMEM((8, 8, d), F32), pltpu.VMEM((2 * h + 8, d), F32),
             pltpu.SMEM((2 * h + 8,), jnp.int32), pltpu.SemaphoreType.DMA],
            8 * h * d * 8, 16 * h * d)(loc, nxt, emb)
        xh = keep + lax.ppermute(send, "tp", sib)
        xm = xh + lax.ppermute(xh, "tp", cross)
        xo = lax.ppermute(xm, "tp", sib)

        de = call(zero_kernel, "zero", S((vl, d), F32), [SMEM], ANY,
                  [pltpu.VMEM((256, d), F32), pltpu.SemaphoreType.DMA], 10_000_000_000, 4 * vl * d)(cnt)

        xown = lax.dynamic_slice_in_dim(xm, (r >> 1) * n, n, 0)
        dx, dgp = call(dx_kernel, "dx", [S((n, d), BF16), S((1, d), F32)], [VMEM] * 7 + [ANY], [VMEM] * 2, [],
                       30 * n * d, 16 * n * d)(xown, p0, q1, q2, q3, dres.reshape(n, d), g2, de)
        dxc = lax.ppermute(dx, "tp", cross)
        dxm = jnp.where(r < 2, jnp.concatenate([dx, dxc]), jnp.concatenate([dxc, dx]))
        dxo = lax.ppermute(dxm, "tp", sib)
        dgp = dgp + lax.ppermute(dgp, "tp", sib)
        dgp = dgp + lax.ppermute(dgp, "tp", cross)

        u, dw = call(
            proj_kernel, "proj", [S((k, t, fc), BF16), S((d, fc), F32)], [VMEM] * 5, [ANY, ANY],
            [pltpu.VMEM((k * t, d), BF16), pltpu.VMEM((k * t, fc), BF16), pltpu.VMEM((k * t, fc), BF16),
             pltpu.VMEM((d // 256, 256, fc), F32), pltpu.SemaphoreType.DMA, pltpu.SemaphoreType.DMA],
            4 * k * t * d * fc, 6 * d * fc)(xm, xo, g2, w, du)

        de = call(scatter_kernel, "scatter", S((vl, d), F32), [SMEM] * 5 + [VMEM, VMEM, ANY], ANY,
                  [pltpu.VMEM((2 * h, d), F32), pltpu.SemaphoreType.DMA], 8 * h * d, 8 * h * d,
                  {7: 0})(loc, nxt, last, dup, cnt, dxm, dxo, de)
        return u, xown.reshape(k, tl, d), de, dw, dgp.reshape(d)

    return jax.shard_map(
        local,
        mesh=mesh,
        in_specs=(P("dp", None), P("tp", None), P(None), P(None, "tp"), P("dp", None, "tp"), P("dp", "tp", None)),
        out_specs=(P("dp", None, "tp"), P("dp", "tp", None), P(("dp", "tp"), None), P(None, ("dp", "tp")), P("dp")),
        check_vma=False,
    )
```

```python
import functools

import jax
import jax.numpy as jnp
from jax import lax
from jax.experimental import pallas as pl
from jax.experimental.pallas import tpu as pltpu
from jax.sharding import PartitionSpec as P


EPS = 1e-6
F32 = jnp.float32
BF16 = jnp.bfloat16
ANY = pl.BlockSpec(memory_space=pl.ANY)
VMEM = pl.BlockSpec(memory_space=pltpu.VMEM)
SMEM = pl.BlockSpec(memory_space=pltpu.SMEM)
VLIM = 60 * 1024 * 1024


def call(body, outs, ins, out_specs, scratch, flops, nbytes, aliases=None):
    return pl.pallas_call(
        body,
        out_shape=outs,
        in_specs=ins,
        out_specs=out_specs,
        scratch_shapes=scratch,
        input_output_aliases=aliases or {},
        cost_estimate=pl.CostEstimate(flops=flops, bytes_accessed=nbytes, transcendentals=0),
        compiler_params=pltpu.CompilerParams(vmem_limit_bytes=VLIM),
    )


def pdn_kernel(js, zrows, tok_ref, du_ref, w_ref, *refs):
    nj = len(js)
    outs = refs[:nj]
    refs = refs[nj:]
    if zrows:
        de_ref, z, zsem = refs[0], refs[-2], refs[-1]
        refs = refs[1:-2]
        z[...] = jnp.zeros_like(z)
        zero_start(z, de_ref, 0, zrows, zsem)
    else:
        for a in range(8):
            refs[0][a] = 0
        refs = refs[1:]
    dub, dup, wb, dsem, wsem = refs
    r = lax.axis_index("tp")
    k, tl = dub.shape[0], dub.shape[1] // 4
    d = wb.shape[0]
    n = k * tl
    blk = 256
    nb = d // blk
    dc = pltpu.make_async_copy(du_ref, dub, dsem)
    dc.start()
    for i in range(nb):
        pltpu.make_async_copy(w_ref.at[pl.ds(i * blk, blk), :], wb.at[pl.ds(i * blk, blk), :], wsem.at[i]).start()
    dc.wait()
    for a, j in enumerate(js):
        q = r ^ j
        for m in range(k):
            dup[pl.ds(a * n + m * tl, tl), :] = dub[m, pl.ds(q * tl, tl), :]
    for i in range(nb):
        pltpu.make_async_copy(w_ref.at[pl.ds(i * blk, blk), :], wb.at[pl.ds(i * blk, blk), :], wsem.at[i]).wait()
        p = lax.dot_general(dup[...], wb[i * blk:(i + 1) * blk, :], (((1,), (1,)), ((), ())), preferred_element_type=F32)
        for a in range(nj):
            outs[a][:, i * blk:(i + 1) * blk] = p[a * n:(a + 1) * n].astype(BF16)
    if zrows:
        zero_wait(z, de_ref, zrows, zsem)


def zero_start(z, de_ref, lo, rows, sem):
    step = z.shape[0]
    for i in range(rows // step):
        pltpu.make_async_copy(z, de_ref.at[pl.ds(lo + i * step, step), :], sem).start()


def zero_wait(z, de_ref, rows, sem):
    step = z.shape[0]
    for _ in range(rows // step):
        pltpu.make_async_copy(z, de_ref.at[pl.ds(0, step), :], sem).wait()


def zero_kernel(tok_ref, de_in, de_ref, z, sem):
    z[...] = jnp.zeros_like(z)
    half = de_ref.shape[0] // 2
    zero_start(z, de_ref, half, half, sem)
    zero_wait(z, de_ref, half, sem)


def gather_kernel(loc_ref, nxt_ref, emb_ref, k0, s0, k1, s1, last_ref, dup_ref, cnt_ref, buf, tmp, xf, lst, sem):
    t = loc_ref.shape[0]
    vl = emb_ref.shape[0]
    h = k0.shape[0]

    def scan(i, c):
        n, nl, nd = c
        v = loc_ref[i]
        own = jnp.logical_and(v >= 0, v < vl)
        lst[n] = i
        has = nxt_ref[i] < t
        last_ref[nl] = i
        dup_ref[nd] = i
        o = own.astype(jnp.int32)
        hi = has.astype(jnp.int32)
        return n + o, nl + o * (1 - hi), nd + o * hi

    n, nl, nd = lax.fori_loop(0, t, scan, (0, 0, 0), unroll=4)
    cnt_ref[0] = nl
    cnt_ref[1] = nd

    def first(i, c):
        return c + (last_ref[i] < t // 2).astype(jnp.int32)

    cnt_ref[2] = lax.fori_loop(0, nl, first, 0)
    lst[n] = 0
    for a in range(1, 8):
        lst[n + a] = 0

    def start(i, c):
        v = loc_ref[lst[i]]
        b = pl.multiple_of((v >> 3) << 3, 8)
        pltpu.make_async_copy(emb_ref.at[pl.ds(b, 8), :], buf.at[i], sem).start()
        return c

    lax.fori_loop(0, n, start, 0)
    xf[...] = jnp.zeros_like(xf)

    def wait(i, c):
        pltpu.make_async_copy(emb_ref.at[pl.ds(0, 8), :], buf.at[0], sem).wait()
        return c

    lax.fori_loop(0, n, wait, 0)

    def take(g, c):
        for a in range(8):
            i = g * 8 + a
            tmp[a] = buf[i].astype(F32)
        for a in range(8):
            i = g * 8 + a
            dst = jnp.where(i < n, lst[i], t)
            sub = loc_ref[lst[i]] & 7
            xf[pl.ds(dst, 1), :] = tmp[a, pl.ds(sub, 1), :]
        return c

    lax.fori_loop(0, (n + 7) // 8, take, 0)
    for a, ref in enumerate((k0, s0, k1, s1)):
        ref[...] = xf[a * h:(a + 1) * h, :].astype(BF16)


def dx_kernel(m, xh_ref, z_ref, p0, p1, p2, p3, dres_ref, g_ref, tok_ref, *refs):
    if m == 1:
        xm0_ref, dg0_ref, xm_ref, dx_ref, dg_ref, x_ref = refs
    else:
        xm_ref, dx_ref, dg_ref = refs
    tl = dx_ref.shape[0]
    chip = lax.axis_index("tp") >> 1
    mine = pl.ds(pl.multiple_of(chip * tl, tl), tl)
    xm_ref[...] = xh_ref[...] + z_ref[...]
    if m == 1:
        x_ref[0] = xm0_ref[mine, :]
        x_ref[1] = xm_ref[mine, :]
    x = xm_ref[mine, :].astype(F32)
    g = g_ref[...].astype(F32)
    rs = lax.rsqrt(jnp.mean(x * x, axis=-1, keepdims=True) + EPS)
    nh = x * rs
    s = slice(m * tl, (m + 1) * tl)
    dn = (p0[s, :].astype(F32) + p1[s, :].astype(F32)) + (p2[s, :].astype(F32) + p3[s, :].astype(F32))
    gdn = g * dn
    mean = jnp.mean(nh * gdn, axis=-1, keepdims=True)
    dxn = rs * (gdn - nh * mean)
    dx_ref[...] = (dres_ref[m].astype(F32) + dxn).astype(BF16)
    dg = jnp.sum(dn * nh, axis=0, keepdims=True)
    dg_ref[...] = dg if m == 0 else dg + dg0_ref[...]


def fill_n(xm_ref, xo_ref, g_ref, n_ref, off):
    r = lax.axis_index("tp")
    par = r & 1
    tl = xm_ref.shape[0] // 2
    g = g_ref[...].astype(F32)
    for side, ref in ((0, xm_ref), (1, xo_ref)):
        for c in range(2):
            q = 2 * c + (par ^ side)
            x = ref[c * tl:(c + 1) * tl, :].astype(F32)
            rs = lax.rsqrt(jnp.mean(x * x, axis=-1, keepdims=True) + EPS)
            n_ref[pl.ds(pl.multiple_of(off + q * tl, tl), tl), :] = ((x * rs) * g).astype(BF16)


def umat(n_ref, w_ref, u_ref, lo):
    t = u_ref.shape[0]
    blk = 256
    for i in range(u_ref.shape[1] // blk):
        u_ref[:, i * blk:(i + 1) * blk] = jnp.dot(
            n_ref[lo:lo + t, :], w_ref[:, i * blk:(i + 1) * blk], preferred_element_type=F32).astype(BF16)


def u_kernel(xm_ref, xo_ref, g_ref, w_ref, tok_ref, u_ref, n_ref):
    fill_n(xm_ref, xo_ref, g_ref, n_ref, 0)
    umat(n_ref, w_ref, u_ref, 0)


def proj_kernel(n0_ref, xm_ref, xo_ref, g_ref, w_ref, du_ref, u0_ref, tok_ref, u_ref, dw_ref, n_ref, du2, ub, dwb, usem, wsem):
    k, t = du_ref.shape[0], du_ref.shape[1]
    d, _ = w_ref.shape
    copies = [pltpu.make_async_copy(u0_ref, u_ref.at[0], usem.at[0])]
    copies[0].start()
    n_ref[0:t, :] = n0_ref[...]
    fill_n(xm_ref, xo_ref, g_ref, n_ref, t)
    for m in range(k):
        du2[m * t:(m + 1) * t, :] = du_ref[m]
    umat(n_ref, w_ref, ub, t)
    c = pltpu.make_async_copy(ub, u_ref.at[1], usem.at[1])
    c.start()
    copies.append(c)
    blk = 256
    for i in range(d // blk):
        dwb[i] = lax.dot_general(n_ref[:, i * blk:(i + 1) * blk], du2[...], (((0,), (0,)), ((), ())),
                                 preferred_element_type=F32)
        c = pltpu.make_async_copy(dwb.at[i], dw_ref.at[pl.ds(i * blk, blk), :], wsem)
        c.start()
        copies.append(c)
    for c in copies:
        c.wait()


def scatter_kernel(m, loc_ref, nxt_ref, last_ref, dup_ref, cnt_ref, *refs):
    nd = 4 * (m + 1)
    ds, de_ref, xf, sem = refs[:nd], refs[-3], refs[-2], refs[-1]
    tl = ds[0].shape[0]
    chip = lax.axis_index("tp") >> 1
    for a, ref in enumerate(ds):
        c = chip if a % 2 == 0 else 1 - chip
        xf[pl.ds(pl.multiple_of((a // 2) * 2 * tl + c * tl, tl), tl), :] = ref[...].astype(F32)

    def add(i, c):
        a = dup_ref[i]
        b = nxt_ref[a]

        @pl.when(b < 4 * tl * (m + 1))
        def _():
            xf[pl.ds(b, 1), :] = xf[pl.ds(b, 1), :] + xf[pl.ds(a, 1), :]

        return c

    lax.fori_loop(0, cnt_ref[1], add, 0)

    def put(i, c):
        a = last_ref[i]
        pltpu.make_async_copy(xf.at[pl.ds(a, 1), :], de_ref.at[pl.ds(loc_ref[a], 1), :], sem).start()
        return c

    def wait(i, c):
        pltpu.make_async_copy(xf.at[pl.ds(0, 1), :], de_ref.at[pl.ds(0, 1), :], sem).wait()
        return c

    n0, n1 = (0, cnt_ref[2]) if m == 0 else (cnt_ref[2], cnt_ref[0])
    lax.fori_loop(n0, n1, put, 0)
    lax.fori_loop(n0, n1, wait, 0)


def solution(mesh):
    groups = mesh.shape["tp"]
    sib = [(i, i ^ 1) for i in range(groups)]
    cross = [(i, i ^ 2) for i in range(groups)]
    diag = [(i, i ^ 3) for i in range(groups)]

    def local(ids, emb, g, w, du, dres):
        r = lax.axis_index("tp")
        par = r & 1
        k, t = ids.shape
        vl, d = emb.shape
        fc = w.shape[1]
        tl = t // groups
        n = k * tl
        h = 2 * n
        g2 = g.reshape(1, d)
        S = jax.ShapeDtypeStruct
        D = pltpu.SemaphoreType.DMA

        def perm(v, p):
            return lax.ppermute(v, "tp", p)

        def pdn(js, zrows, tok):
            de = [S((vl, d), F32)] if zrows else [S((8,), jnp.int32)]
            return call(
                functools.partial(pdn_kernel, js, zrows), [S((n, d), BF16)] * len(js) + de,
                [ANY] * 3, [VMEM] * len(js) + [ANY if zrows else SMEM],
                [pltpu.VMEM((k, t, fc), BF16), pltpu.VMEM((len(js) * n, fc), BF16), pltpu.VMEM((d, fc), BF16), D, D((d // 256,))]
                + ([pltpu.VMEM((256, d), F32), D] if zrows else []),
                2 * len(js) * n * fc * d + (5_000_000_000 if zrows else 0), 2 * d * fc + 4 * n * (fc + d))(tok, du, w)

        p2, p3, zi = pdn((2, 3), 0, g2)
        q2 = perm(p2, cross)
        q3 = perm(p3, diag)

        o = ids.reshape(k, 2, 2, tl).transpose(0, 2, 1, 3) + zi[0]
        o = jnp.where(par == 0, o, o[:, ::-1]).reshape(-1)
        loc = o - r * vl
        pos = jnp.arange(2 * h, dtype=jnp.int32)
        nxt = jnp.min(jnp.where((o[:, None] == o[None, :]) & (pos[None, :] > pos[:, None]), pos[None, :], 2 * h), axis=1)
        k0, s0, k1, s1, last, dup, cnt = call(
            gather_kernel,
            [S((n, d), BF16)] * 4 + [S((2 * h,), jnp.int32), S((2 * h,), jnp.int32), S((8,), jnp.int32)],
            [SMEM, SMEM, ANY], [VMEM] * 4 + [SMEM] * 3,
            [pltpu.VMEM((2 * h, 8, d), BF16), pltpu.VMEM((8, 8, d), F32), pltpu.VMEM((2 * h + 8, d), F32),
             pltpu.SMEM((2 * h + 8,), jnp.int32), D],
            8 * h * d * 8, 16 * h * d)(loc, nxt, emb)
        y0 = perm(s0, sib)
        y1 = perm(s1, sib)
        p0, p1, de = pdn((0, 1), vl // 2, cnt)
        q1 = perm(p1, sib)
        xh0 = k0 + y0
        xh1 = k1 + y1
        z0 = perm(xh0, cross)
        z1 = perm(xh1, cross)
        de = call(zero_kernel, S((vl, d), F32), [ANY, ANY], ANY,
                  [pltpu.VMEM((256, d), F32), D], 5_000_000_000, 2 * vl * d, {1: 0})(xh1, de)

        def dxk(m, xh, z, tok, more):
            outs = [S((n, d), BF16), S((tl, d), BF16), S((1, d), F32)] + ([S((k, tl, d), BF16)] if m else [])
            return call(functools.partial(dx_kernel, m), outs, [VMEM] * 8 + [ANY] + [VMEM] * len(more),
                        [VMEM] * len(outs), [], 30 * n * d, 16 * n * d)(xh, z, p0, q1, q2, q3, dres, g2, tok, *more)

        xm0, dx0, dg0 = dxk(0, xh0, z0, de, ())
        c0 = perm(dx0, cross)
        xo0 = perm(xm0, sib)
        a0 = perm(dx0, sib)
        u0, n0 = call(u_kernel, [S((t, fc), BF16), S((t, d), BF16)], [VMEM] * 4 + [ANY], [VMEM] * 2, [],
                      2 * t * d * fc, 2 * d * fc)(xm0, xo0, g2, w, dg0)
        xm1, dx1, dg, x = dxk(1, xh1, z1, n0, (xm0, dg0))
        c1 = perm(dx1, cross)
        xo1 = perm(xm1, sib)
        a1 = perm(dx1, sib)
        b0 = perm(c0, sib)
        b1 = perm(c1, sib)
        dgs = dg + perm(dg, sib)
        dgs = dgs + perm(dgs, cross)

        u, dw = call(
            proj_kernel, [S((k, t, fc), BF16), S((d, fc), F32)], [VMEM] * 7 + [ANY], [ANY, ANY],
            [pltpu.VMEM((k * t, d), BF16), pltpu.VMEM((k * t, fc), BF16), pltpu.VMEM((t, fc), BF16),
             pltpu.VMEM((d // 256, 256, fc), F32), D((2,)), D],
            3 * k * t * d * fc, 6 * d * fc)(n0, xm1, xo1, g2, w, du, u0, dg)

        def scatter(m, parts, de, tok):
            return call(functools.partial(scatter_kernel, m), S((vl, d), F32),
                        [SMEM] * 5 + [VMEM] * len(parts) + [ANY, ANY], ANY,
                        [pltpu.VMEM((h * (m + 1), d), F32), D], 8 * h * d, 8 * h * d,
                        {6 + len(parts): 0})(loc, nxt, last, dup, cnt, *parts, tok, de)

        de = scatter(0, (dx0, c0, a0, b0), de, dw)
        de = scatter(1, (dx0, c0, a0, b0, dx1, c1, a1, b1), de, dw)
        return u, x, de, dw, dgs.reshape(d)

    return jax.shard_map(
        local,
        mesh=mesh,
        in_specs=(P("dp", None), P("tp", None), P(None), P(None, "tp"), P("dp", None, "tp"), P("dp", "tp", None)),
        out_specs=(P("dp", None, "tp"), P("dp", "tp", None), P(("dp", "tp"), None), P(None, ("dp", "tp")), P("dp")),
        check_vma=False,
    )
```

```python
import functools

import jax
import jax.numpy as jnp
from jax import lax
from jax.experimental import pallas as pl
from jax.experimental.pallas import tpu as pltpu
from jax.sharding import PartitionSpec as P


EPS = 1e-6
F32 = jnp.float32
BF16 = jnp.bfloat16
ANY = pl.BlockSpec(memory_space=pl.ANY)
VMEM = pl.BlockSpec(memory_space=pltpu.VMEM)
SMEM = pl.BlockSpec(memory_space=pltpu.SMEM)
VLIM = 60 * 1024 * 1024


def call(body, outs, ins, out_specs, scratch, flops, nbytes, aliases=None):
    return pl.pallas_call(
        body,
        out_shape=outs,
        in_specs=ins,
        out_specs=out_specs,
        scratch_shapes=scratch,
        input_output_aliases=aliases or {},
        cost_estimate=pl.CostEstimate(flops=flops, bytes_accessed=nbytes, transcendentals=0),
        compiler_params=pltpu.CompilerParams(vmem_limit_bytes=VLIM),
    )


def pdn_kernel(js, du_ref, w_ref, *refs):
    nj = len(js)
    outs = refs[:nj]
    flag_ref, dub, dup, wb, dsem, wsem = refs[nj:]
    for a in range(8):
        flag_ref[a] = 0
    r = lax.axis_index("tp")
    k, tl = dub.shape[0], dub.shape[1] // 4
    d = wb.shape[0]
    n = k * tl
    blk = 256
    nb = d // blk
    dc = pltpu.make_async_copy(du_ref, dub, dsem)
    dc.start()
    for i in range(nb):
        pltpu.make_async_copy(w_ref.at[pl.ds(i * blk, blk), :], wb.at[pl.ds(i * blk, blk), :], wsem.at[i]).start()
    dc.wait()
    for a, j in enumerate(js):
        q = r ^ j
        for m in range(k):
            dup[pl.ds(a * n + m * tl, tl), :] = dub[m, pl.ds(q * tl, tl), :]
    for i in range(nb):
        pltpu.make_async_copy(w_ref.at[pl.ds(i * blk, blk), :], wb.at[pl.ds(i * blk, blk), :], wsem.at[i]).wait()
        p = lax.dot_general(dup[...], wb[i * blk:(i + 1) * blk, :], (((1,), (1,)), ((), ())), preferred_element_type=F32)
        for a in range(nj):
            outs[a][:, i * blk:(i + 1) * blk] = p[a * n:(a + 1) * n].astype(BF16)


def zero_start(z, de_ref, lo, rows, sem):
    step = z.shape[0]
    for i in range(rows // step):
        pltpu.make_async_copy(z, de_ref.at[pl.ds(lo + i * step, step), :], sem).start()


def zero_wait(z, de_ref, rows, sem):
    step = z.shape[0]
    for _ in range(rows // step):
        pltpu.make_async_copy(z, de_ref.at[pl.ds(0, step), :], sem).wait()


def zero_kernel(tok_ref, de_in, de_ref, z, sem):
    z[...] = jnp.zeros_like(z)
    half = de_ref.shape[0] // 2
    zero_start(z, de_ref, half, half, sem)
    zero_wait(z, de_ref, half, sem)


def gather_kernel(loc_ref, nxt_ref, emb_ref, k0, s0, k1, s1, last_ref, dup_ref, cnt_ref, de_ref, buf, tmp, xf, lst, z, sem, zsem):
    t = loc_ref.shape[0]
    vl = emb_ref.shape[0]
    h = k0.shape[0]

    def scan(i, c):
        n, nl, nd = c
        v = loc_ref[i]
        own = jnp.logical_and(v >= 0, v < vl)
        lst[n] = i
        has = nxt_ref[i] < t
        last_ref[nl] = i
        dup_ref[nd] = i
        o = own.astype(jnp.int32)
        hi = has.astype(jnp.int32)
        return n + o, nl + o * (1 - hi), nd + o * hi

    n, nl, nd = lax.fori_loop(0, t, scan, (0, 0, 0), unroll=4)
    cnt_ref[0] = nl
    cnt_ref[1] = nd

    def first(i, c):
        return c + (last_ref[i] < t // 2).astype(jnp.int32)

    cnt_ref[2] = lax.fori_loop(0, nl, first, 0)
    lst[n] = 0
    for a in range(1, 8):
        lst[n + a] = 0

    def start(i, c):
        v = loc_ref[lst[i]]
        b = pl.multiple_of((v >> 3) << 3, 8)
        pltpu.make_async_copy(emb_ref.at[pl.ds(b, 8), :], buf.at[i], sem).start()
        return c

    lax.fori_loop(0, n, start, 0)
    z[...] = jnp.zeros_like(z)
    zero_start(z, de_ref, 0, vl // 2, zsem)
    xf[...] = jnp.zeros_like(xf)

    def wait(i, c):
        pltpu.make_async_copy(emb_ref.at[pl.ds(0, 8), :], buf.at[0], sem).wait()
        return c

    lax.fori_loop(0, n, wait, 0)

    def take(g, c):
        for a in range(8):
            i = g * 8 + a
            tmp[a] = buf[i].astype(F32)
        for a in range(8):
            i = g * 8 + a
            dst = jnp.where(i < n, lst[i], t)
            sub = loc_ref[lst[i]] & 7
            xf[pl.ds(dst, 1), :] = tmp[a, pl.ds(sub, 1), :]
        return c

    lax.fori_loop(0, (n + 7) // 8, take, 0)
    for a, ref in enumerate((k0, s0, k1, s1)):
        ref[...] = xf[a * h:(a + 1) * h, :].astype(BF16)
    zero_wait(z, de_ref, vl // 2, zsem)


def dx_kernel(m, xh_ref, z_ref, p0, p1, p2, p3, dres_ref, g_ref, tok_ref, *refs):
    if m == 1:
        xm0_ref, dg0_ref, xm_ref, dx_ref, dg_ref, x_ref = refs
    else:
        xm_ref, dx_ref, dg_ref = refs
    tl = dx_ref.shape[0]
    chip = lax.axis_index("tp") >> 1
    mine = pl.ds(pl.multiple_of(chip * tl, tl), tl)
    xm_ref[...] = xh_ref[...] + z_ref[...]
    if m == 1:
        x_ref[0] = xm0_ref[mine, :]
        x_ref[1] = xm_ref[mine, :]
    x = xm_ref[mine, :].astype(F32)
    g = g_ref[...].astype(F32)
    rs = lax.rsqrt(jnp.mean(x * x, axis=-1, keepdims=True) + EPS)
    nh = x * rs
    s = slice(m * tl, (m + 1) * tl)
    dn = (p0[s, :].astype(F32) + p1[s, :].astype(F32)) + (p2[s, :].astype(F32) + p3[s, :].astype(F32))
    gdn = g * dn
    mean = jnp.mean(nh * gdn, axis=-1, keepdims=True)
    dxn = rs * (gdn - nh * mean)
    dx_ref[...] = (dres_ref[m].astype(F32) + dxn).astype(BF16)
    dg = jnp.sum(dn * nh, axis=0, keepdims=True)
    dg_ref[...] = dg if m == 0 else dg + dg0_ref[...]


def fill_n(xm_ref, xo_ref, g_ref, n_ref, off):
    r = lax.axis_index("tp")
    par = r & 1
    tl = xm_ref.shape[0] // 2
    g = g_ref[...].astype(F32)
    for side, ref in ((0, xm_ref), (1, xo_ref)):
        for c in range(2):
            q = 2 * c + (par ^ side)
            x = ref[c * tl:(c + 1) * tl, :].astype(F32)
            rs = lax.rsqrt(jnp.mean(x * x, axis=-1, keepdims=True) + EPS)
            n_ref[pl.ds(pl.multiple_of(off + q * tl, tl), tl), :] = ((x * rs) * g).astype(BF16)


def umat(n_ref, w_ref, u_ref, lo):
    t = u_ref.shape[0]
    blk = 256
    for i in range(u_ref.shape[1] // blk):
        u_ref[:, i * blk:(i + 1) * blk] = jnp.dot(
            n_ref[lo:lo + t, :], w_ref[:, i * blk:(i + 1) * blk], preferred_element_type=F32).astype(BF16)


def u_kernel(xm_ref, xo_ref, g_ref, w_ref, tok_ref, u_ref, n_ref):
    fill_n(xm_ref, xo_ref, g_ref, n_ref, 0)
    umat(n_ref, w_ref, u_ref, 0)


def proj_kernel(n0_ref, xm_ref, xo_ref, g_ref, w_ref, du_ref, u0_ref, tok_ref, u_ref, dw_ref, n_ref, du2, ub, dwb, usem, wsem):
    k, t = du_ref.shape[0], du_ref.shape[1]
    d, _ = w_ref.shape
    copies = [pltpu.make_async_copy(u0_ref, u_ref.at[0], usem.at[0])]
    copies[0].start()
    n_ref[0:t, :] = n0_ref[...]
    fill_n(xm_ref, xo_ref, g_ref, n_ref, t)
    for m in range(k):
        du2[m * t:(m + 1) * t, :] = du_ref[m]
    umat(n_ref, w_ref, ub, t)
    c = pltpu.make_async_copy(ub, u_ref.at[1], usem.at[1])
    c.start()
    copies.append(c)
    blk = 256
    for i in range(d // blk):
        dwb[i] = lax.dot_general(n_ref[:, i * blk:(i + 1) * blk], du2[...], (((0,), (0,)), ((), ())),
                                 preferred_element_type=F32)
        c = pltpu.make_async_copy(dwb.at[i], dw_ref.at[pl.ds(i * blk, blk), :], wsem)
        c.start()
        copies.append(c)
    for c in copies:
        c.wait()


def scatter_kernel(m, loc_ref, nxt_ref, last_ref, dup_ref, cnt_ref, *refs):
    nd = 4 * (m + 1)
    ds, de_ref, xf, sem = refs[:nd], refs[-3], refs[-2], refs[-1]
    tl = ds[0].shape[0]
    chip = lax.axis_index("tp") >> 1
    for a, ref in enumerate(ds):
        c = chip if a % 2 == 0 else 1 - chip
        xf[pl.ds(pl.multiple_of((a // 2) * 2 * tl + c * tl, tl), tl), :] = ref[...].astype(F32)

    def add(i, c):
        a = dup_ref[i]
        b = nxt_ref[a]

        @pl.when(b < 4 * tl * (m + 1))
        def _():
            xf[pl.ds(b, 1), :] = xf[pl.ds(b, 1), :] + xf[pl.ds(a, 1), :]

        return c

    lax.fori_loop(0, cnt_ref[1], add, 0)

    def put(i, c):
        a = last_ref[i]
        pltpu.make_async_copy(xf.at[pl.ds(a, 1), :], de_ref.at[pl.ds(loc_ref[a], 1), :], sem).start()
        return c

    def wait(i, c):
        pltpu.make_async_copy(xf.at[pl.ds(0, 1), :], de_ref.at[pl.ds(0, 1), :], sem).wait()
        return c

    n0, n1 = (0, cnt_ref[2]) if m == 0 else (cnt_ref[2], cnt_ref[0])
    lax.fori_loop(n0, n1, put, 0)
    lax.fori_loop(n0, n1, wait, 0)


def solution(mesh):
    groups = mesh.shape["tp"]
    sib = [(i, i ^ 1) for i in range(groups)]
    cross = [(i, i ^ 2) for i in range(groups)]
    diag = [(i, i ^ 3) for i in range(groups)]

    def local(ids, emb, g, w, du, dres):
        r = lax.axis_index("tp")
        par = r & 1
        k, t = ids.shape
        vl, d = emb.shape
        fc = w.shape[1]
        tl = t // groups
        n = k * tl
        h = 2 * n
        g2 = g.reshape(1, d)
        S = jax.ShapeDtypeStruct
        D = pltpu.SemaphoreType.DMA

        def perm(v, p):
            return lax.ppermute(v, "tp", p)

        p2, p3, p1, p0, zi = call(
            functools.partial(pdn_kernel, (2, 3, 1, 0)), [S((n, d), BF16)] * 4 + [S((8,), jnp.int32)],
            [ANY] * 2, [VMEM] * 4 + [SMEM],
            [pltpu.VMEM((k, t, fc), BF16), pltpu.VMEM((4 * n, fc), BF16), pltpu.VMEM((d, fc), BF16), D, D((d // 256,))],
            8 * n * fc * d, 2 * d * fc + 8 * n * (fc + d))(du, w)
        q2 = perm(p2, cross)
        q3 = perm(p3, diag)
        q1 = perm(p1, sib)

        o = ids.reshape(k, 2, 2, tl).transpose(0, 2, 1, 3) + zi[0]
        o = jnp.where(par == 0, o, o[:, ::-1]).reshape(-1)
        loc = o - r * vl
        pos = jnp.arange(2 * h, dtype=jnp.int32)
        nxt = jnp.min(jnp.where((o[:, None] == o[None, :]) & (pos[None, :] > pos[:, None]), pos[None, :], 2 * h), axis=1)
        k0, s0, k1, s1, last, dup, cnt, de = call(
            gather_kernel,
            [S((n, d), BF16)] * 4 + [S((2 * h,), jnp.int32), S((2 * h,), jnp.int32), S((8,), jnp.int32), S((vl, d), F32)],
            [SMEM, SMEM, ANY], [VMEM] * 4 + [SMEM] * 3 + [ANY],
            [pltpu.VMEM((2 * h, 8, d), BF16), pltpu.VMEM((8, 8, d), F32), pltpu.VMEM((2 * h + 8, d), F32),
             pltpu.SMEM((2 * h + 8,), jnp.int32), pltpu.VMEM((256, d), F32), D, D],
            5_000_000_000, 16 * h * d)(loc, nxt, emb)
        y0 = perm(s0, sib)
        y1 = perm(s1, sib)
        xh0 = k0 + y0
        xh1 = k1 + y1
        z0 = perm(xh0, cross)
        z1 = perm(xh1, cross)
        de = call(zero_kernel, S((vl, d), F32), [ANY, ANY], ANY,
                  [pltpu.VMEM((256, d), F32), D], 5_000_000_000, 2 * vl * d, {1: 0})(xh1, de)

        def dxk(m, xh, z, tok, more):
            outs = [S((n, d), BF16), S((tl, d), BF16), S((1, d), F32)] + ([S((k, tl, d), BF16)] if m else [])
            return call(functools.partial(dx_kernel, m), outs, [VMEM] * 8 + [ANY] + [VMEM] * len(more),
                        [VMEM] * len(outs), [], 30 * n * d, 16 * n * d)(xh, z, p0, q1, q2, q3, dres, g2, tok, *more)

        xm0, dx0, dg0 = dxk(0, xh0, z0, de, ())
        c0 = perm(dx0, cross)
        xo0 = perm(xm0, sib)
        a0 = perm(dx0, sib)
        u0, n0 = call(u_kernel, [S((t, fc), BF16), S((t, d), BF16)], [VMEM] * 4 + [ANY], [VMEM] * 2, [],
                      2 * t * d * fc, 2 * d * fc)(xm0, xo0, g2, w, dg0)
        xm1, dx1, dg, x = dxk(1, xh1, z1, n0, (xm0, dg0))
        c1 = perm(dx1, cross)
        xo1 = perm(xm1, sib)
        a1 = perm(dx1, sib)
        b0 = perm(c0, sib)
        b1 = perm(c1, sib)
        dgs = dg + perm(dg, sib)
        dgs = dgs + perm(dgs, cross)

        u, dw = call(
            proj_kernel, [S((k, t, fc), BF16), S((d, fc), F32)], [VMEM] * 7 + [ANY], [ANY, ANY],
            [pltpu.VMEM((k * t, d), BF16), pltpu.VMEM((k * t, fc), BF16), pltpu.VMEM((t, fc), BF16),
             pltpu.VMEM((d // 256, 256, fc), F32), D((2,)), D],
            3 * k * t * d * fc, 6 * d * fc)(n0, xm1, xo1, g2, w, du, u0, dg)

        def scatter(m, parts, de, tok):
            return call(functools.partial(scatter_kernel, m), S((vl, d), F32),
                        [SMEM] * 5 + [VMEM] * len(parts) + [ANY, ANY], ANY,
                        [pltpu.VMEM((h * (m + 1), d), F32), D], 8 * h * d, 8 * h * d,
                        {6 + len(parts): 0})(loc, nxt, last, dup, cnt, *parts, tok, de)

        de = scatter(0, (dx0, c0, a0, b0), de, dw)
        de = scatter(1, (dx0, c0, a0, b0, dx1, c1, a1, b1), de, dw)
        return u, x, de, dw, dgs.reshape(d)

    return jax.shard_map(
        local,
        mesh=mesh,
        in_specs=(P("dp", None), P("tp", None), P(None), P(None, "tp"), P("dp", None, "tp"), P("dp", "tp", None)),
        out_specs=(P("dp", None, "tp"), P("dp", "tp", None), P(("dp", "tp"), None), P(None, ("dp", "tp")), P("dp")),
        check_vma=False,
    )
```

```python
import functools

import jax
import jax.numpy as jnp
from jax import lax
from jax.experimental import pallas as pl
from jax.experimental.pallas import tpu as pltpu
from jax.sharding import PartitionSpec as P


EPS = 1e-6
F32 = jnp.float32
BF16 = jnp.bfloat16
HBM = pl.BlockSpec(memory_space=pltpu.HBM)
VMEM = pl.BlockSpec(memory_space=pltpu.VMEM)
SMEM = pl.BlockSpec(memory_space=pltpu.SMEM)


def call(body, mib, outs, ins, out_specs, scratch, flops, nbytes, aliases=None):
    return pl.pallas_call(
        body,
        out_shape=outs,
        in_specs=ins,
        out_specs=out_specs,
        scratch_shapes=scratch,
        input_output_aliases=aliases or {},
        cost_estimate=pl.CostEstimate(flops=flops, bytes_accessed=nbytes, transcendentals=0),
        compiler_params=pltpu.CompilerParams(vmem_limit_bytes=mib << 20),
    )


def pdn_kernel(lo, first, *refs):
    if first:
        du_ref, w_ref, *outs, dup_ref, dub, wb, dsem, wsem = refs
    else:
        dup_ref, w_ref, *outs, wb, wsem = refs
    width = outs[0].shape[1]
    n = outs[0].shape[0]
    blk = 256
    nb = width // blk
    for i in range(nb):
        pltpu.make_async_copy(w_ref.at[pl.ds(lo + i * blk, blk), :], wb.at[pl.ds(i * blk, blk), :], wsem.at[i]).start()
    if first:
        k, tl = dub.shape[0], dub.shape[1] // 4
        dc = pltpu.make_async_copy(du_ref, dub, dsem)
        dc.start()
        r = lax.axis_index("tp")
        dc.wait()
        for a, j in enumerate((2, 3, 1, 0)):
            q = r ^ j
            for m in range(k):
                dup_ref[pl.ds(a * n + m * tl, tl), :] = dub[m, pl.ds(pl.multiple_of(q * tl, tl), tl), :]
    for i in range(nb):
        pltpu.make_async_copy(w_ref.at[pl.ds(lo + i * blk, blk), :], wb.at[pl.ds(i * blk, blk), :], wsem.at[i]).wait()
        p = lax.dot_general(dup_ref[...], wb[i * blk:(i + 1) * blk, :], (((1,), (1,)), ((), ())), preferred_element_type=F32)
        for a in range(4):
            outs[a][:, i * blk:(i + 1) * blk] = p[a * n:(a + 1) * n].astype(BF16)


def zero_start(z, de_ref, lo, rows, sem):
    step = z.shape[0]
    for i in range(rows // step):
        pltpu.make_async_copy(z, de_ref.at[pl.ds(lo + i * step, step), :], sem).start()


def zero_wait(z, de_ref, rows, sem):
    step = z.shape[0]
    for _ in range(rows // step):
        pltpu.make_async_copy(z, de_ref.at[pl.ds(0, step), :], sem).wait()


def zero_kernel(tok_ref, de_in, de_ref, z, sem):
    z[...] = jnp.zeros_like(z)
    half = de_ref.shape[0] // 2
    zero_start(z, de_ref, half, half, sem)
    zero_wait(z, de_ref, half, sem)


def gather_kernel(tok_ref, ids_ref, emb_ref, k0, s0, k1, s1, last_ref, dup_ref, cnt_ref, de_ref,
                  buf, tmp, xf, z, lpos, lrow, lnxt, tab, sem, zsem):
    k, t = ids_ref.shape
    vl = emb_ref.shape[0]
    h = k0.shape[0]
    tl = t // 4
    r = lax.axis_index("tp")
    z[...] = jnp.zeros_like(z)
    zero_start(z, de_ref, 0, vl // 2, zsem)
    n = 0
    for m in range(k):
        def scan(i, n):
            v = ids_ref[m, i] - r * vl
            q = i // tl
            lpos[n] = m * t + ((q ^ r) & 1) * h + (q >> 1) * tl + (i & (tl - 1))
            lrow[n] = v
            return n + jnp.logical_and(v >= 0, v < vl).astype(jnp.int32)

        n = lax.fori_loop(0, t, scan, n, unroll=8)

    def start(i, c):
        v = lrow[i]
        b = pl.multiple_of((v >> 3) << 3, 8)
        pltpu.make_async_copy(emb_ref.at[pl.ds(b, 8), :], buf.at[i], sem).start()
        lnxt[i] = -1
        return c

    lax.fori_loop(0, n, start, 0)
    for a in range(8):
        lpos[n + a] = k * t
        lrow[n + a] = 0
    xf[...] = jnp.zeros_like(xf)

    def link(i, c):
        v = lrow[i]
        p = tab[v]
        ok = jnp.logical_and(p >= 0, p < i)
        p = jnp.where(ok, p, 0)
        ok = jnp.logical_and(ok, lrow[p] == v)
        lnxt[jnp.where(ok, p, k * t)] = i
        tab[v] = i
        return c

    lax.fori_loop(0, n, link, 0)

    def lists(i, c):
        nl, nd, n0 = c
        x = lnxt[i]
        end = (x < 0).astype(jnp.int32)
        last_ref[0, nl] = lpos[i]
        last_ref[1, nl] = lrow[i]
        dup_ref[0, nd] = lpos[i]
        dup_ref[1, nd] = lpos[jnp.maximum(x, 0)]
        return nl + end, nd + 1 - end, n0 + end * (lpos[i] < t).astype(jnp.int32)

    nl, nd, n0 = lax.fori_loop(0, n, lists, (0, 0, 0))
    cnt_ref[0] = nl
    cnt_ref[1] = nd
    cnt_ref[2] = n0

    def wait(i, c):
        pltpu.make_async_copy(emb_ref.at[pl.ds(0, 8), :], buf.at[0], sem).wait()
        return c

    lax.fori_loop(0, n, wait, 0)

    def take(g, c):
        for a in range(8):
            tmp[a] = buf[g * 8 + a].astype(F32)
        for a in range(8):
            i = g * 8 + a
            xf[pl.ds(lpos[i], 1), :] = tmp[a, pl.ds(lrow[i] & 7, 1), :]
        return c

    lax.fori_loop(0, (n + 7) // 8, take, 0)
    for a, ref in enumerate((k0, s0, k1, s1)):
        ref[...] = xf[a * h:(a + 1) * h, :].astype(BF16)
    zero_wait(z, de_ref, vl // 2, zsem)


def dx_kernel(m, xh_ref, z_ref, p0, p1, p2, p3, r0, r1, r2, r3, dres_ref, g_ref, tok_ref, *refs):
    if m == 1:
        xm0_ref, dg0_ref, xm_ref, dx_ref, dg_ref, x_ref = refs
    else:
        xm_ref, dx_ref, dg_ref = refs
    tl = dx_ref.shape[0]
    chip = lax.axis_index("tp") >> 1
    mine = pl.ds(pl.multiple_of(chip * tl, tl), tl)
    xm_ref[...] = xh_ref[...] + z_ref[...]
    if m == 1:
        x_ref[0] = xm0_ref[mine, :]
        x_ref[1] = xm_ref[mine, :]
    x = xm_ref[mine, :].astype(F32)
    g = g_ref[...].astype(F32)
    rs = lax.rsqrt(jnp.mean(x * x, axis=-1, keepdims=True) + EPS)
    nh = x * rs
    s = slice(m * tl, (m + 1) * tl)
    dn = jnp.concatenate([
        (a[s, :].astype(F32) + b[s, :].astype(F32)) + (c[s, :].astype(F32) + e[s, :].astype(F32))
        for a, b, c, e in ((p0, p1, p2, p3), (r0, r1, r2, r3))], axis=1)
    gdn = g * dn
    mean = jnp.mean(nh * gdn, axis=-1, keepdims=True)
    dxn = rs * (gdn - nh * mean)
    dx_ref[...] = (dres_ref[m].astype(F32) + dxn).astype(BF16)
    dg = jnp.sum(dn * nh, axis=0, keepdims=True)
    dg_ref[...] = dg if m == 0 else dg + dg0_ref[...]


def fill_n(xm_ref, xo_ref, g_ref, n_ref, off):
    r = lax.axis_index("tp")
    par = r & 1
    tl = xm_ref.shape[0] // 2
    g = g_ref[...].astype(F32)
    for side, ref in ((0, xm_ref), (1, xo_ref)):
        for c in range(2):
            q = 2 * c + (par ^ side)
            x = ref[c * tl:(c + 1) * tl, :].astype(F32)
            rs = lax.rsqrt(jnp.mean(x * x, axis=-1, keepdims=True) + EPS)
            n_ref[pl.ds(pl.multiple_of(off + q * tl, tl), tl), :] = ((x * rs) * g).astype(BF16)


def umat(n_ref, w_ref, u_ref, lo):
    t = u_ref.shape[0]
    blk = 256
    for i in range(u_ref.shape[1] // blk):
        u_ref[:, i * blk:(i + 1) * blk] = jnp.dot(
            n_ref[lo:lo + t, :], w_ref[:, i * blk:(i + 1) * blk], preferred_element_type=F32).astype(BF16)


def u_kernel(xm_ref, xo_ref, g_ref, w_ref, tok_ref, u_ref, n_ref, flag_ref, ub, usem):
    flag_ref[0] = 0
    fill_n(xm_ref, xo_ref, g_ref, n_ref, 0)
    umat(n_ref, w_ref, ub, 0)
    c = pltpu.make_async_copy(ub, u_ref.at[0], usem)
    c.start()
    c.wait()


def proj_kernel(n0_ref, xm_ref, xo_ref, g_ref, w_ref, du_ref, u_in, tok_ref, u_ref, dw_ref, flag_ref, n_ref, du2, ub, dwb, usem, wsem):
    flag_ref[0] = 0
    k, t = du_ref.shape[0], du_ref.shape[1]
    d, _ = w_ref.shape
    copies = []
    n_ref[0:t, :] = n0_ref[...]
    fill_n(xm_ref, xo_ref, g_ref, n_ref, t)
    for m in range(k):
        du2[m * t:(m + 1) * t, :] = du_ref[m]
    umat(n_ref, w_ref, ub, t)
    c = pltpu.make_async_copy(ub, u_ref.at[1], usem)
    c.start()
    copies.append(c)
    blk = 256
    for i in range(d // blk):
        dwb[i] = lax.dot_general(n_ref[:, i * blk:(i + 1) * blk], du2[...], (((0,), (0,)), ((), ())),
                                 preferred_element_type=F32)
        c = pltpu.make_async_copy(dwb.at[i], dw_ref.at[pl.ds(i * blk, blk), :], wsem)
        c.start()
        copies.append(c)
    for c in copies:
        c.wait()


def scatter_kernel(m, last_ref, dup_ref, cnt_ref, *refs):
    nd = 4 * (m + 1)
    ds, de_ref, xf, sem = refs[:nd], refs[-3], refs[-2], refs[-1]
    tl = ds[0].shape[0]
    chip = lax.axis_index("tp") >> 1
    for a, ref in enumerate(ds):
        c = chip if a % 2 == 0 else 1 - chip
        xf[pl.ds(pl.multiple_of((a // 2) * 2 * tl + c * tl, tl), tl), :] = ref[...].astype(F32)

    def add(i, c):
        a = dup_ref[0, i]
        b = dup_ref[1, i]

        @pl.when(b < 4 * tl * (m + 1))
        def _():
            xf[pl.ds(b, 1), :] = xf[pl.ds(b, 1), :] + xf[pl.ds(a, 1), :]

        return c

    lax.fori_loop(0, cnt_ref[1], add, 0)

    def put(i, c):
        pltpu.make_async_copy(xf.at[pl.ds(last_ref[0, i], 1), :], de_ref.at[pl.ds(last_ref[1, i], 1), :], sem).start()
        return c

    def wait(i, c):
        pltpu.make_async_copy(xf.at[pl.ds(0, 1), :], de_ref.at[pl.ds(0, 1), :], sem).wait()
        return c

    n0, n1 = (0, cnt_ref[2]) if m == 0 else (cnt_ref[2], cnt_ref[0])
    lax.fori_loop(n0, n1, put, 0)
    lax.fori_loop(n0, n1, wait, 0)


def solution(mesh):
    groups = mesh.shape["tp"]
    sib = [(i, i ^ 1) for i in range(groups)]
    cross = [(i, i ^ 2) for i in range(groups)]
    diag = [(i, i ^ 3) for i in range(groups)]

    def local(ids, emb, g, w, du, dres):
        k, t = ids.shape
        vl, d = emb.shape
        fc = w.shape[1]
        tl = t // groups
        n = k * tl
        h = 2 * n
        g2 = g.reshape(1, d)
        S = jax.ShapeDtypeStruct
        D = pltpu.SemaphoreType.DMA

        def perm(v, p):
            return lax.ppermute(v, "tp", p)

        d1 = 5 * 256
        d2 = d - d1
        p2, p3, p1, p0, dup4 = call(
            functools.partial(pdn_kernel, 0, True), 60, [S((n, d1), BF16)] * 4 + [S((4 * n, fc), BF16)],
            [HBM] * 2, [VMEM] * 5, [pltpu.VMEM((k, t, fc), BF16), pltpu.VMEM((d1, fc), BF16), D, D((d1 // 256,))],
            8 * n * fc * d1, 2 * d1 * fc + 8 * n * (fc + d1))(du, w)
        r2, r3, r1, r0 = call(
            functools.partial(pdn_kernel, d1, False), 60, [S((n, d2), BF16)] * 4,
            [VMEM, HBM], [VMEM] * 4, [pltpu.VMEM((d2, fc), BF16), D((d2 // 256,))],
            8 * n * fc * d2, 2 * d2 * fc + 8 * n * (fc + d2))(dup4, w)
        q2 = perm(p2, cross)
        q3 = perm(p3, diag)
        v2 = perm(r2, cross)
        v3 = perm(r3, diag)
        q1 = perm(p1, sib)
        v1 = perm(r1, sib)

        k0, s0, k1, s1, last, dup, cnt, de = call(
            gather_kernel, 60,
            [S((n, d), BF16)] * 4 + [S((2, 2 * h + 8), jnp.int32)] * 2 + [S((8,), jnp.int32), S((vl, d), F32)],
            [HBM, SMEM, HBM], [VMEM] * 4 + [SMEM] * 3 + [HBM],
            [pltpu.VMEM((2 * h, 8, d), BF16), pltpu.VMEM((8, 8, d), F32), pltpu.VMEM((2 * h + 8, d), F32), pltpu.VMEM((256, d), F32)]
            + [pltpu.SMEM((2 * h + 8,), jnp.int32)] * 3 + [pltpu.SMEM((vl,), jnp.int32), D, D],
            5_000_000_000, 16 * h * d)(r2, ids, emb)
        y0 = perm(s0, sib)
        y1 = perm(s1, sib)
        xh0 = k0 + y0
        xh1 = k1 + y1
        z0 = perm(xh0, cross)
        z1 = perm(xh1, cross)
        de = call(zero_kernel, 8, S((vl, d), F32), [HBM, HBM], HBM,
                  [pltpu.VMEM((256, d), F32), D], 5_000_000_000, 2 * vl * d, {1: 0})(xh1, de)

        def dxk(m, xh, z, tok, more):
            outs = [S((n, d), BF16), S((tl, d), BF16), S((1, d), F32)] + ([S((k, tl, d), BF16)] if m else [])
            return call(functools.partial(dx_kernel, m), 16, outs, [VMEM] * 12 + [SMEM if m else HBM] + [VMEM] * len(more),
                        [VMEM] * len(outs), [], 30 * n * d, 16 * n * d)(xh, z, p0, q1, q2, q3, r0, v1, v2, v3, dres, g2, tok, *more)

        xm0, dx0, dg0 = dxk(0, xh0, z0, de, ())
        c0 = perm(dx0, cross)
        xo0 = perm(xm0, sib)
        a0 = perm(dx0, sib)
        u, n0, done0 = call(
            u_kernel, 24, [S((k, t, fc), BF16), S((t, d), BF16), S((8,), jnp.int32)], [VMEM] * 5, [HBM, VMEM, SMEM],
            [pltpu.VMEM((t, fc), BF16), D], 2 * t * d * fc, 2 * d * fc)(xm0, xo0, g2, w, dg0)
        xm1, dx1, dg, x = dxk(1, xh1, z1, done0, (xm0, dg0))
        c1 = perm(dx1, cross)
        xo1 = perm(xm1, sib)
        a1 = perm(dx1, sib)
        b0 = perm(c0, sib)
        b1 = perm(c1, sib)
        dgs = dg + perm(dg, sib)
        dgs = dgs + perm(dgs, cross)

        u, dw, done1 = call(
            proj_kernel, 36, [S((k, t, fc), BF16), S((d, fc), F32), S((8,), jnp.int32)],
            [VMEM] * 6 + [HBM, VMEM], [HBM, HBM, SMEM],
            [pltpu.VMEM((k * t, d), BF16), pltpu.VMEM((k * t, fc), BF16), pltpu.VMEM((t, fc), BF16),
             pltpu.VMEM((d // 256, 256, fc), F32), D, D],
            3 * k * t * d * fc, 6 * d * fc, {6: 0})(n0, xm1, xo1, g2, w, du, u, dg)

        def scatter(m, parts, de, tok):
            return call(functools.partial(scatter_kernel, m), 16, S((vl, d), F32),
                        [SMEM] * 3 + [VMEM] * len(parts) + [SMEM, HBM], HBM,
                        [pltpu.VMEM((h * (m + 1), d), F32), D], 8 * h * d, 8 * h * d,
                        {4 + len(parts): 0})(last, dup, cnt, *parts, tok, de)

        de = scatter(0, (dx0, c0, a0, b0), de, done1)
        de = scatter(1, (dx0, c0, a0, b0, dx1, c1, a1, b1), de, done1)
        return u, x, de, dw, dgs.reshape(d)

    return jax.shard_map(
        local,
        mesh=mesh,
        in_specs=(P("dp", None), P("tp", None), P(None), P(None, "tp"), P("dp", None, "tp"), P("dp", "tp", None)),
        out_specs=(P("dp", None, "tp"), P("dp", "tp", None), P(("dp", "tp"), None), P(None, ("dp", "tp")), P("dp")),
        check_vma=False,
    )
```

```python
import functools

import jax
import jax.numpy as jnp
from jax import lax
from jax.experimental import pallas as pl
from jax.experimental.pallas import tpu as pltpu
from jax.sharding import PartitionSpec as P


EPS = 1e-6
F32 = jnp.float32
BF16 = jnp.bfloat16
HBM = pl.BlockSpec(memory_space=pltpu.HBM)
VMEM = pl.BlockSpec(memory_space=pltpu.VMEM)
SMEM = pl.BlockSpec(memory_space=pltpu.SMEM)


def call(body, mib, outs, ins, out_specs, scratch, flops, nbytes, aliases=None):
    return pl.pallas_call(
        body,
        out_shape=outs,
        in_specs=ins,
        out_specs=out_specs,
        scratch_shapes=scratch,
        input_output_aliases=aliases or {},
        cost_estimate=pl.CostEstimate(flops=flops, bytes_accessed=nbytes, transcendentals=0),
        compiler_params=pltpu.CompilerParams(vmem_limit_bytes=mib << 20),
    )


def pdn_kernel(lo, first, *refs):
    if first:
        du_ref, w_ref, *outs, dup_ref, dub, wb, dsem, wsem = refs
    else:
        dup_ref, w_ref, *outs, wb, wsem = refs
    width = outs[0].shape[1]
    n = outs[0].shape[0]
    blk = 256
    nb = width // blk
    for i in range(nb):
        pltpu.make_async_copy(w_ref.at[pl.ds(lo + i * blk, blk), :], wb.at[pl.ds(i * blk, blk), :], wsem.at[i]).start()
    if first:
        k, tl = dub.shape[0], dub.shape[1] // 4
        dc = pltpu.make_async_copy(du_ref, dub, dsem)
        dc.start()
        r = lax.axis_index("tp")
        dc.wait()
        for a, j in enumerate((2, 3, 1, 0)):
            q = r ^ j
            for m in range(k):
                dup_ref[pl.ds(a * n + m * tl, tl), :] = dub[m, pl.ds(pl.multiple_of(q * tl, tl), tl), :]
    for i in range(nb):
        pltpu.make_async_copy(w_ref.at[pl.ds(lo + i * blk, blk), :], wb.at[pl.ds(i * blk, blk), :], wsem.at[i]).wait()
        p = lax.dot_general(dup_ref[...], wb[i * blk:(i + 1) * blk, :], (((1,), (1,)), ((), ())), preferred_element_type=F32)
        for a in range(4):
            outs[a][:, i * blk:(i + 1) * blk] = p[a * n:(a + 1) * n].astype(BF16)


def zero_start(z, de_ref, lo, rows, sem):
    step = z.shape[0]
    for i in range(rows // step):
        pltpu.make_async_copy(z, de_ref.at[pl.ds(lo + i * step, step), :], sem).start()


def zero_wait(z, de_ref, rows, sem):
    step = z.shape[0]
    for _ in range(rows // step):
        pltpu.make_async_copy(z, de_ref.at[pl.ds(0, step), :], sem).wait()


def zero_kernel(tok_ref, de_ref, z, sem):
    z[...] = jnp.zeros_like(z)
    zero_start(z, de_ref, 0, de_ref.shape[0], sem)
    zero_wait(z, de_ref, de_ref.shape[0], sem)


def gather_kernel(tok_ref, ids_ref, emb_ref, k0, s0, k1, s1, last_ref, dup_ref, cnt_ref,
                  buf, tmp, xf, lpos, lrow, lnxt, tab, sem):
    k, t = ids_ref.shape
    vl = emb_ref.shape[0]
    h = k0.shape[0]
    tl = t // 4
    r = lax.axis_index("tp")
    n = 0
    for m in range(k):
        def scan(i, n):
            v = ids_ref[m, i] - r * vl
            q = i // tl
            lpos[n] = m * t + ((q ^ r) & 1) * h + (q >> 1) * tl + (i & (tl - 1))
            lrow[n] = v
            return n + jnp.logical_and(v >= 0, v < vl).astype(jnp.int32)

        n = lax.fori_loop(0, t, scan, n, unroll=8)

    def start(i, c):
        v = lrow[i]
        b = pl.multiple_of((v >> 3) << 3, 8)
        pltpu.make_async_copy(emb_ref.at[pl.ds(b, 8), :], buf.at[i], sem).start()
        lnxt[i] = -1
        return c

    lax.fori_loop(0, n, start, 0)
    for a in range(8):
        lpos[n + a] = k * t
        lrow[n + a] = 0
    xf[...] = jnp.zeros_like(xf)

    def link(i, c):
        v = lrow[i]
        p = tab[v]
        ok = jnp.logical_and(p >= 0, p < i)
        p = jnp.where(ok, p, 0)
        ok = jnp.logical_and(ok, lrow[p] == v)
        lnxt[jnp.where(ok, p, k * t)] = i
        tab[v] = i
        return c

    lax.fori_loop(0, n, link, 0)

    def lists(i, c):
        nl, nd, n0 = c
        x = lnxt[i]
        end = (x < 0).astype(jnp.int32)
        last_ref[0, nl] = lpos[i]
        last_ref[1, nl] = lrow[i]
        dup_ref[0, nd] = lpos[i]
        dup_ref[1, nd] = lpos[jnp.maximum(x, 0)]
        return nl + end, nd + 1 - end, n0 + end * (lpos[i] < t).astype(jnp.int32)

    nl, nd, n0 = lax.fori_loop(0, n, lists, (0, 0, 0))
    cnt_ref[0] = nl
    cnt_ref[1] = nd
    cnt_ref[2] = n0

    def wait(i, c):
        pltpu.make_async_copy(emb_ref.at[pl.ds(0, 8), :], buf.at[0], sem).wait()
        return c

    lax.fori_loop(0, n, wait, 0)

    def take(g, c):
        for a in range(8):
            tmp[a] = buf[g * 8 + a].astype(F32)
        for a in range(8):
            i = g * 8 + a
            xf[pl.ds(lpos[i], 1), :] = tmp[a, pl.ds(lrow[i] & 7, 1), :]
        return c

    lax.fori_loop(0, (n + 7) // 8, take, 0)
    for a, ref in enumerate((k0, s0, k1, s1)):
        ref[...] = xf[a * h:(a + 1) * h, :].astype(BF16)


def dx_kernel(m, xh_ref, z_ref, p0, p1, p2, p3, r0, r1, r2, r3, dres_ref, g_ref, tok_ref, *refs):
    if m == 1:
        xm0_ref, dg0_ref, xm_ref, dx_ref, dg_ref, x_ref = refs
    else:
        xm_ref, dx_ref, dg_ref = refs
    tl = dx_ref.shape[0]
    chip = lax.axis_index("tp") >> 1
    mine = pl.ds(pl.multiple_of(chip * tl, tl), tl)
    xm_ref[...] = xh_ref[...] + z_ref[...]
    if m == 1:
        x_ref[0] = xm0_ref[mine, :]
        x_ref[1] = xm_ref[mine, :]
    x = xm_ref[mine, :].astype(F32)
    g = g_ref[...].astype(F32)
    rs = lax.rsqrt(jnp.mean(x * x, axis=-1, keepdims=True) + EPS)
    nh = x * rs
    s = slice(m * tl, (m + 1) * tl)
    dn = jnp.concatenate([
        (a[s, :].astype(F32) + b[s, :].astype(F32)) + (c[s, :].astype(F32) + e[s, :].astype(F32))
        for a, b, c, e in ((p0, p1, p2, p3), (r0, r1, r2, r3))], axis=1)
    gdn = g * dn
    mean = jnp.mean(nh * gdn, axis=-1, keepdims=True)
    dxn = rs * (gdn - nh * mean)
    dx_ref[...] = (dres_ref[m].astype(F32) + dxn).astype(BF16)
    dg = jnp.sum(dn * nh, axis=0, keepdims=True)
    dg_ref[...] = dg if m == 0 else dg + dg0_ref[...]


def fill_n(xm_ref, xo_ref, g_ref, n_ref, off):
    r = lax.axis_index("tp")
    par = r & 1
    tl = xm_ref.shape[0] // 2
    g = g_ref[...].astype(F32)
    for side, ref in ((0, xm_ref), (1, xo_ref)):
        for c in range(2):
            q = 2 * c + (par ^ side)
            x = ref[c * tl:(c + 1) * tl, :].astype(F32)
            rs = lax.rsqrt(jnp.mean(x * x, axis=-1, keepdims=True) + EPS)
            n_ref[pl.ds(pl.multiple_of(off + q * tl, tl), tl), :] = ((x * rs) * g).astype(BF16)


def umat(n_ref, w_ref, u_ref, lo):
    t = u_ref.shape[0]
    blk = 256
    for i in range(u_ref.shape[1] // blk):
        u_ref[:, i * blk:(i + 1) * blk] = jnp.dot(
            n_ref[lo:lo + t, :], w_ref[:, i * blk:(i + 1) * blk], preferred_element_type=F32).astype(BF16)


def u_kernel(xm_ref, xo_ref, g_ref, w_ref, tok_ref, u_ref, n_ref, flag_ref, ub, usem):
    flag_ref[0] = 0
    fill_n(xm_ref, xo_ref, g_ref, n_ref, 0)
    umat(n_ref, w_ref, ub, 0)
    c = pltpu.make_async_copy(ub, u_ref.at[0], usem)
    c.start()
    c.wait()


def proj_kernel(n0_ref, xm_ref, xo_ref, g_ref, w_ref, du_ref, u_in, tok_ref, u_ref, dw_ref, flag_ref, n_ref, du2, ub, dwb, usem, wsem):
    flag_ref[0] = 0
    k, t = du_ref.shape[0], du_ref.shape[1]
    d, _ = w_ref.shape
    copies = []
    n_ref[0:t, :] = n0_ref[...]
    fill_n(xm_ref, xo_ref, g_ref, n_ref, t)
    for m in range(k):
        du2[m * t:(m + 1) * t, :] = du_ref[m]
    umat(n_ref, w_ref, ub, t)
    c = pltpu.make_async_copy(ub, u_ref.at[1], usem)
    c.start()
    copies.append(c)
    blk = 256
    for i in range(d // blk):
        dwb[i] = lax.dot_general(n_ref[:, i * blk:(i + 1) * blk], du2[...], (((0,), (0,)), ((), ())),
                                 preferred_element_type=F32)
        c = pltpu.make_async_copy(dwb.at[i], dw_ref.at[pl.ds(i * blk, blk), :], wsem)
        c.start()
        copies.append(c)
    for c in copies:
        c.wait()


def scatter_kernel(m, last_ref, dup_ref, cnt_ref, *refs):
    nd = 4 * (m + 1)
    ds, de_ref, xf, sem = refs[:nd], refs[-3], refs[-2], refs[-1]
    tl = ds[0].shape[0]
    chip = lax.axis_index("tp") >> 1
    for a, ref in enumerate(ds):
        c = chip if a % 2 == 0 else 1 - chip
        xf[pl.ds(pl.multiple_of((a // 2) * 2 * tl + c * tl, tl), tl), :] = ref[...].astype(F32)

    def add(i, c):
        a = dup_ref[0, i]
        b = dup_ref[1, i]

        @pl.when(b < 4 * tl * (m + 1))
        def _():
            xf[pl.ds(b, 1), :] = xf[pl.ds(b, 1), :] + xf[pl.ds(a, 1), :]

        return c

    lax.fori_loop(0, cnt_ref[1], add, 0)

    def put(i, c):
        pltpu.make_async_copy(xf.at[pl.ds(last_ref[0, i], 1), :], de_ref.at[pl.ds(last_ref[1, i], 1), :], sem).start()
        return c

    def wait(i, c):
        pltpu.make_async_copy(xf.at[pl.ds(0, 1), :], de_ref.at[pl.ds(0, 1), :], sem).wait()
        return c

    n0, n1 = (0, cnt_ref[2]) if m == 0 else (cnt_ref[2], cnt_ref[0])
    lax.fori_loop(n0, n1, put, 0)
    lax.fori_loop(n0, n1, wait, 0)


def solution(mesh):
    groups = mesh.shape["tp"]
    sib = [(i, i ^ 1) for i in range(groups)]
    cross = [(i, i ^ 2) for i in range(groups)]
    diag = [(i, i ^ 3) for i in range(groups)]

    def local(ids, emb, g, w, du, dres):
        k, t = ids.shape
        vl, d = emb.shape
        fc = w.shape[1]
        tl = t // groups
        n = k * tl
        h = 2 * n
        g2 = g.reshape(1, d)
        S = jax.ShapeDtypeStruct
        D = pltpu.SemaphoreType.DMA

        def perm(v, p):
            return lax.ppermute(v, "tp", p)

        d1 = 5 * 256
        d2 = d - d1
        p2, p3, p1, p0, dup4 = call(
            functools.partial(pdn_kernel, 0, True), 60, [S((n, d1), BF16)] * 4 + [S((4 * n, fc), BF16)],
            [HBM] * 2, [VMEM] * 5, [pltpu.VMEM((k, t, fc), BF16), pltpu.VMEM((d1, fc), BF16), D, D((d1 // 256,))],
            8 * n * fc * d1, 2 * d1 * fc + 8 * n * (fc + d1))(du, w)
        r2, r3, r1, r0 = call(
            functools.partial(pdn_kernel, d1, False), 60, [S((n, d2), BF16)] * 4,
            [VMEM, HBM], [VMEM] * 4, [pltpu.VMEM((d2, fc), BF16), D((d2 // 256,))],
            8 * n * fc * d2, 2 * d2 * fc + 8 * n * (fc + d2))(dup4, w)
        q2 = perm(p2, cross)
        q3 = perm(p3, diag)
        v2 = perm(r2, cross)
        v3 = perm(r3, diag)
        q1 = perm(p1, sib)
        v1 = perm(r1, sib)

        k0, s0, k1, s1, last, dup, cnt = call(
            gather_kernel, 60,
            [S((n, d), BF16)] * 4 + [S((2, 2 * h + 8), jnp.int32)] * 2 + [S((8,), jnp.int32)],
            [HBM, SMEM, HBM], [VMEM] * 4 + [SMEM] * 3,
            [pltpu.VMEM((2 * h, 8, d), BF16), pltpu.VMEM((8, 8, d), F32), pltpu.VMEM((2 * h + 8, d), F32)]
            + [pltpu.SMEM((2 * h + 8,), jnp.int32)] * 3 + [pltpu.SMEM((vl,), jnp.int32), D],
            500_000_000, 16 * h * d)(r2, ids, emb)
        y0 = perm(s0, sib)
        y1 = perm(s1, sib)
        xh0 = k0 + y0
        xh1 = k1 + y1
        z0 = perm(xh0, cross)
        z1 = perm(xh1, cross)
        de = call(zero_kernel, 8, S((vl, d), F32), [SMEM], HBM,
                  [pltpu.VMEM((256, d), F32), D], 10_000_000_000, 4 * vl * d)(cnt)

        def dxk(m, xh, z, tok, more):
            outs = [S((n, d), BF16), S((tl, d), BF16), S((1, d), F32)] + ([S((k, tl, d), BF16)] if m else [])
            return call(functools.partial(dx_kernel, m), 16, outs, [VMEM] * 12 + [SMEM if m else HBM] + [VMEM] * len(more),
                        [VMEM] * len(outs), [], 30 * n * d, 16 * n * d)(xh, z, p0, q1, q2, q3, r0, v1, v2, v3, dres, g2, tok, *more)

        xm0, dx0, dg0 = dxk(0, xh0, z0, de, ())
        c0 = perm(dx0, cross)
        xo0 = perm(xm0, sib)
        a0 = perm(dx0, sib)
        u, n0, done0 = call(
            u_kernel, 24, [S((k, t, fc), BF16), S((t, d), BF16), S((8,), jnp.int32)], [VMEM] * 5, [HBM, VMEM, SMEM],
            [pltpu.VMEM((t, fc), BF16), D], 2 * t * d * fc, 2 * d * fc)(xm0, xo0, g2, w, dg0)
        xm1, dx1, dg, x = dxk(1, xh1, z1, done0, (xm0, dg0))
        c1 = perm(dx1, cross)
        xo1 = perm(xm1, sib)
        a1 = perm(dx1, sib)
        b0 = perm(c0, sib)
        b1 = perm(c1, sib)
        dgs = dg + perm(dg, sib)
        dgs = dgs + perm(dgs, cross)

        u, dw, done1 = call(
            proj_kernel, 36, [S((k, t, fc), BF16), S((d, fc), F32), S((8,), jnp.int32)],
            [VMEM] * 6 + [HBM, VMEM], [HBM, HBM, SMEM],
            [pltpu.VMEM((k * t, d), BF16), pltpu.VMEM((k * t, fc), BF16), pltpu.VMEM((t, fc), BF16),
             pltpu.VMEM((d // 256, 256, fc), F32), D, D],
            3 * k * t * d * fc, 6 * d * fc, {6: 0})(n0, xm1, xo1, g2, w, du, u, dg)

        def scatter(m, parts, de, tok):
            return call(functools.partial(scatter_kernel, m), 16, S((vl, d), F32),
                        [SMEM] * 3 + [VMEM] * len(parts) + [SMEM, HBM], HBM,
                        [pltpu.VMEM((h * (m + 1), d), F32), D], 8 * h * d, 8 * h * d,
                        {4 + len(parts): 0})(last, dup, cnt, *parts, tok, de)

        de = scatter(0, (dx0, c0, a0, b0), de, done1)
        de = scatter(1, (dx0, c0, a0, b0, dx1, c1, a1, b1), de, done1)
        return u, x, de, dw, dgs.reshape(d)

    return jax.shard_map(
        local,
        mesh=mesh,
        in_specs=(P("dp", None), P("tp", None), P(None), P(None, "tp"), P("dp", None, "tp"), P("dp", "tp", None)),
        out_specs=(P("dp", None, "tp"), P("dp", "tp", None), P(("dp", "tp"), None), P(None, ("dp", "tp")), P("dp")),
        check_vma=False,
    )
```

```python
import functools

import jax
import jax.numpy as jnp
from jax import lax
from jax.experimental import pallas as pl
from jax.experimental.pallas import tpu as pltpu
from jax.sharding import PartitionSpec as P


EPS = 1e-6
F32 = jnp.float32
BF16 = jnp.bfloat16
HBM = pl.BlockSpec(memory_space=pltpu.HBM)
VMEM = pl.BlockSpec(memory_space=pltpu.VMEM)
SMEM = pl.BlockSpec(memory_space=pltpu.SMEM)


def call(body, mib, outs, ins, out_specs, scratch, flops, nbytes, aliases=None):
    return pl.pallas_call(
        body,
        out_shape=outs,
        in_specs=ins,
        out_specs=out_specs,
        scratch_shapes=scratch,
        input_output_aliases=aliases or {},
        cost_estimate=pl.CostEstimate(flops=flops, bytes_accessed=nbytes, transcendentals=0),
        compiler_params=pltpu.CompilerParams(vmem_limit_bytes=mib << 20),
    )


def pdn_kernel(lo, first, *refs):
    if first:
        du_ref, w_ref, *outs, dup_ref, dub, wb, dsem, wsem = refs
    else:
        dup_ref, w_ref, *outs, wb, wsem = refs
    width = outs[0].shape[1]
    n = outs[0].shape[0]
    blk = 256
    nb = width // blk
    for i in range(nb):
        pltpu.make_async_copy(w_ref.at[pl.ds(lo + i * blk, blk), :], wb.at[pl.ds(i * blk, blk), :], wsem.at[i]).start()
    if first:
        k, tl = dub.shape[0], dub.shape[1] // 4
        dc = pltpu.make_async_copy(du_ref, dub, dsem)
        dc.start()
        r = lax.axis_index("tp")
        dc.wait()
        for a, j in enumerate((2, 3, 1, 0)):
            q = r ^ j
            for m in range(k):
                dup_ref[pl.ds(a * n + m * tl, tl), :] = dub[m, pl.ds(pl.multiple_of(q * tl, tl), tl), :]
    for i in range(nb):
        pltpu.make_async_copy(w_ref.at[pl.ds(lo + i * blk, blk), :], wb.at[pl.ds(i * blk, blk), :], wsem.at[i]).wait()
        p = lax.dot_general(dup_ref[...], wb[i * blk:(i + 1) * blk, :], (((1,), (1,)), ((), ())), preferred_element_type=F32)
        for a in range(4):
            outs[a][:, i * blk:(i + 1) * blk] = p[a * n:(a + 1) * n].astype(BF16)


def zero_start(z, de_ref, lo, rows, sem):
    step = z.shape[0]
    for i in range(rows // step):
        pltpu.make_async_copy(z, de_ref.at[pl.ds(lo + i * step, step), :], sem).start()


def zero_wait(z, de_ref, rows, sem):
    step = z.shape[0]
    for _ in range(rows // step):
        pltpu.make_async_copy(z, de_ref.at[pl.ds(0, step), :], sem).wait()


def zero_kernel(lpos, lrow, cnt, last_ref, dup_ref, out_ref, de_ref, z, lnxt, tab, sem):
    z[...] = jnp.zeros_like(z)
    zero_start(z, de_ref, 0, de_ref.shape[0], sem)
    n = cnt[0]
    t = lnxt.shape[0] - 8

    def link(i, c):
        v = lrow[i]
        p = tab[v]
        ok = jnp.logical_and(p >= 0, p < i)
        p = jnp.where(ok, p, 0)
        ok = jnp.logical_and(ok, lrow[p] == v)
        lnxt[i] = -1
        lnxt[jnp.where(ok, p, t)] = i
        tab[v] = i
        return c

    lax.fori_loop(0, n, link, 0)

    def lists(i, c):
        nl, nd, n0 = c
        x = lnxt[i]
        end = (x < 0).astype(jnp.int32)
        last_ref[0, nl] = lpos[i]
        last_ref[1, nl] = lrow[i]
        dup_ref[0, nd] = lpos[i]
        dup_ref[1, nd] = lpos[jnp.maximum(x, 0)]
        return nl + end, nd + 1 - end, n0 + end * (lpos[i] < t // 2).astype(jnp.int32)

    nl, nd, n0 = lax.fori_loop(0, n, lists, (0, 0, 0))
    out_ref[0] = nl
    out_ref[1] = nd
    out_ref[2] = n0
    zero_wait(z, de_ref, de_ref.shape[0], sem)


def gather_kernel(tok_ref, ids_ref, emb_ref, k0, s0, k1, s1, lpos, lrow, cnt, buf, tmp, xf, lst, sem):
    k, t = ids_ref.shape
    vl = emb_ref.shape[0]
    h = k0.shape[0]
    tl = t // 4
    r = lax.axis_index("tp")
    n = 0
    for m in range(k):
        def scan(i, n):
            lst[n] = m * t + i
            return n + (lax.shift_right_logical(ids_ref[m, i], vl.bit_length() - 1) == r).astype(jnp.int32)

        n = lax.fori_loop(0, t, scan, n, unroll=16)
    cnt[0] = n

    def start(i, c):
        j = lst[i]
        m = j // t
        v = ids_ref[m, j & (t - 1)] - r * vl
        q = (j & (t - 1)) // tl
        pltpu.make_async_copy(emb_ref.at[pl.ds(pl.multiple_of((v >> 3) << 3, 8), 8), :], buf.at[i], sem).start()
        lpos[i] = m * t + ((q ^ r) & 1) * h + (q >> 1) * tl + (j & (tl - 1))
        lrow[i] = v
        return c

    lax.fori_loop(0, n, start, 0)
    for a in range(8):
        lpos[n + a] = k * t
        lrow[n + a] = 0
    xf[...] = jnp.zeros_like(xf)

    def wait(i, c):
        pltpu.make_async_copy(emb_ref.at[pl.ds(0, 8), :], buf.at[0], sem).wait()
        return c

    lax.fori_loop(0, n, wait, 0)

    def take(g, c):
        for a in range(8):
            tmp[a] = buf[g * 8 + a].astype(F32)
        for a in range(8):
            i = g * 8 + a
            xf[pl.ds(lpos[i], 1), :] = tmp[a, pl.ds(lrow[i] & 7, 1), :]
        return c

    lax.fori_loop(0, (n + 7) // 8, take, 0)
    for a, ref in enumerate((k0, s0, k1, s1)):
        ref[...] = xf[a * h:(a + 1) * h, :].astype(BF16)


def dx_kernel(m, xh_ref, z_ref, p0, p1, p2, p3, r0, r1, r2, r3, dres_ref, g_ref, tok_ref, *refs):
    if m == 1:
        xm0_ref, dg0_ref, xm_ref, dx_ref, dg_ref, x_ref = refs
    else:
        xm_ref, dx_ref, dg_ref = refs
    tl = dx_ref.shape[0]
    chip = lax.axis_index("tp") >> 1
    mine = pl.ds(pl.multiple_of(chip * tl, tl), tl)
    xm_ref[...] = xh_ref[...] + z_ref[...]
    if m == 1:
        x_ref[0] = xm0_ref[mine, :]
        x_ref[1] = xm_ref[mine, :]
    x = xm_ref[mine, :].astype(F32)
    g = g_ref[...].astype(F32)
    rs = lax.rsqrt(jnp.mean(x * x, axis=-1, keepdims=True) + EPS)
    nh = x * rs
    s = slice(m * tl, (m + 1) * tl)
    dn = jnp.concatenate([
        (a[s, :].astype(F32) + b[s, :].astype(F32)) + (c[s, :].astype(F32) + e[s, :].astype(F32))
        for a, b, c, e in ((p0, p1, p2, p3), (r0, r1, r2, r3))], axis=1)
    gdn = g * dn
    mean = jnp.mean(nh * gdn, axis=-1, keepdims=True)
    dxn = rs * (gdn - nh * mean)
    dx_ref[...] = (dres_ref[m].astype(F32) + dxn).astype(BF16)
    dg = jnp.sum(dn * nh, axis=0, keepdims=True)
    dg_ref[...] = dg if m == 0 else dg + dg0_ref[...]


def fill_n(xm_ref, xo_ref, g_ref, n_ref, off):
    r = lax.axis_index("tp")
    par = r & 1
    tl = xm_ref.shape[0] // 2
    g = g_ref[...].astype(F32)
    for side, ref in ((0, xm_ref), (1, xo_ref)):
        for c in range(2):
            q = 2 * c + (par ^ side)
            x = ref[c * tl:(c + 1) * tl, :].astype(F32)
            rs = lax.rsqrt(jnp.mean(x * x, axis=-1, keepdims=True) + EPS)
            n_ref[pl.ds(pl.multiple_of(off + q * tl, tl), tl), :] = ((x * rs) * g).astype(BF16)


def umat(n_ref, w_ref, u_ref, lo):
    t = u_ref.shape[0]
    blk = 256
    for i in range(u_ref.shape[1] // blk):
        u_ref[:, i * blk:(i + 1) * blk] = jnp.dot(
            n_ref[lo:lo + t, :], w_ref[:, i * blk:(i + 1) * blk], preferred_element_type=F32).astype(BF16)


def u_kernel(xm_ref, xo_ref, g_ref, w_ref, tok_ref, u_ref, n_ref, flag_ref, ub, usem):
    flag_ref[0] = 0
    fill_n(xm_ref, xo_ref, g_ref, n_ref, 0)
    umat(n_ref, w_ref, ub, 0)
    c = pltpu.make_async_copy(ub, u_ref.at[0], usem)
    c.start()
    c.wait()


def proj_kernel(n0_ref, xm_ref, xo_ref, g_ref, w_ref, du_ref, u_in, tok_ref, u_ref, dw_ref, flag_ref, n_ref, du2, ub, dwb, usem, wsem):
    flag_ref[0] = 0
    k, t = du_ref.shape[0], du_ref.shape[1]
    d, _ = w_ref.shape
    copies = []
    n_ref[0:t, :] = n0_ref[...]
    fill_n(xm_ref, xo_ref, g_ref, n_ref, t)
    for m in range(k):
        du2[m * t:(m + 1) * t, :] = du_ref[m]
    umat(n_ref, w_ref, ub, t)
    c = pltpu.make_async_copy(ub, u_ref.at[1], usem)
    c.start()
    copies.append(c)
    blk = 256
    for i in range(d // blk):
        dwb[i] = lax.dot_general(n_ref[:, i * blk:(i + 1) * blk], du2[...], (((0,), (0,)), ((), ())),
                                 preferred_element_type=F32)
        c = pltpu.make_async_copy(dwb.at[i], dw_ref.at[pl.ds(i * blk, blk), :], wsem)
        c.start()
        copies.append(c)
    for c in copies:
        c.wait()


def scatter_kernel(m, last_ref, dup_ref, cnt_ref, *refs):
    nd = 4 * (m + 1)
    ds, de_ref, xf, sem = refs[:nd], refs[-3], refs[-2], refs[-1]
    tl = ds[0].shape[0]
    chip = lax.axis_index("tp") >> 1
    for a, ref in enumerate(ds):
        c = chip if a % 2 == 0 else 1 - chip
        xf[pl.ds(pl.multiple_of((a // 2) * 2 * tl + c * tl, tl), tl), :] = ref[...].astype(F32)

    def add(i, c):
        a = dup_ref[0, i]
        b = dup_ref[1, i]

        @pl.when(b < 4 * tl * (m + 1))
        def _():
            xf[pl.ds(b, 1), :] = xf[pl.ds(b, 1), :] + xf[pl.ds(a, 1), :]

        return c

    lax.fori_loop(0, cnt_ref[1], add, 0)

    def put(i, c):
        pltpu.make_async_copy(xf.at[pl.ds(last_ref[0, i], 1), :], de_ref.at[pl.ds(last_ref[1, i], 1), :], sem).start()
        return c

    def wait(i, c):
        pltpu.make_async_copy(xf.at[pl.ds(0, 1), :], de_ref.at[pl.ds(0, 1), :], sem).wait()
        return c

    n0, n1 = (0, cnt_ref[2]) if m == 0 else (cnt_ref[2], cnt_ref[0])
    lax.fori_loop(n0, n1, put, 0)
    lax.fori_loop(n0, n1, wait, 0)


def solution(mesh):
    groups = mesh.shape["tp"]
    sib = [(i, i ^ 1) for i in range(groups)]
    cross = [(i, i ^ 2) for i in range(groups)]
    diag = [(i, i ^ 3) for i in range(groups)]

    def local(ids, emb, g, w, du, dres):
        k, t = ids.shape
        vl, d = emb.shape
        fc = w.shape[1]
        tl = t // groups
        n = k * tl
        h = 2 * n
        g2 = g.reshape(1, d)
        S = jax.ShapeDtypeStruct
        D = pltpu.SemaphoreType.DMA

        def perm(v, p):
            return lax.ppermute(v, "tp", p)

        d1 = 5 * 256
        d2 = d - d1
        p2, p3, p1, p0, dup4 = call(
            functools.partial(pdn_kernel, 0, True), 60, [S((n, d1), BF16)] * 4 + [S((4 * n, fc), BF16)],
            [HBM] * 2, [VMEM] * 5, [pltpu.VMEM((k, t, fc), BF16), pltpu.VMEM((d1, fc), BF16), D, D((d1 // 256,))],
            8 * n * fc * d1, 2 * d1 * fc + 8 * n * (fc + d1))(du, w)
        r2, r3, r1, r0 = call(
            functools.partial(pdn_kernel, d1, False), 60, [S((n, d2), BF16)] * 4,
            [VMEM, HBM], [VMEM] * 4, [pltpu.VMEM((d2, fc), BF16), D((d2 // 256,))],
            8 * n * fc * d2, 2 * d2 * fc + 8 * n * (fc + d2))(dup4, w)
        q2 = perm(p2, cross)
        q3 = perm(p3, diag)
        v2 = perm(r2, cross)
        v3 = perm(r3, diag)
        q1 = perm(p1, sib)
        v1 = perm(r1, sib)

        k0, s0, k1, s1, lpos, lrow, nown = call(
            gather_kernel, 60,
            [S((n, d), BF16)] * 4 + [S((2 * h + 8,), jnp.int32)] * 2 + [S((8,), jnp.int32)],
            [HBM, SMEM, HBM], [VMEM] * 4 + [SMEM] * 3,
            [pltpu.VMEM((2 * h, 8, d), BF16), pltpu.VMEM((8, 8, d), F32), pltpu.VMEM((2 * h + 8, d), F32)]
            + [pltpu.SMEM((2 * h + 8,), jnp.int32), D],
            500_000_000, 16 * h * d)(r2, ids, emb)
        y0 = perm(s0, sib)
        y1 = perm(s1, sib)
        xh0 = k0 + y0
        xh1 = k1 + y1
        z0 = perm(xh0, cross)
        z1 = perm(xh1, cross)
        last, dup, cnt, de = call(
            zero_kernel, 8, [S((2, 2 * h + 8), jnp.int32)] * 2 + [S((8,), jnp.int32), S((vl, d), F32)],
            [SMEM] * 3, [SMEM] * 3 + [HBM],
            [pltpu.VMEM((256, d), F32), pltpu.SMEM((2 * h + 8,), jnp.int32), pltpu.SMEM((vl,), jnp.int32), D],
            10_000_000_000, 4 * vl * d)(lpos, lrow, nown)

        def dxk(m, xh, z, tok, more):
            outs = [S((n, d), BF16), S((tl, d), BF16), S((1, d), F32)] + ([S((k, tl, d), BF16)] if m else [])
            return call(functools.partial(dx_kernel, m), 16, outs, [VMEM] * 12 + [SMEM if m else HBM] + [VMEM] * len(more),
                        [VMEM] * len(outs), [], 30 * n * d, 16 * n * d)(xh, z, p0, q1, q2, q3, r0, v1, v2, v3, dres, g2, tok, *more)

        xm0, dx0, dg0 = dxk(0, xh0, z0, de, ())
        c0 = perm(dx0, cross)
        xo0 = perm(xm0, sib)
        a0 = perm(dx0, sib)
        u, n0, done0 = call(
            u_kernel, 24, [S((k, t, fc), BF16), S((t, d), BF16), S((8,), jnp.int32)], [VMEM] * 5, [HBM, VMEM, SMEM],
            [pltpu.VMEM((t, fc), BF16), D], 2 * t * d * fc, 2 * d * fc)(xm0, xo0, g2, w, dg0)
        xm1, dx1, dg, x = dxk(1, xh1, z1, done0, (xm0, dg0))
        c1 = perm(dx1, cross)
        xo1 = perm(xm1, sib)
        a1 = perm(dx1, sib)
        b0 = perm(c0, sib)
        b1 = perm(c1, sib)
        dgs = dg + perm(dg, sib)
        dgs = dgs + perm(dgs, cross)

        u, dw, done1 = call(
            proj_kernel, 36, [S((k, t, fc), BF16), S((d, fc), F32), S((8,), jnp.int32)],
            [VMEM] * 6 + [HBM, VMEM], [HBM, HBM, SMEM],
            [pltpu.VMEM((k * t, d), BF16), pltpu.VMEM((k * t, fc), BF16), pltpu.VMEM((t, fc), BF16),
             pltpu.VMEM((d // 256, 256, fc), F32), D, D],
            3 * k * t * d * fc, 6 * d * fc, {6: 0})(n0, xm1, xo1, g2, w, du, u, dg)

        def scatter(m, parts, de, tok):
            return call(functools.partial(scatter_kernel, m), 16, S((vl, d), F32),
                        [SMEM] * 3 + [VMEM] * len(parts) + [SMEM, HBM], HBM,
                        [pltpu.VMEM((h * (m + 1), d), F32), D], 8 * h * d, 8 * h * d,
                        {4 + len(parts): 0})(last, dup, cnt, *parts, tok, de)

        de = scatter(0, (dx0, c0, a0, b0), de, done1)
        de = scatter(1, (dx0, c0, a0, b0, dx1, c1, a1, b1), de, done1)
        return u, x, de, dw, dgs.reshape(d)

    return jax.shard_map(
        local,
        mesh=mesh,
        in_specs=(P("dp", None), P("tp", None), P(None), P(None, "tp"), P("dp", None, "tp"), P("dp", "tp", None)),
        out_specs=(P("dp", None, "tp"), P("dp", "tp", None), P(("dp", "tp"), None), P(None, ("dp", "tp")), P("dp")),
        check_vma=False,
    )
```

```python
import functools

import jax
import jax.numpy as jnp
from jax import lax
from jax.experimental import pallas as pl
from jax.experimental.pallas import tpu as pltpu
from jax.sharding import PartitionSpec as P


EPS = 1e-6
F32 = jnp.float32
BF16 = jnp.bfloat16
HBM = pl.BlockSpec(memory_space=pltpu.HBM)
VMEM = pl.BlockSpec(memory_space=pltpu.VMEM)
SMEM = pl.BlockSpec(memory_space=pltpu.SMEM)


def call(body, mib, outs, ins, out_specs, scratch, flops, nbytes, aliases=None):
    return pl.pallas_call(
        body,
        out_shape=outs,
        in_specs=ins,
        out_specs=out_specs,
        scratch_shapes=scratch,
        input_output_aliases=aliases or {},
        cost_estimate=pl.CostEstimate(flops=flops, bytes_accessed=nbytes, transcendentals=0),
        compiler_params=pltpu.CompilerParams(vmem_limit_bytes=mib << 20),
    )


def pdn_kernel(lo, first, *refs):
    if first:
        du_ref, w_ref, *outs, dup_ref, dub, wb, dsem, wsem = refs
    else:
        dup_ref, w_ref, *outs, de_ref, wb, z, wsem, zsem = refs
    width = outs[0].shape[1]
    n = outs[0].shape[0]
    blk = 256
    nb = width // blk
    for i in range(nb):
        pltpu.make_async_copy(w_ref.at[pl.ds(lo + i * blk, blk), :], wb.at[pl.ds(i * blk, blk), :], wsem.at[i]).start()
    if not first:
        z[...] = jnp.zeros_like(z)
        zero_start(z, de_ref, *FILL[0], zsem)
    if first:
        k, tl = dub.shape[0], dub.shape[1] // 4
        dc = pltpu.make_async_copy(du_ref, dub, dsem)
        dc.start()
        r = lax.axis_index("tp")
        dc.wait()
        for a, j in enumerate((2, 3, 1, 0)):
            q = r ^ j
            for m in range(k):
                dup_ref[pl.ds(a * n + m * tl, tl), :] = dub[m, pl.ds(pl.multiple_of(q * tl, tl), tl), :]
    for i in range(nb):
        pltpu.make_async_copy(w_ref.at[pl.ds(lo + i * blk, blk), :], wb.at[pl.ds(i * blk, blk), :], wsem.at[i]).wait()
        p = lax.dot_general(dup_ref[...], wb[i * blk:(i + 1) * blk, :], (((1,), (1,)), ((), ())), preferred_element_type=F32)
        for a in range(4):
            outs[a][:, i * blk:(i + 1) * blk] = p[a * n:(a + 1) * n].astype(BF16)
    if not first:
        zero_wait(z, de_ref, *FILL[0], zsem)


FILL = ((0, 3), (3, 6), (6, 9), (9, 16))


def zero_start(z, de_ref, lo, hi, sem):
    step = z.shape[0]
    per = de_ref.shape[0] // 16
    for i in range((hi - lo) * per // step):
        pltpu.make_async_copy(z, de_ref.at[pl.ds(lo * per + i * step, step), :], sem).start()


def zero_wait(z, de_ref, lo, hi, sem):
    step = z.shape[0]
    for _ in range((hi - lo) * (de_ref.shape[0] // 16) // step):
        pltpu.make_async_copy(z, de_ref.at[pl.ds(0, step), :], sem).wait()


def zero_kernel(lpos, lrow, cnt, de_in, last_ref, dup_ref, out_ref, de_ref, z, lnxt, tab, sem):
    z[...] = jnp.zeros_like(z)
    zero_start(z, de_ref, *FILL[3], sem)
    n = cnt[0]
    t = lnxt.shape[0] - 8

    def link(i, c):
        v = lrow[i]
        p = tab[v]
        ok = jnp.logical_and(p >= 0, p < i)
        p = jnp.where(ok, p, 0)
        ok = jnp.logical_and(ok, lrow[p] == v)
        lnxt[i] = -1
        lnxt[jnp.where(ok, p, t)] = i
        tab[v] = i
        return c

    lax.fori_loop(0, n, link, 0)

    def lists(i, c):
        nl, nd, n0 = c
        x = lnxt[i]
        end = (x < 0).astype(jnp.int32)
        last_ref[0, nl] = lpos[i]
        last_ref[1, nl] = lrow[i]
        dup_ref[0, nd] = lpos[i]
        dup_ref[1, nd] = lpos[jnp.maximum(x, 0)]
        return nl + end, nd + 1 - end, n0 + end * (lpos[i] < t // 2).astype(jnp.int32)

    nl, nd, n0 = lax.fori_loop(0, n, lists, (0, 0, 0))
    out_ref[0] = nl
    out_ref[1] = nd
    out_ref[2] = n0
    zero_wait(z, de_ref, *FILL[3], sem)


def gather_kernel(ids_ref, emb_ref, de_in, k0, s0, k1, s1, lpos, lrow, cnt, de_ref, buf, tmp, xf, z, lst, sem, zsem):
    k, t = ids_ref.shape
    vl = emb_ref.shape[0]
    h = k0.shape[0]
    tl = t // 4
    r = lax.axis_index("tp")
    z[...] = jnp.zeros_like(z)
    zero_start(z, de_ref, *FILL[1], zsem)
    n = 0
    for m in range(k):
        def scan(i, n):
            lst[n] = m * t + i
            return n + (lax.shift_right_logical(ids_ref[m, i], vl.bit_length() - 1) == r).astype(jnp.int32)

        n = lax.fori_loop(0, t, scan, n, unroll=16)
    cnt[0] = n

    def start(i, c):
        j = lst[i]
        m = j // t
        v = ids_ref[m, j & (t - 1)] - r * vl
        q = (j & (t - 1)) // tl
        pltpu.make_async_copy(emb_ref.at[pl.ds(pl.multiple_of((v >> 3) << 3, 8), 8), :], buf.at[i], sem).start()
        lpos[i] = m * t + ((q ^ r) & 1) * h + (q >> 1) * tl + (j & (tl - 1))
        lrow[i] = v
        return c

    lax.fori_loop(0, n, start, 0)
    zero_start(z, de_ref, *FILL[2], zsem)
    for a in range(8):
        lpos[n + a] = k * t
        lrow[n + a] = 0
    xf[...] = jnp.zeros_like(xf)

    def wait(i, c):
        pltpu.make_async_copy(emb_ref.at[pl.ds(0, 8), :], buf.at[0], sem).wait()
        return c

    lax.fori_loop(0, n, wait, 0)

    def take(g, c):
        for a in range(8):
            tmp[a] = buf[g * 8 + a].astype(F32)
        for a in range(8):
            i = g * 8 + a
            xf[pl.ds(lpos[i], 1), :] = tmp[a, pl.ds(lrow[i] & 7, 1), :]
        return c

    lax.fori_loop(0, (n + 7) // 8, take, 0)
    for a, ref in enumerate((k0, s0, k1, s1)):
        ref[...] = xf[a * h:(a + 1) * h, :].astype(BF16)
    zero_wait(z, de_ref, FILL[1][0], FILL[2][1], zsem)


def dx_kernel(m, xh_ref, z_ref, p0, p1, p2, p3, r0, r1, r2, r3, dres_ref, g_ref, tok_ref, *refs):
    if m == 1:
        xm0_ref, dg0_ref, xm_ref, dx_ref, dg_ref, x_ref = refs
    else:
        xm_ref, dx_ref, dg_ref = refs
    tl = dx_ref.shape[0]
    chip = lax.axis_index("tp") >> 1
    mine = pl.ds(pl.multiple_of(chip * tl, tl), tl)
    xm_ref[...] = xh_ref[...] + z_ref[...]
    if m == 1:
        x_ref[0] = xm0_ref[mine, :]
        x_ref[1] = xm_ref[mine, :]
    x = xm_ref[mine, :].astype(F32)
    g = g_ref[...].astype(F32)
    rs = lax.rsqrt(jnp.mean(x * x, axis=-1, keepdims=True) + EPS)
    nh = x * rs
    s = slice(m * tl, (m + 1) * tl)
    dn = jnp.concatenate([
        (a[s, :].astype(F32) + b[s, :].astype(F32)) + (c[s, :].astype(F32) + e[s, :].astype(F32))
        for a, b, c, e in ((p0, p1, p2, p3), (r0, r1, r2, r3))], axis=1)
    gdn = g * dn
    mean = jnp.mean(nh * gdn, axis=-1, keepdims=True)
    dxn = rs * (gdn - nh * mean)
    dx_ref[...] = (dres_ref[m].astype(F32) + dxn).astype(BF16)
    dg = jnp.sum(dn * nh, axis=0, keepdims=True)
    dg_ref[...] = dg if m == 0 else dg + dg0_ref[...]


def fill_n(xm_ref, xo_ref, g_ref, n_ref, off):
    r = lax.axis_index("tp")
    par = r & 1
    tl = xm_ref.shape[0] // 2
    g = g_ref[...].astype(F32)
    for side, ref in ((0, xm_ref), (1, xo_ref)):
        for c in range(2):
            q = 2 * c + (par ^ side)
            x = ref[c * tl:(c + 1) * tl, :].astype(F32)
            rs = lax.rsqrt(jnp.mean(x * x, axis=-1, keepdims=True) + EPS)
            n_ref[pl.ds(pl.multiple_of(off + q * tl, tl), tl), :] = ((x * rs) * g).astype(BF16)


def umat(n_ref, w_ref, u_ref, lo):
    t = u_ref.shape[0]
    blk = 256
    for i in range(u_ref.shape[1] // blk):
        u_ref[:, i * blk:(i + 1) * blk] = jnp.dot(
            n_ref[lo:lo + t, :], w_ref[:, i * blk:(i + 1) * blk], preferred_element_type=F32).astype(BF16)


def u_kernel(xm_ref, xo_ref, g_ref, w_ref, tok_ref, u_ref, n_ref, flag_ref, ub, usem):
    flag_ref[0] = 0
    fill_n(xm_ref, xo_ref, g_ref, n_ref, 0)
    umat(n_ref, w_ref, ub, 0)
    c = pltpu.make_async_copy(ub, u_ref.at[0], usem)
    c.start()
    c.wait()


def proj_kernel(n0_ref, xm_ref, xo_ref, g_ref, w_ref, du_ref, u_in, tok_ref, u_ref, dw_ref, flag_ref, n_ref, du2, ub, dwb, usem, wsem):
    flag_ref[0] = 0
    k, t = du_ref.shape[0], du_ref.shape[1]
    d, _ = w_ref.shape
    copies = []
    n_ref[0:t, :] = n0_ref[...]
    fill_n(xm_ref, xo_ref, g_ref, n_ref, t)
    for m in range(k):
        du2[m * t:(m + 1) * t, :] = du_ref[m]
    umat(n_ref, w_ref, ub, t)
    c = pltpu.make_async_copy(ub, u_ref.at[1], usem)
    c.start()
    copies.append(c)
    blk = 256
    for i in range(d // blk):
        dwb[i] = lax.dot_general(n_ref[:, i * blk:(i + 1) * blk], du2[...], (((0,), (0,)), ((), ())),
                                 preferred_element_type=F32)
        c = pltpu.make_async_copy(dwb.at[i], dw_ref.at[pl.ds(i * blk, blk), :], wsem)
        c.start()
        copies.append(c)
    for c in copies:
        c.wait()


def scatter_kernel(m, last_ref, dup_ref, cnt_ref, *refs):
    nd = 4 * (m + 1)
    ds, de_ref, xf, sem = refs[:nd], refs[-3], refs[-2], refs[-1]
    tl = ds[0].shape[0]
    chip = lax.axis_index("tp") >> 1
    for a, ref in enumerate(ds):
        c = chip if a % 2 == 0 else 1 - chip
        xf[pl.ds(pl.multiple_of((a // 2) * 2 * tl + c * tl, tl), tl), :] = ref[...].astype(F32)

    def add(i, c):
        a = dup_ref[0, i]
        b = dup_ref[1, i]

        @pl.when(b < 4 * tl * (m + 1))
        def _():
            xf[pl.ds(b, 1), :] = xf[pl.ds(b, 1), :] + xf[pl.ds(a, 1), :]

        return c

    lax.fori_loop(0, cnt_ref[1], add, 0)

    def put(i, c):
        pltpu.make_async_copy(xf.at[pl.ds(last_ref[0, i], 1), :], de_ref.at[pl.ds(last_ref[1, i], 1), :], sem).start()
        return c

    def wait(i, c):
        pltpu.make_async_copy(xf.at[pl.ds(0, 1), :], de_ref.at[pl.ds(0, 1), :], sem).wait()
        return c

    n0, n1 = (0, cnt_ref[2]) if m == 0 else (cnt_ref[2], cnt_ref[0])
    lax.fori_loop(n0, n1, put, 0)
    lax.fori_loop(n0, n1, wait, 0)


def solution(mesh):
    groups = mesh.shape["tp"]
    sib = [(i, i ^ 1) for i in range(groups)]
    cross = [(i, i ^ 2) for i in range(groups)]
    diag = [(i, i ^ 3) for i in range(groups)]

    def local(ids, emb, g, w, du, dres):
        k, t = ids.shape
        vl, d = emb.shape
        fc = w.shape[1]
        tl = t // groups
        n = k * tl
        h = 2 * n
        g2 = g.reshape(1, d)
        S = jax.ShapeDtypeStruct
        D = pltpu.SemaphoreType.DMA

        def perm(v, p):
            return lax.ppermute(v, "tp", p)

        d1 = 5 * 256
        d2 = d - d1
        p2, p3, p1, p0, dup4 = call(
            functools.partial(pdn_kernel, 0, True), 60, [S((n, d1), BF16)] * 4 + [S((4 * n, fc), BF16)],
            [HBM] * 2, [VMEM] * 5, [pltpu.VMEM((k, t, fc), BF16), pltpu.VMEM((d1, fc), BF16), D, D((d1 // 256,))],
            8 * n * fc * d1, 2 * d1 * fc + 8 * n * (fc + d1))(du, w)
        r2, r3, r1, r0, de = call(
            functools.partial(pdn_kernel, d1, False), 60, [S((n, d2), BF16)] * 4 + [S((vl, d), F32)],
            [VMEM, HBM], [VMEM] * 4 + [HBM], [pltpu.VMEM((d2, fc), BF16), pltpu.VMEM((256, d), F32), D((d2 // 256,)), D],
            8 * n * fc * d2, 2 * d2 * fc + 8 * n * (fc + d2))(dup4, w)
        q2 = perm(p2, cross)
        q3 = perm(p3, diag)
        v2 = perm(r2, cross)
        v3 = perm(r3, diag)
        q1 = perm(p1, sib)
        v1 = perm(r1, sib)

        k0, s0, k1, s1, lpos, lrow, nown, de = call(
            gather_kernel, 60,
            [S((n, d), BF16)] * 4 + [S((2 * h + 8,), jnp.int32)] * 2 + [S((8,), jnp.int32), S((vl, d), F32)],
            [SMEM, HBM, HBM], [VMEM] * 4 + [SMEM] * 3 + [HBM],
            [pltpu.VMEM((2 * h, 8, d), BF16), pltpu.VMEM((8, 8, d), F32), pltpu.VMEM((2 * h + 8, d), F32), pltpu.VMEM((256, d), F32)]
            + [pltpu.SMEM((2 * h + 8,), jnp.int32), D, D],
            500_000_000, 16 * h * d, {2: 7})(ids, emb, de)
        y0 = perm(s0, sib)
        y1 = perm(s1, sib)
        xh0 = k0 + y0
        xh1 = k1 + y1
        z0 = perm(xh0, cross)
        z1 = perm(xh1, cross)
        last, dup, cnt, de = call(
            zero_kernel, 8, [S((2, 2 * h + 8), jnp.int32)] * 2 + [S((8,), jnp.int32), S((vl, d), F32)],
            [SMEM] * 3 + [HBM], [SMEM] * 3 + [HBM],
            [pltpu.VMEM((256, d), F32), pltpu.SMEM((2 * h + 8,), jnp.int32), pltpu.SMEM((vl,), jnp.int32), D],
            10_000_000_000, 4 * vl * d, {3: 3})(lpos, lrow, nown, de)

        def dxk(m, xh, z, tok, more):
            outs = [S((n, d), BF16), S((tl, d), BF16), S((1, d), F32)] + ([S((k, tl, d), BF16)] if m else [])
            return call(functools.partial(dx_kernel, m), 16, outs, [VMEM] * 12 + [SMEM if m else HBM] + [VMEM] * len(more),
                        [VMEM] * len(outs), [], 30 * n * d, 16 * n * d)(xh, z, p0, q1, q2, q3, r0, v1, v2, v3, dres, g2, tok, *more)

        xm0, dx0, dg0 = dxk(0, xh0, z0, de, ())
        c0 = perm(dx0, cross)
        xo0 = perm(xm0, sib)
        a0 = perm(dx0, sib)
        u, n0, done0 = call(
            u_kernel, 24, [S((k, t, fc), BF16), S((t, d), BF16), S((8,), jnp.int32)], [VMEM] * 5, [HBM, VMEM, SMEM],
            [pltpu.VMEM((t, fc), BF16), D], 2 * t * d * fc, 2 * d * fc)(xm0, xo0, g2, w, dg0)
        xm1, dx1, dg, x = dxk(1, xh1, z1, done0, (xm0, dg0))
        c1 = perm(dx1, cross)
        xo1 = perm(xm1, sib)
        a1 = perm(dx1, sib)
        b0 = perm(c0, sib)
        b1 = perm(c1, sib)
        dgs = dg + perm(dg, sib)
        dgs = dgs + perm(dgs, cross)

        u, dw, done1 = call(
            proj_kernel, 36, [S((k, t, fc), BF16), S((d, fc), F32), S((8,), jnp.int32)],
            [VMEM] * 6 + [HBM, VMEM], [HBM, HBM, SMEM],
            [pltpu.VMEM((k * t, d), BF16), pltpu.VMEM((k * t, fc), BF16), pltpu.VMEM((t, fc), BF16),
             pltpu.VMEM((d // 256, 256, fc), F32), D, D],
            3 * k * t * d * fc, 6 * d * fc, {6: 0})(n0, xm1, xo1, g2, w, du, u, dg)

        def scatter(m, parts, de, tok):
            return call(functools.partial(scatter_kernel, m), 16, S((vl, d), F32),
                        [SMEM] * 3 + [VMEM] * len(parts) + [SMEM, HBM], HBM,
                        [pltpu.VMEM((h * (m + 1), d), F32), D], 8 * h * d, 8 * h * d,
                        {4 + len(parts): 0})(last, dup, cnt, *parts, tok, de)

        de = scatter(0, (dx0, c0, a0, b0), de, done1)
        de = scatter(1, (dx0, c0, a0, b0, dx1, c1, a1, b1), de, done1)
        return u, x, de, dw, dgs.reshape(d)

    return jax.shard_map(
        local,
        mesh=mesh,
        in_specs=(P("dp", None), P("tp", None), P(None), P(None, "tp"), P("dp", None, "tp"), P("dp", "tp", None)),
        out_specs=(P("dp", None, "tp"), P("dp", "tp", None), P(("dp", "tp"), None), P(None, ("dp", "tp")), P("dp")),
        check_vma=False,
    )
```

```python
import functools

import jax
import jax.numpy as jnp
from jax import lax
from jax.experimental import pallas as pl
from jax.experimental.pallas import tpu as pltpu
from jax.sharding import PartitionSpec as P


EPS = 1e-6
F32 = jnp.float32
BF16 = jnp.bfloat16
HBM = pl.BlockSpec(memory_space=pltpu.HBM)
VMEM = pl.BlockSpec(memory_space=pltpu.VMEM)
SMEM = pl.BlockSpec(memory_space=pltpu.SMEM)


def call(body, mib, outs, ins, out_specs, scratch, flops, nbytes, aliases=None):
    return pl.pallas_call(
        body,
        out_shape=outs,
        in_specs=ins,
        out_specs=out_specs,
        scratch_shapes=scratch,
        input_output_aliases=aliases or {},
        cost_estimate=pl.CostEstimate(flops=flops, bytes_accessed=nbytes, transcendentals=0),
        compiler_params=pltpu.CompilerParams(vmem_limit_bytes=mib << 20),
    )


def pdn_kernel(lo, first, *refs):
    if first:
        du_ref, w_ref, *outs, dup_ref, dub, wb, dsem, wsem = refs
    else:
        dup_ref, w_ref, de_in, *outs, de_ref, wb, z, wsem, zsem = refs
    width = outs[0].shape[1]
    n = outs[0].shape[0]
    blk = 256
    nb = width // blk
    if first:
        dc = pltpu.make_async_copy(du_ref, dub, dsem)
        dc.start()
    for i in range(nb):
        pltpu.make_async_copy(w_ref.at[pl.ds(lo + i * blk, blk), :], wb.at[pl.ds(i * blk, blk), :], wsem.at[i]).start()
    if not first:
        z[...] = jnp.zeros_like(z)
        zero_start(z, de_ref, *FILL[0], zsem)
    if first:
        k, tl = dub.shape[0], dub.shape[1] // 4
        r = lax.axis_index("tp")
        dc.wait()
        for a, j in enumerate((2, 3, 1, 0)):
            q = r ^ j
            for m in range(k):
                dup_ref[pl.ds(a * n + m * tl, tl), :] = dub[m, pl.ds(pl.multiple_of(q * tl, tl), tl), :]
    for i in range(nb):
        pltpu.make_async_copy(w_ref.at[pl.ds(lo + i * blk, blk), :], wb.at[pl.ds(i * blk, blk), :], wsem.at[i]).wait()
        p = lax.dot_general(dup_ref[...], wb[i * blk:(i + 1) * blk, :], (((1,), (1,)), ((), ())), preferred_element_type=F32)
        for a in range(4):
            outs[a][:, i * blk:(i + 1) * blk] = p[a * n:(a + 1) * n].astype(BF16)
    if not first:
        zero_wait(z, de_ref, *FILL[0], zsem)


FILL = ((0, 2), (2, 4), (4, 6), (6, 16))


def zero_start(z, de_ref, lo, hi, sem):
    step = z.shape[0]
    per = de_ref.shape[0] // 16
    for i in range((hi - lo) * per // step):
        pltpu.make_async_copy(z, de_ref.at[pl.ds(lo * per + i * step, step), :], sem).start()


def zero_wait(z, de_ref, lo, hi, sem):
    step = z.shape[0]
    for _ in range((hi - lo) * (de_ref.shape[0] // 16) // step):
        pltpu.make_async_copy(z, de_ref.at[pl.ds(0, step), :], sem).wait()


def zero_kernel(lpos, lrow, cnt, de_in, last_ref, dup_ref, out_ref, de_ref, z, lnxt, tab, sem):
    z[...] = jnp.zeros_like(z)
    zero_start(z, de_ref, *FILL[3], sem)
    n = cnt[0]
    t = lnxt.shape[0] - 8

    def link(i, c):
        v = lrow[i]
        p = tab[v]
        ok = jnp.logical_and(p >= 0, p < i)
        p = jnp.where(ok, p, 0)
        ok = jnp.logical_and(ok, lrow[p] == v)
        lnxt[i] = -1
        lnxt[jnp.where(ok, p, t)] = i
        tab[v] = i
        return c

    lax.fori_loop(0, n, link, 0)

    def lists(i, c):
        nl, nd = c
        x = lnxt[i]
        end = (x < 0).astype(jnp.int32)
        last_ref[0, nl] = lpos[i]
        last_ref[1, nl] = lrow[i]
        dup_ref[0, nd] = lpos[i]
        dup_ref[1, nd] = lpos[jnp.maximum(x, 0)]
        return nl + end, nd + 1 - end

    nl, nd = lax.fori_loop(0, n, lists, (0, 0))
    out_ref[0] = nl
    out_ref[1] = nd
    zero_wait(z, de_ref, *FILL[3], sem)


def gather_kernel(ids_ref, emb_ref, k0, s0, k1, s1, lpos, lrow, cnt, de_ref, buf, tmp, xf, z, lst, sem, zsem):
    k, t = ids_ref.shape
    vl = emb_ref.shape[0]
    h = k0.shape[0]
    tl = t // 4
    r = lax.axis_index("tp")
    z[...] = jnp.zeros_like(z)
    zero_start(z, de_ref, *FILL[1], zsem)
    n = 0
    for m in range(k):
        def scan(i, n):
            lst[n] = m * t + i
            return n + (lax.shift_right_logical(ids_ref[m, i], vl.bit_length() - 1) == r).astype(jnp.int32)

        n = lax.fori_loop(0, t, scan, n, unroll=16)
    cnt[0] = n

    def start(i, c):
        j = lst[i]
        m = j // t
        v = ids_ref[m, j & (t - 1)] - r * vl
        q = (j & (t - 1)) // tl
        pltpu.make_async_copy(emb_ref.at[pl.ds(pl.multiple_of((v >> 3) << 3, 8), 8), :], buf.at[i], sem).start()
        lpos[i] = m * t + ((q ^ r) & 1) * h + (q >> 1) * tl + (j & (tl - 1))
        lrow[i] = v
        return c

    lax.fori_loop(0, n, start, 0)
    zero_start(z, de_ref, *FILL[2], zsem)
    for a in range(8):
        lpos[n + a] = k * t
        lrow[n + a] = 0
    xf[...] = jnp.zeros_like(xf)

    def wait(i, c):
        pltpu.make_async_copy(emb_ref.at[pl.ds(0, 8), :], buf.at[0], sem).wait()
        return c

    lax.fori_loop(0, n, wait, 0)

    def take(g, c):
        for a in range(8):
            tmp[a] = buf[g * 8 + a].astype(F32)
        for a in range(8):
            i = g * 8 + a
            xf[pl.ds(lpos[i], 1), :] = tmp[a, pl.ds(lrow[i] & 7, 1), :]
        return c

    lax.fori_loop(0, (n + 7) // 8, take, 0)
    for a, ref in enumerate((k0, s0, k1, s1)):
        ref[...] = xf[a * h:(a + 1) * h, :].astype(BF16)
    zero_wait(z, de_ref, FILL[1][0], FILL[2][1], zsem)


def dx_kernel(m, xh_ref, z_ref, p0, p1, p2, p3, r0, r1, r2, r3, dres_ref, g_ref, tok_ref, *refs):
    if m == 1:
        xm0_ref, dg0_ref, xm_ref, dx_ref, dg_ref, x_ref = refs
    else:
        xm_ref, dx_ref, dg_ref = refs
    tl = dx_ref.shape[0]
    chip = lax.axis_index("tp") >> 1
    mine = pl.ds(pl.multiple_of(chip * tl, tl), tl)
    xm_ref[...] = xh_ref[...] + z_ref[...]
    if m == 1:
        x_ref[0] = xm0_ref[mine, :]
        x_ref[1] = xm_ref[mine, :]
    x = xm_ref[mine, :].astype(F32)
    g = g_ref[...].astype(F32)
    rs = lax.rsqrt(jnp.mean(x * x, axis=-1, keepdims=True) + EPS)
    nh = x * rs
    s = slice(m * tl, (m + 1) * tl)
    dn = jnp.concatenate([
        (a[s, :].astype(F32) + b[s, :].astype(F32)) + (c[s, :].astype(F32) + e[s, :].astype(F32))
        for a, b, c, e in ((p0, p1, p2, p3), (r0, r1, r2, r3))], axis=1)
    gdn = g * dn
    mean = jnp.mean(nh * gdn, axis=-1, keepdims=True)
    dxn = rs * (gdn - nh * mean)
    dx_ref[...] = (dres_ref[m].astype(F32) + dxn).astype(BF16)
    dg = jnp.sum(dn * nh, axis=0, keepdims=True)
    dg_ref[...] = dg if m == 0 else dg + dg0_ref[...]


def fill_n(xm_ref, xo_ref, g_ref, n_ref, off):
    r = lax.axis_index("tp")
    par = r & 1
    tl = xm_ref.shape[0] // 2
    g = g_ref[...].astype(F32)
    for side, ref in ((0, xm_ref), (1, xo_ref)):
        for c in range(2):
            q = 2 * c + (par ^ side)
            x = ref[c * tl:(c + 1) * tl, :].astype(F32)
            rs = lax.rsqrt(jnp.mean(x * x, axis=-1, keepdims=True) + EPS)
            n_ref[pl.ds(pl.multiple_of(off + q * tl, tl), tl), :] = ((x * rs) * g).astype(BF16)


def umat(n_ref, w_ref, u_ref, lo):
    t = u_ref.shape[0]
    blk = 256
    for i in range(u_ref.shape[1] // blk):
        u_ref[:, i * blk:(i + 1) * blk] = jnp.dot(
            n_ref[lo:lo + t, :], w_ref[:, i * blk:(i + 1) * blk], preferred_element_type=F32).astype(BF16)


def u_kernel(xm_ref, xo_ref, g_ref, w_ref, tok_ref, u_ref, n_ref, flag_ref, ub, usem):
    flag_ref[0] = 0
    fill_n(xm_ref, xo_ref, g_ref, n_ref, 0)
    umat(n_ref, w_ref, ub, 0)
    c = pltpu.make_async_copy(ub, u_ref.at[0], usem)
    c.start()
    c.wait()


def proj_kernel(n0_ref, xm_ref, xo_ref, g_ref, w_ref, du_ref, u_in, tok_ref, u_ref, dw_ref, flag_ref, n_ref, du2, ub, dwb, usem, wsem):
    flag_ref[0] = 0
    k, t = du_ref.shape[0], du_ref.shape[1]
    d, _ = w_ref.shape
    copies = []
    n_ref[0:t, :] = n0_ref[...]
    fill_n(xm_ref, xo_ref, g_ref, n_ref, t)
    for m in range(k):
        du2[m * t:(m + 1) * t, :] = du_ref[m]
    umat(n_ref, w_ref, ub, t)
    c = pltpu.make_async_copy(ub, u_ref.at[1], usem)
    c.start()
    copies.append(c)
    blk = 256
    for i in range(d // blk):
        dwb[i] = lax.dot_general(n_ref[:, i * blk:(i + 1) * blk], du2[...], (((0,), (0,)), ((), ())),
                                 preferred_element_type=F32)
        c = pltpu.make_async_copy(dwb.at[i], dw_ref.at[pl.ds(i * blk, blk), :], wsem)
        c.start()
        copies.append(c)
    for c in copies:
        c.wait()


def scatter_kernel(last_ref, dup_ref, cnt_ref, *refs):
    ds, de_ref, xf, sem = refs[:8], refs[-3], refs[-2], refs[-1]
    tl = ds[0].shape[0]
    chip = lax.axis_index("tp") >> 1
    for a, ref in enumerate(ds):
        c = chip if a % 2 == 0 else 1 - chip
        xf[pl.ds(pl.multiple_of((a // 2) * 2 * tl + c * tl, tl), tl), :] = ref[...].astype(F32)

    def add(i, c):
        a = dup_ref[0, i]
        b = dup_ref[1, i]
        xf[pl.ds(b, 1), :] = xf[pl.ds(b, 1), :] + xf[pl.ds(a, 1), :]
        return c

    lax.fori_loop(0, cnt_ref[1], add, 0)

    def put(i, c):
        pltpu.make_async_copy(xf.at[pl.ds(last_ref[0, i], 1), :], de_ref.at[pl.ds(last_ref[1, i], 1), :], sem).start()
        return c

    def wait(i, c):
        pltpu.make_async_copy(xf.at[pl.ds(0, 1), :], de_ref.at[pl.ds(0, 1), :], sem).wait()
        return c

    lax.fori_loop(0, cnt_ref[0], put, 0)
    lax.fori_loop(0, cnt_ref[0], wait, 0)


def solution(mesh):
    groups = mesh.shape["tp"]
    sib = [(i, i ^ 1) for i in range(groups)]
    cross = [(i, i ^ 2) for i in range(groups)]
    diag = [(i, i ^ 3) for i in range(groups)]

    def local(ids, emb, g, w, du, dres):
        k, t = ids.shape
        vl, d = emb.shape
        fc = w.shape[1]
        tl = t // groups
        n = k * tl
        h = 2 * n
        g2 = g.reshape(1, d)
        S = jax.ShapeDtypeStruct
        D = pltpu.SemaphoreType.DMA

        def perm(v, p):
            return lax.ppermute(v, "tp", p)

        d1 = 7 * 256
        d2 = d - d1
        p2, p3, p1, p0, dup4 = call(
            functools.partial(pdn_kernel, 0, True), 60, [S((n, d1), BF16)] * 4 + [S((4 * n, fc), BF16)],
            [HBM] * 2, [VMEM] * 5, [pltpu.VMEM((k, t, fc), BF16), pltpu.VMEM((d1, fc), BF16), D, D((d1 // 256,))],
            8 * n * fc * d1, 2 * d1 * fc + 8 * n * (fc + d1))(du, w)
        q2 = perm(p2, cross)
        q3 = perm(p3, diag)
        k0, s0, k1, s1, lpos, lrow, nown, de = call(
            gather_kernel, 60,
            [S((n, d), BF16)] * 4 + [S((2 * h + 8,), jnp.int32)] * 2 + [S((8,), jnp.int32), S((vl, d), F32)],
            [SMEM, HBM], [VMEM] * 4 + [SMEM] * 3 + [HBM],
            [pltpu.VMEM((2 * h, 8, d), BF16), pltpu.VMEM((8, 8, d), F32), pltpu.VMEM((2 * h + 8, d), F32), pltpu.VMEM((256, d), F32)]
            + [pltpu.SMEM((2 * h + 8,), jnp.int32), D, D],
            500_000_000, 16 * h * d)(ids, emb)
        y0 = perm(s0, sib)
        y1 = perm(s1, sib)
        r2, r3, r1, r0, de = call(
            functools.partial(pdn_kernel, d1, False), 60, [S((n, d2), BF16)] * 4 + [S((vl, d), F32)],
            [VMEM, HBM, HBM], [VMEM] * 4 + [HBM], [pltpu.VMEM((d2, fc), BF16), pltpu.VMEM((256, d), F32), D((d2 // 256,)), D],
            8 * n * fc * d2, 2 * d2 * fc + 8 * n * (fc + d2), {2: 4})(dup4, w, de)
        v2 = perm(r2, cross)
        v3 = perm(r3, diag)
        q1 = perm(p1, sib)
        v1 = perm(r1, sib)
        xh0 = k0 + y0
        xh1 = k1 + y1
        z0 = perm(xh0, cross)
        z1 = perm(xh1, cross)
        last, dup, cnt, de = call(
            zero_kernel, 8, [S((2, 2 * h + 8), jnp.int32)] * 2 + [S((8,), jnp.int32), S((vl, d), F32)],
            [SMEM] * 3 + [HBM], [SMEM] * 3 + [HBM],
            [pltpu.VMEM((256, d), F32), pltpu.SMEM((2 * h + 8,), jnp.int32), pltpu.SMEM((vl,), jnp.int32), D],
            10_000_000_000, 4 * vl * d, {3: 3})(lpos, lrow, nown, de)

        def dxk(m, xh, z, tok, more):
            outs = [S((n, d), BF16), S((tl, d), BF16), S((1, d), F32)] + ([S((k, tl, d), BF16)] if m else [])
            return call(functools.partial(dx_kernel, m), 16, outs, [VMEM] * 12 + [SMEM if m else HBM] + [VMEM] * len(more),
                        [VMEM] * len(outs), [], 30 * n * d, 16 * n * d)(xh, z, p0, q1, q2, q3, r0, v1, v2, v3, dres, g2, tok, *more)

        xm0, dx0, dg0 = dxk(0, xh0, z0, de, ())
        c0 = perm(dx0, cross)
        xo0 = perm(xm0, sib)
        a0 = perm(dx0, sib)
        u, n0, done0 = call(
            u_kernel, 24, [S((k, t, fc), BF16), S((t, d), BF16), S((8,), jnp.int32)], [VMEM] * 5, [HBM, VMEM, SMEM],
            [pltpu.VMEM((t, fc), BF16), D], 2 * t * d * fc, 2 * d * fc)(xm0, xo0, g2, w, dg0)
        xm1, dx1, dg, x = dxk(1, xh1, z1, done0, (xm0, dg0))
        c1 = perm(dx1, cross)
        xo1 = perm(xm1, sib)
        a1 = perm(dx1, sib)
        b0 = perm(c0, sib)
        b1 = perm(c1, sib)
        dgs = dg + perm(dg, sib)
        dgs = dgs + perm(dgs, cross)

        u, dw, done1 = call(
            proj_kernel, 36, [S((k, t, fc), BF16), S((d, fc), F32), S((8,), jnp.int32)],
            [VMEM] * 6 + [HBM, VMEM], [HBM, HBM, SMEM],
            [pltpu.VMEM((k * t, d), BF16), pltpu.VMEM((k * t, fc), BF16), pltpu.VMEM((t, fc), BF16),
             pltpu.VMEM((d // 256, 256, fc), F32), D, D],
            3 * k * t * d * fc, 6 * d * fc, {6: 0})(n0, xm1, xo1, g2, w, du, u, dg)

        de = call(scatter_kernel, 16, S((vl, d), F32), [SMEM] * 3 + [VMEM] * 8 + [SMEM, HBM], HBM,
                  [pltpu.VMEM((2 * h, d), F32), D], 8 * h * d, 8 * h * d,
                  {12: 0})(last, dup, cnt, dx0, c0, a0, b0, dx1, c1, a1, b1, done1, de)
        return u, x, de, dw, dgs.reshape(d)

    return jax.shard_map(
        local,
        mesh=mesh,
        in_specs=(P("dp", None), P("tp", None), P(None), P(None, "tp"), P("dp", None, "tp"), P("dp", "tp", None)),
        out_specs=(P("dp", None, "tp"), P("dp", "tp", None), P(("dp", "tp"), None), P(None, ("dp", "tp")), P("dp")),
        check_vma=False,
    )
```

```python
import functools

import jax
import jax.numpy as jnp
from jax import lax
from jax.experimental import pallas as pl
from jax.experimental.pallas import tpu as pltpu
from jax.sharding import PartitionSpec as P


EPS = 1e-6
F32 = jnp.float32
BF16 = jnp.bfloat16
HBM = pl.BlockSpec(memory_space=pltpu.HBM)
VMEM = pl.BlockSpec(memory_space=pltpu.VMEM)
SMEM = pl.BlockSpec(memory_space=pltpu.SMEM)


def call(body, mib, outs, ins, out_specs, scratch, flops, nbytes, aliases=None):
    return pl.pallas_call(
        body,
        out_shape=outs,
        in_specs=ins,
        out_specs=out_specs,
        scratch_shapes=scratch,
        input_output_aliases=aliases or {},
        cost_estimate=pl.CostEstimate(flops=flops, bytes_accessed=nbytes, transcendentals=0),
        compiler_params=pltpu.CompilerParams(vmem_limit_bytes=mib << 20),
    )


def pdn_kernel(lo, first, *refs):
    if first:
        du_ref, w_ref, *outs, dup_ref, dub, wb, dsem, wsem = refs
    else:
        dup_ref, w_ref, de_in, *outs, de_ref, wb, z, wsem, zsem = refs
    width = outs[0].shape[1]
    n = outs[0].shape[0]
    blk = 256
    nb = width // blk
    if first:
        dc = pltpu.make_async_copy(du_ref, dub, dsem)
        dc.start()
    for i in range(nb):
        pltpu.make_async_copy(w_ref.at[pl.ds(lo + i * blk, blk), :], wb.at[pl.ds(i * blk, blk), :], wsem.at[i]).start()
    if not first:
        z[...] = jnp.zeros_like(z)
        zero_start(z, de_ref, *FILL[0], zsem)
    if first:
        k, tl = dub.shape[0], dub.shape[1] // 4
        r = lax.axis_index("tp")
        dc.wait()
        for a, j in enumerate((2, 3, 1, 0)):
            q = r ^ j
            for m in range(k):
                dup_ref[pl.ds(a * n + m * tl, tl), :] = dub[m, pl.ds(pl.multiple_of(q * tl, tl), tl), :]
    for i in range(nb):
        pltpu.make_async_copy(w_ref.at[pl.ds(lo + i * blk, blk), :], wb.at[pl.ds(i * blk, blk), :], wsem.at[i]).wait()
        p = lax.dot_general(dup_ref[...], wb[i * blk:(i + 1) * blk, :], (((1,), (1,)), ((), ())), preferred_element_type=F32)
        for a in range(4):
            outs[a][:, i * blk:(i + 1) * blk] = p[a * n:(a + 1) * n].astype(BF16)
    if not first:
        zero_wait(z, de_ref, *FILL[0], zsem)


FILL = ((0, 2), (2, 4), (4, 6), (6, 10), (10, 13), (13, 16))


def zero_start(z, de_ref, lo, hi, sem):
    step = z.shape[0]
    per = de_ref.shape[0] // 16
    for i in range((hi - lo) * per // step):
        pltpu.make_async_copy(z, de_ref.at[pl.ds(lo * per + i * step, step), :], sem).start()


def zero_wait(z, de_ref, lo, hi, sem):
    step = z.shape[0]
    for _ in range((hi - lo) * (de_ref.shape[0] // 16) // step):
        pltpu.make_async_copy(z, de_ref.at[pl.ds(0, step), :], sem).wait()


def zero_kernel(lpos, lrow, cnt, de_in, last_ref, dup_ref, out_ref, de_ref, z, lnxt, tab, sem):
    z[...] = jnp.zeros_like(z)
    zero_start(z, de_ref, *FILL[3], sem)
    n = cnt[0]
    t = lnxt.shape[0] - 8

    def link(i, c):
        v = lrow[i]
        p = tab[v]
        ok = jnp.logical_and(p >= 0, p < i)
        p = jnp.where(ok, p, 0)
        ok = jnp.logical_and(ok, lrow[p] == v)
        lnxt[i] = -1
        lnxt[jnp.where(ok, p, t)] = i
        tab[v] = i
        return c

    lax.fori_loop(0, n, link, 0)

    def lists(i, c):
        nl, nd = c
        x = lnxt[i]
        end = (x < 0).astype(jnp.int32)
        last_ref[0, nl] = lpos[i]
        last_ref[1, nl] = lrow[i]
        dup_ref[0, nd] = lpos[i]
        dup_ref[1, nd] = lpos[jnp.maximum(x, 0)]
        return nl + end, nd + 1 - end

    nl, nd = lax.fori_loop(0, n, lists, (0, 0))
    out_ref[0] = nl
    out_ref[1] = nd
    zero_wait(z, de_ref, *FILL[3], sem)


def zero2_kernel(tok_ref, de_in, de_ref, z, sem):
    z[...] = jnp.zeros_like(z)
    zero_start(z, de_ref, *FILL[4], sem)
    zero_wait(z, de_ref, *FILL[4], sem)


def gather_kernel(ids_ref, emb_ref, k0, s0, k1, s1, lpos, lrow, cnt, de_ref, buf, tmp, xf, z, lst, sem, zsem):
    k, t = ids_ref.shape
    vl = emb_ref.shape[0]
    h = k0.shape[0]
    tl = t // 4
    r = lax.axis_index("tp")
    z[...] = jnp.zeros_like(z)
    zero_start(z, de_ref, *FILL[1], zsem)
    n = 0
    for m in range(k):
        def scan(i, n):
            lst[n] = m * t + i
            return n + (lax.shift_right_logical(ids_ref[m, i], vl.bit_length() - 1) == r).astype(jnp.int32)

        n = lax.fori_loop(0, t, scan, n, unroll=16)
    cnt[0] = n

    def start(i, c):
        j = lst[i]
        m = j // t
        v = ids_ref[m, j & (t - 1)] - r * vl
        q = (j & (t - 1)) // tl
        pltpu.make_async_copy(emb_ref.at[pl.ds(pl.multiple_of((v >> 3) << 3, 8), 8), :], buf.at[i], sem).start()
        lpos[i] = m * t + ((q ^ r) & 1) * h + ((q ^ r) >> 1) * tl + (j & (tl - 1))
        lrow[i] = v
        return c

    lax.fori_loop(0, n, start, 0)
    zero_start(z, de_ref, *FILL[2], zsem)
    for a in range(8):
        lpos[n + a] = k * t
        lrow[n + a] = 0
    xf[...] = jnp.zeros_like(xf)

    def wait(i, c):
        pltpu.make_async_copy(emb_ref.at[pl.ds(0, 8), :], buf.at[0], sem).wait()
        return c

    lax.fori_loop(0, n, wait, 0)

    def take(g, c):
        for a in range(8):
            tmp[a] = buf[g * 8 + a].astype(F32)
        for a in range(8):
            i = g * 8 + a
            xf[pl.ds(lpos[i], 1), :] = tmp[a, pl.ds(lrow[i] & 7, 1), :]
        return c

    lax.fori_loop(0, (n + 7) // 8, take, 0)
    for a, ref in enumerate((k0, s0, k1, s1)):
        ref[...] = xf[a * h:(a + 1) * h, :].astype(BF16)
    zero_wait(z, de_ref, FILL[1][0], FILL[2][1], zsem)


def sum_kernel(k0, y0, k1, y1, a0, t0, a1, t1):
    tl = a0.shape[0]
    for x, y, a, t in ((k0, y0, a0, t0), (k1, y1, a1, t1)):
        a[...] = x[0:tl, :] + y[0:tl, :]
        t[...] = x[tl:2 * tl, :] + y[tl:2 * tl, :]


def chip_mask(ids_ref, m, q, tl, chip_rows):
    t = ids_ref.shape[1]
    row = lax.broadcasted_iota(jnp.int32, (tl, t), 0) + q * tl
    lane = lax.broadcasted_iota(jnp.int32, (tl, t), 1)
    ids = jnp.broadcast_to(ids_ref[m:m + 1, :].astype(F32), (tl, t))
    col = jnp.sum(jnp.where(row == lane, ids, 0.0), axis=1, keepdims=True)
    lo = ((lax.axis_index("tp") >> 1) * chip_rows).astype(F32)
    return jnp.logical_and(col >= lo, col < lo + chip_rows)


def dx_kernel(m, chip_rows, xh_ref, z_ref, p0, p1, p2, p3, r0, r1, r2, r3, dres_ref, g_ref, ids_ref, tok_ref, *refs):
    if m == 1:
        x0_ref, dg0_ref, x_ref, dx_ref, slot_ref, dg_ref, xs_ref = refs
    else:
        x_ref, dx_ref, slot_ref, dg_ref = refs
    tl = dx_ref.shape[0]
    xh = xh_ref[...].astype(F32)
    x = xh + z_ref[...].astype(F32)
    x_ref[...] = x.astype(BF16)
    if m == 1:
        xs_ref[0] = x0_ref[...]
        xs_ref[1] = x.astype(BF16)
    g = g_ref[...].astype(F32)
    rs = lax.rsqrt(jnp.mean(x * x, axis=-1, keepdims=True) + EPS)
    nh = x * rs
    s = slice(m * tl, (m + 1) * tl)
    dn = jnp.concatenate([
        (a[s, :].astype(F32) + b[s, :].astype(F32)) + (c[s, :].astype(F32) + e[s, :].astype(F32))
        for a, b, c, e in ((p0, p1, p2, p3), (r0, r1, r2, r3))], axis=1)
    gdn = g * dn
    mean = jnp.mean(nh * gdn, axis=-1, keepdims=True)
    dxn = rs * (gdn - nh * mean)
    dx = (dres_ref[m].astype(F32) + dxn).astype(BF16)
    dx_ref[...] = dx
    own = chip_mask(ids_ref, m, lax.axis_index("tp"), tl, chip_rows)
    slot_ref[...] = jnp.where(own, xh, dx.astype(F32)).astype(BF16)
    dg = jnp.sum(dn * nh, axis=0, keepdims=True)
    dg_ref[...] = dg if m == 0 else dg + dg0_ref[...]


def norm(x, g_ref):
    rs = lax.rsqrt(jnp.mean(x * x, axis=-1, keepdims=True) + EPS)
    return ((x * rs) * g_ref[...].astype(F32)).astype(BF16)


def umat(n, w_ref, ub, u_ref, q0, q1, sem):
    blk = 256
    for i in range(ub.shape[1] // blk):
        ub[:, i * blk:(i + 1) * blk] = jnp.dot(n, w_ref[:, i * blk:(i + 1) * blk], preferred_element_type=F32).astype(BF16)
    k = u_ref.shape[0]
    tl = u_ref.shape[1] // 4
    copies = []
    for m in range(k):
        for a, q in enumerate((q0, q1)):
            c = pltpu.make_async_copy(ub.at[pl.ds((m * 2 + a) * tl, tl), :],
                                      u_ref.at[m, pl.ds(pl.multiple_of(q * tl, tl), tl), :], sem)
            c.start()
            copies.append(c)
    return copies


def u_kernel(x0, y0, x1, y1, g_ref, w_ref, tok_ref, de_in, u_ref, n_ref, flag_ref, de_ref, ub, z, usem, zsem):
    flag_ref[0] = 0
    z[...] = jnp.zeros_like(z)
    zero_start(z, de_ref, *FILL[5], zsem)
    r = lax.axis_index("tp")
    tl = x0.shape[0]
    for a, x in enumerate((x0, y0, x1, y1)):
        n_ref[a * tl:(a + 1) * tl, :] = norm(x[...].astype(F32), g_ref)
    for c in umat(n_ref[...], w_ref, ub, u_ref, r, r ^ 1, usem):
        c.wait()
    zero_wait(z, de_ref, *FILL[5], zsem)


def last_kernel(chip_rows, last_ref, dup_ref, cnt_ref, d0, c0, a0, b0, d1, c1, a1, b1, t0, w0, t1, w1, n0_ref, ids_ref, g_ref,
                w_ref, du_ref, u_in, de_in, u_ref, dw_ref, de_ref, xf, n_ref, du2, ub, dwb, usem, wsem, sem):
    t = du_ref.shape[1]
    d, _ = w_ref.shape
    tl = d0.shape[0]
    r = lax.axis_index("tp")
    for a, ref in enumerate((d0, c0, a0, b0, d1, c1, a1, b1)):
        xf[a * tl:(a + 1) * tl, :] = ref[...].astype(F32)

    def add(i, c):
        a = dup_ref[0, i]
        b = dup_ref[1, i]
        xf[pl.ds(b, 1), :] = xf[pl.ds(b, 1), :] + xf[pl.ds(a, 1), :]
        return c

    lax.fori_loop(0, cnt_ref[1], add, 0)

    n_ref[0:t, :] = n0_ref[...]
    for a, (m, q, own, got) in enumerate(((0, r ^ 2, t0, c0), (0, r ^ 3, w0, b0), (1, r ^ 2, t1, c1), (1, r ^ 3, w1, b1))):
        x = jnp.where(chip_mask(ids_ref, m, q, tl, chip_rows), own[...].astype(F32), got[...].astype(F32))
        n_ref[t + a * tl:t + (a + 1) * tl, :] = norm(x, g_ref)

    def put(i, c):
        pltpu.make_async_copy(xf.at[pl.ds(last_ref[0, i], 1), :], de_ref.at[pl.ds(last_ref[1, i], 1), :], sem).start()
        return c

    lax.fori_loop(0, cnt_ref[0], put, 0)
    for a, (m, q) in enumerate(((0, r), (0, r ^ 1), (1, r), (1, r ^ 1), (0, r ^ 2), (0, r ^ 3), (1, r ^ 2), (1, r ^ 3))):
        du2[a * tl:(a + 1) * tl, :] = du_ref[m, pl.ds(pl.multiple_of(q * tl, tl), tl), :]
    copies = umat(n_ref[t:2 * t, :], w_ref, ub, u_ref, r ^ 2, r ^ 3, usem)
    blk = 256
    for i in range(d // blk):
        dwb[i] = lax.dot_general(n_ref[:, i * blk:(i + 1) * blk], du2[...], (((0,), (0,)), ((), ())),
                                 preferred_element_type=F32)
        c = pltpu.make_async_copy(dwb.at[i], dw_ref.at[pl.ds(i * blk, blk), :], wsem)
        c.start()
        copies.append(c)

    def wait(i, c):
        pltpu.make_async_copy(xf.at[pl.ds(0, 1), :], de_ref.at[pl.ds(0, 1), :], sem).wait()
        return c

    lax.fori_loop(0, cnt_ref[0], wait, 0)
    for c in copies:
        c.wait()


def solution(mesh):
    groups = mesh.shape["tp"]
    sib = [(i, i ^ 1) for i in range(groups)]
    cross = [(i, i ^ 2) for i in range(groups)]
    diag = [(i, i ^ 3) for i in range(groups)]

    def local(ids, emb, g, w, du, dres):
        k, t = ids.shape
        vl, d = emb.shape
        fc = w.shape[1]
        tl = t // groups
        n = k * tl
        h = 2 * n
        g2 = g.reshape(1, d)
        S = jax.ShapeDtypeStruct
        D = pltpu.SemaphoreType.DMA

        def perm(v, p):
            return lax.ppermute(v, "tp", p)

        d1 = 7 * 256
        d2 = d - d1
        p2, p3, p1, p0, dup4 = call(
            functools.partial(pdn_kernel, 0, True), 60, [S((n, d1), BF16)] * 4 + [S((4 * n, fc), BF16)],
            [HBM] * 2, [VMEM] * 5, [pltpu.VMEM((k, t, fc), BF16), pltpu.VMEM((d1, fc), BF16), D, D((d1 // 256,))],
            8 * n * fc * d1, 2 * d1 * fc + 8 * n * (fc + d1))(du, w)
        q2 = perm(p2, cross)
        q3 = perm(p3, diag)
        k0, s0, k1, s1, lpos, lrow, nown, de = call(
            gather_kernel, 60,
            [S((n, d), BF16)] * 4 + [S((2 * h + 8,), jnp.int32)] * 2 + [S((8,), jnp.int32), S((vl, d), F32)],
            [SMEM, HBM], [VMEM] * 4 + [SMEM] * 3 + [HBM],
            [pltpu.VMEM((2 * h, 8, d), BF16), pltpu.VMEM((8, 8, d), F32), pltpu.VMEM((2 * h + 8, d), F32), pltpu.VMEM((256, d), F32)]
            + [pltpu.SMEM((2 * h + 8,), jnp.int32), D, D],
            500_000_000, 16 * h * d)(ids, emb)
        y0 = perm(s0, sib)
        y1 = perm(s1, sib)
        r2, r3, r1, r0, de = call(
            functools.partial(pdn_kernel, d1, False), 60, [S((n, d2), BF16)] * 4 + [S((vl, d), F32)],
            [VMEM, HBM, HBM], [VMEM] * 4 + [HBM], [pltpu.VMEM((d2, fc), BF16), pltpu.VMEM((256, d), F32), D((d2 // 256,)), D],
            8 * n * fc * d2, 2 * d2 * fc + 8 * n * (fc + d2), {2: 4})(dup4, w, de)
        v2 = perm(r2, cross)
        v3 = perm(r3, diag)
        q1 = perm(p1, sib)
        v1 = perm(r1, sib)
        own0, oth0, own1, oth1 = call(sum_kernel, 16, [S((tl, d), BF16)] * 4, [VMEM] * 4, [VMEM] * 4, [],
                                      8 * tl * d, 24 * tl * d)(k0, y0, k1, y1)
        z0 = perm(oth0, cross)
        z1 = perm(oth1, cross)
        w0 = perm(oth0, sib)
        w1 = perm(oth1, sib)
        last, dup, cnt, de = call(
            zero_kernel, 8, [S((2, 2 * h + 8), jnp.int32)] * 2 + [S((8,), jnp.int32), S((vl, d), F32)],
            [SMEM] * 3 + [HBM], [SMEM] * 3 + [HBM],
            [pltpu.VMEM((256, d), F32), pltpu.SMEM((2 * h + 8,), jnp.int32), pltpu.SMEM((vl,), jnp.int32), D],
            3_000_000_000, vl * d, {3: 3})(lpos, lrow, nown, de)

        def dxk(m, xh, z, tok, more):
            outs = [S((tl, d), BF16)] * 3 + [S((1, d), F32)] + ([S((k, tl, d), BF16)] if m else [])
            return call(functools.partial(dx_kernel, m, 2 * vl), 16, outs,
                        [VMEM] * 13 + [HBM] + [VMEM] * len(more),
                        [VMEM] * len(outs), [], 30 * n * d, 16 * n * d)(
                            xh, z, p0, q1, q2, q3, r0, v1, v2, v3, dres, g2, ids, tok, *more)

        x0, dx0, slot0, dg0 = dxk(0, own0, z0, de, ())
        c0 = perm(slot0, cross)
        de = call(zero2_kernel, 8, S((vl, d), F32), [VMEM, HBM], HBM, [pltpu.VMEM((256, d), F32), D],
                  2_000_000_000, vl * d, {1: 0})(dg0, de)
        x1, dx1, slot1, dg, x = dxk(1, own1, z1, de, (x0, dg0))
        c1 = perm(slot1, cross)
        xo0 = perm(x0, sib)
        xo1 = perm(x1, sib)
        a0 = perm(dx0, sib)
        a1 = perm(dx1, sib)
        u, nown2, _, de = call(
            u_kernel, 28, [S((k, t, fc), BF16), S((t, d), BF16), S((8,), jnp.int32), S((vl, d), F32)],
            [VMEM] * 7 + [HBM], [HBM, VMEM, SMEM, HBM],
            [pltpu.VMEM((t, fc), BF16), pltpu.VMEM((256, d), F32), D, D], 2 * t * d * fc, 2 * d * fc,
            {7: 3})(x0, xo0, x1, xo1, g2, w, dg, de)
        b0 = perm(c0, sib)
        b1 = perm(c1, sib)
        dgs = dg + perm(dg, sib)
        dgs = dgs + perm(dgs, cross)

        u, dw, de = call(
            functools.partial(last_kernel, 2 * vl), 44, [S((k, t, fc), BF16), S((d, fc), F32), S((vl, d), F32)],
            [SMEM] * 3 + [VMEM] * 17 + [HBM] * 2, [HBM] * 3,
            [pltpu.VMEM((2 * h, d), F32), pltpu.VMEM((k * t, d), BF16), pltpu.VMEM((k * t, fc), BF16), pltpu.VMEM((t, fc), BF16),
             pltpu.VMEM((d // 256, 256, fc), F32), D, D, D],
            3 * k * t * d * fc, 6 * d * fc, {20: 0, 21: 2})(
                last, dup, cnt, dx0, c0, a0, b0, dx1, c1, a1, b1, oth0, w0, oth1, w1, nown2, ids, g2, w, du, u, de)
        return u, x, de, dw, dgs.reshape(d)

    return jax.shard_map(
        local,
        mesh=mesh,
        in_specs=(P("dp", None), P("tp", None), P(None), P(None, "tp"), P("dp", None, "tp"), P("dp", "tp", None)),
        out_specs=(P("dp", None, "tp"), P("dp", "tp", None), P(("dp", "tp"), None), P(None, ("dp", "tp")), P("dp")),
        check_vma=False,
    )
```

```python
import functools

import jax
import jax.numpy as jnp
from jax import lax
from jax.experimental import pallas as pl
from jax.experimental.pallas import tpu as pltpu
from jax.sharding import PartitionSpec as P


EPS = 1e-6
F32 = jnp.float32
BF16 = jnp.bfloat16
HBM = pl.BlockSpec(memory_space=pltpu.HBM)
VMEM = pl.BlockSpec(memory_space=pltpu.VMEM)
SMEM = pl.BlockSpec(memory_space=pltpu.SMEM)


def call(body, mib, outs, ins, out_specs, scratch, flops, nbytes, aliases=None):
    return pl.pallas_call(
        body,
        out_shape=outs,
        in_specs=ins,
        out_specs=out_specs,
        scratch_shapes=scratch,
        input_output_aliases=aliases or {},
        cost_estimate=pl.CostEstimate(flops=flops, bytes_accessed=nbytes, transcendentals=0),
        compiler_params=pltpu.CompilerParams(vmem_limit_bytes=mib << 20),
    )


def pdn_kernel(du_ref, w_ref, *refs):
    outs = refs[:4]
    de_ref, dub, dup, wb, z, dsem, wsem, zsem = refs[4:]
    n, d = outs[0].shape
    k, tl = dub.shape[0], dub.shape[1] // 4
    blk = 256
    nb = d // blk
    dc = pltpu.make_async_copy(du_ref, dub, dsem)
    dc.start()
    for i in range(nb):
        pltpu.make_async_copy(w_ref.at[pl.ds(i * blk, blk), :], wb.at[pl.ds(i * blk, blk), :], wsem.at[i]).start()
    z[...] = jnp.zeros_like(z)
    zero_start(z, de_ref, *FILL[0], zsem)
    r = lax.axis_index("tp")
    dc.wait()
    for a, j in enumerate((2, 3, 1, 0)):
        q = r ^ j
        for m in range(k):
            dup[pl.ds(a * n + m * tl, tl), :] = dub[m, pl.ds(pl.multiple_of(q * tl, tl), tl), :]
    for i in range(nb):
        pltpu.make_async_copy(w_ref.at[pl.ds(i * blk, blk), :], wb.at[pl.ds(i * blk, blk), :], wsem.at[i]).wait()
        p = lax.dot_general(dup[...], wb[i * blk:(i + 1) * blk, :], (((1,), (1,)), ((), ())), preferred_element_type=F32)
        for a in range(4):
            outs[a][:, i * blk:(i + 1) * blk] = p[a * n:(a + 1) * n].astype(BF16)
    zero_wait(z, de_ref, *FILL[0], zsem)


FILL = ((0, 4), (4, 6), (6, 8), (8, 16))


def zero_start(z, de_ref, lo, hi, sem):
    step = z.shape[0]
    per = de_ref.shape[0] // 16
    for i in range((hi - lo) * per // step):
        pltpu.make_async_copy(z, de_ref.at[pl.ds(lo * per + i * step, step), :], sem).start()


def zero_wait(z, de_ref, lo, hi, sem):
    step = z.shape[0]
    for _ in range((hi - lo) * (de_ref.shape[0] // 16) // step):
        pltpu.make_async_copy(z, de_ref.at[pl.ds(0, step), :], sem).wait()


def zero_kernel(own_ref, de_in, list_ref, de_ref, z, lnxt, tab, sem):
    z[...] = jnp.zeros_like(z)
    zero_start(z, de_ref, *FILL[3], sem)
    n = own_ref[0, own_ref.shape[1] - 1]
    t = lnxt.shape[0] - 8

    def link(i, c):
        v = own_ref[1, i]
        p = tab[v]
        ok = jnp.logical_and(p >= 0, p < i)
        p = jnp.where(ok, p, 0)
        ok = jnp.logical_and(ok, own_ref[1, p] == v)
        lnxt[i] = -1
        lnxt[jnp.where(ok, p, t)] = i
        tab[v] = i
        return c

    lax.fori_loop(0, n, link, 0)

    def lists(i, c):
        nl, nd = c
        x = lnxt[i]
        end = (x < 0).astype(jnp.int32)
        pos = own_ref[0, i]
        list_ref[0, nl] = pos
        list_ref[1, nl] = own_ref[1, i]
        list_ref[2, nd] = pos
        list_ref[3, nd] = own_ref[0, jnp.maximum(x, 0)]
        return nl + end, nd + 1 - end

    nl, nd = lax.fori_loop(0, n, lists, (0, 0))
    list_ref[0, list_ref.shape[1] - 1] = nl
    list_ref[2, list_ref.shape[1] - 1] = nd
    zero_wait(z, de_ref, *FILL[3], sem)


def gather_kernel(ids_ref, emb_ref, de_in, k0, s0, k1, s1, own_ref, de_ref, buf, tmp, xf, z, lst, sem, zsem):
    k, t = ids_ref.shape
    vl = emb_ref.shape[0]
    h = k0.shape[0]
    tl = t // 4
    r = lax.axis_index("tp")
    z[...] = jnp.zeros_like(z)
    zero_start(z, de_ref, *FILL[1], zsem)
    n = 0
    for m in range(k):
        def scan(i, n):
            lst[n] = m * t + i
            return n + (lax.shift_right_logical(ids_ref[m, i], vl.bit_length() - 1) == r).astype(jnp.int32)

        n = lax.fori_loop(0, t, scan, n, unroll=16)
    own_ref[0, own_ref.shape[1] - 1] = n

    def start(i, c):
        j = lst[i]
        m = j // t
        v = ids_ref[m, j & (t - 1)] - r * vl
        q = (j & (t - 1)) // tl
        pltpu.make_async_copy(emb_ref.at[pl.ds(pl.multiple_of((v >> 3) << 3, 8), 8), :], buf.at[i], sem).start()
        own_ref[0, i] = m * t + ((q ^ r) & 1) * h + ((q ^ r) >> 1) * tl + (j & (tl - 1))
        own_ref[1, i] = v
        return c

    lax.fori_loop(0, n, start, 0)
    zero_start(z, de_ref, *FILL[2], zsem)
    for a in range(8):
        own_ref[0, n + a] = k * t
        own_ref[1, n + a] = 0
    xf[...] = jnp.zeros_like(xf)

    def wait(i, c):
        pltpu.make_async_copy(emb_ref.at[pl.ds(0, 8), :], buf.at[0], sem).wait()
        return c

    lax.fori_loop(0, n, wait, 0)

    def take(g, c):
        for a in range(8):
            tmp[a] = buf[g * 8 + a].astype(F32)
        for a in range(8):
            i = g * 8 + a
            xf[pl.ds(own_ref[0, i], 1), :] = tmp[a, pl.ds(own_ref[1, i] & 7, 1), :]
        return c

    lax.fori_loop(0, (n + 7) // 8, take, 0)
    for a, ref in enumerate((k0, s0, k1, s1)):
        ref[...] = xf[a * h:(a + 1) * h, :].astype(BF16)
    zero_wait(z, de_ref, FILL[1][0], FILL[2][1], zsem)


def sum_kernel(k0, y0, k1, y1, a0, t0, a1, t1):
    tl = a0.shape[0]
    for x, y, a, t in ((k0, y0, a0, t0), (k1, y1, a1, t1)):
        a[...] = x[0:tl, :] + y[0:tl, :]
        t[...] = x[tl:2 * tl, :] + y[tl:2 * tl, :]


def chip_mask(ids_ref, m, q, tl, chip_rows):
    t = ids_ref.shape[1]
    row = lax.broadcasted_iota(jnp.int32, (tl, t), 0) + q * tl
    lane = lax.broadcasted_iota(jnp.int32, (tl, t), 1)
    ids = jnp.broadcast_to(ids_ref[m:m + 1, :].astype(F32), (tl, t))
    col = jnp.sum(jnp.where(row == lane, ids, 0.0), axis=1, keepdims=True)
    lo = ((lax.axis_index("tp") >> 1) * chip_rows).astype(F32)
    return jnp.logical_and(col >= lo, col < lo + chip_rows)


def dx_kernel(m, chip_rows, xh_ref, z_ref, p0, p1, p2, p3, dres_ref, g_ref, ids_ref, tok_ref, *refs):
    if m == 1:
        x0_ref, dg0_ref, x_ref, dx_ref, slot_ref, dg_ref, xs_ref = refs
    else:
        x_ref, dx_ref, slot_ref, dg_ref = refs
    tl = dx_ref.shape[0]
    xh = xh_ref[...].astype(F32)
    x = xh + z_ref[...].astype(F32)
    x_ref[...] = x.astype(BF16)
    if m == 1:
        xs_ref[0] = x0_ref[...]
        xs_ref[1] = x.astype(BF16)
    g = g_ref[...].astype(F32)
    rs = lax.rsqrt(jnp.mean(x * x, axis=-1, keepdims=True) + EPS)
    nh = x * rs
    s = slice(m * tl, (m + 1) * tl)
    dn = (p0[s, :].astype(F32) + p1[s, :].astype(F32)) + (p2[s, :].astype(F32) + p3[s, :].astype(F32))
    gdn = g * dn
    mean = jnp.mean(nh * gdn, axis=-1, keepdims=True)
    dxn = rs * (gdn - nh * mean)
    dx = (dres_ref[m].astype(F32) + dxn).astype(BF16)
    dx_ref[...] = dx
    own = chip_mask(ids_ref, m, lax.axis_index("tp"), tl, chip_rows)
    slot_ref[...] = jnp.where(own, xh, dx.astype(F32)).astype(BF16)
    dg = jnp.sum(dn * nh, axis=0, keepdims=True)
    dg_ref[...] = dg if m == 0 else dg + dg0_ref[...]


def norm(x, g_ref):
    rs = lax.rsqrt(jnp.mean(x * x, axis=-1, keepdims=True) + EPS)
    return ((x * rs) * g_ref[...].astype(F32)).astype(BF16)


def umat(n, w_ref, ub, u_ref, q0, q1, sem):
    blk = 256
    for i in range(ub.shape[1] // blk):
        ub[:, i * blk:(i + 1) * blk] = jnp.dot(n, w_ref[:, i * blk:(i + 1) * blk], preferred_element_type=F32).astype(BF16)
    k = u_ref.shape[0]
    tl = u_ref.shape[1] // 4
    copies = []
    for m in range(k):
        for a, q in enumerate((q0, q1)):
            c = pltpu.make_async_copy(ub.at[pl.ds((m * 2 + a) * tl, tl), :],
                                      u_ref.at[m, pl.ds(pl.multiple_of(q * tl, tl), tl), :], sem)
            c.start()
            copies.append(c)
    return copies


def take_du(du_ref, out_ref, tl, order):
    for a, (m, q) in enumerate(order):
        out_ref[a * tl:(a + 1) * tl, :] = du_ref[m, pl.ds(pl.multiple_of(q * tl, tl), tl), :]


def dw_tile(n_ref, du2, i, blk):
    return lax.dot_general(n_ref[:, i * blk:(i + 1) * blk], du2[...], (((0,), (0,)), ((), ())), preferred_element_type=F32)


def u_kernel(x0, y0, x1, y1, g_ref, w_ref, du_ref, tok_ref, u_ref, dwp_ref, n_ref, du2, ub, usem):
    r = lax.axis_index("tp")
    tl = x0.shape[0]
    for a, x in enumerate((x0, y0, x1, y1)):
        n_ref[a * tl:(a + 1) * tl, :] = norm(x[...].astype(F32), g_ref)
    take_du(du_ref, du2, tl, ((0, r), (0, r ^ 1), (1, r), (1, r ^ 1)))
    copies = umat(n_ref[...], w_ref, ub, u_ref, r, r ^ 1, usem)
    blk = 256
    for i in range(dwp_ref.shape[0] // blk):
        dwp_ref[i * blk:(i + 1) * blk, :] = dw_tile(n_ref, du2, i, blk)
    for c in copies:
        c.wait()


def last_kernel(chip_rows, list_ref, d0, c0, a0, b0, d1, c1, a1, b1, t0, w0, t1, w1, dwp_ref, ids_ref, g_ref,
                w_ref, du_ref, u_in, de_in, u_ref, dw_ref, de_ref, xf, n_ref, du2, ub, dwb, usem, wsem, sem):
    d = w_ref.shape[0]
    tl = d0.shape[0]
    r = lax.axis_index("tp")
    for a, ref in enumerate((d0, c0, a0, b0, d1, c1, a1, b1)):
        xf[a * tl:(a + 1) * tl, :] = ref[...].astype(F32)

    def add(i, c):
        a = list_ref[2, i]
        b = list_ref[3, i]
        xf[pl.ds(b, 1), :] = xf[pl.ds(b, 1), :] + xf[pl.ds(a, 1), :]
        return c

    lax.fori_loop(0, list_ref[2, list_ref.shape[1] - 1], add, 0)

    for a, (m, q, own, got) in enumerate(((0, r ^ 2, t0, c0), (0, r ^ 3, w0, b0), (1, r ^ 2, t1, c1), (1, r ^ 3, w1, b1))):
        x = jnp.where(chip_mask(ids_ref, m, q, tl, chip_rows), own[...].astype(F32), got[...].astype(F32))
        n_ref[a * tl:(a + 1) * tl, :] = norm(x, g_ref)

    def put(i, c):
        pltpu.make_async_copy(xf.at[pl.ds(list_ref[0, i], 1), :], de_ref.at[pl.ds(list_ref[1, i], 1), :], sem).start()
        return c

    lax.fori_loop(0, list_ref[0, list_ref.shape[1] - 1], put, 0)
    take_du(du_ref, du2, tl, ((0, r ^ 2), (0, r ^ 3), (1, r ^ 2), (1, r ^ 3)))
    copies = umat(n_ref[...], w_ref, ub, u_ref, r ^ 2, r ^ 3, usem)
    blk = 256
    for i in range(d // blk):
        dwb[i] = dwp_ref[i * blk:(i + 1) * blk, :] + dw_tile(n_ref, du2, i, blk)
        c = pltpu.make_async_copy(dwb.at[i], dw_ref.at[pl.ds(i * blk, blk), :], wsem)
        c.start()
        copies.append(c)

    def wait(i, c):
        pltpu.make_async_copy(xf.at[pl.ds(0, 1), :], de_ref.at[pl.ds(0, 1), :], sem).wait()
        return c

    lax.fori_loop(0, list_ref[0, list_ref.shape[1] - 1], wait, 0)
    for c in copies:
        c.wait()


def solution(mesh):
    groups = mesh.shape["tp"]
    sib = [(i, i ^ 1) for i in range(groups)]
    cross = [(i, i ^ 2) for i in range(groups)]
    diag = [(i, i ^ 3) for i in range(groups)]

    def local(ids, emb, g, w, du, dres):
        k, t = ids.shape
        vl, d = emb.shape
        fc = w.shape[1]
        tl = t // groups
        n = k * tl
        h = 2 * n
        g2 = g.reshape(1, d)
        S = jax.ShapeDtypeStruct
        D = pltpu.SemaphoreType.DMA

        def perm(v, p):
            return lax.ppermute(v, "tp", p)

        p2, p3, p1, p0, de = call(
            pdn_kernel, 60, [S((n, d), BF16)] * 4 + [S((vl, d), F32)], [HBM] * 2, [VMEM] * 4 + [HBM],
            [pltpu.VMEM((k, t, fc), BF16), pltpu.VMEM((4 * n, fc), BF16), pltpu.VMEM((d, fc), BF16), pltpu.VMEM((256, d), F32),
             D, D((d // 256,)), D], 8 * n * fc * d, 2 * d * fc + 8 * n * (fc + d))(du, w)
        q2 = perm(p2, cross)
        q3 = perm(p3, diag)
        k0, s0, k1, s1, owned, de = call(
            gather_kernel, 60,
            [S((n, d), BF16)] * 4 + [S((2, 2 * h + 16), jnp.int32), S((vl, d), F32)],
            [SMEM, HBM, HBM], [VMEM] * 4 + [SMEM, HBM],
            [pltpu.VMEM((2 * h, 8, d), BF16), pltpu.VMEM((8, 8, d), F32), pltpu.VMEM((2 * h + 8, d), F32), pltpu.VMEM((256, d), F32)]
            + [pltpu.SMEM((2 * h + 8,), jnp.int32), D, D],
            500_000_000, 16 * h * d, {2: 5})(ids, emb, de)
        y0 = perm(s0, sib)
        y1 = perm(s1, sib)
        q1 = perm(p1, sib)
        own0, oth0, own1, oth1 = call(sum_kernel, 16, [S((tl, d), BF16)] * 4, [VMEM] * 4, [VMEM] * 4, [],
                                      8 * tl * d, 24 * tl * d)(k0, y0, k1, y1)
        z0 = perm(oth0, cross)
        z1 = perm(oth1, cross)
        w0 = perm(oth0, sib)
        w1 = perm(oth1, sib)
        lists, de = call(
            zero_kernel, 8, [S((4, 2 * h + 16), jnp.int32), S((vl, d), F32)], [SMEM, HBM], [SMEM, HBM],
            [pltpu.VMEM((256, d), F32), pltpu.SMEM((2 * h + 8,), jnp.int32), pltpu.SMEM((vl,), jnp.int32), D],
            6_000_000_000, 2 * vl * d, {1: 1})(owned, de)

        def dxk(m, xh, z, tok, more):
            outs = [S((tl, d), BF16)] * 3 + [S((1, d), F32)] + ([S((k, tl, d), BF16)] if m else [])
            return call(functools.partial(dx_kernel, m, 2 * vl), 16, outs,
                        [VMEM] * 9 + [SMEM if m else HBM] + [VMEM] * len(more),
                        [VMEM] * len(outs), [], 30 * n * d, 16 * n * d)(
                            xh, z, p0, q1, q2, q3, dres, g2, ids, tok, *more)

        x0, dx0, slot0, dg0 = dxk(0, own0, z0, de, ())
        c0 = perm(slot0, cross)
        x1, dx1, slot1, dg, x = dxk(1, own1, z1, lists, (x0, dg0))
        c1 = perm(slot1, cross)
        xo0 = perm(x0, sib)
        xo1 = perm(x1, sib)
        a0 = perm(dx0, sib)
        a1 = perm(dx1, sib)
        u, dwp = call(
            u_kernel, 32, [S((k, t, fc), BF16), S((d, fc), F32)], [VMEM] * 8, [HBM, VMEM],
            [pltpu.VMEM((t, d), BF16), pltpu.VMEM((t, fc), BF16), pltpu.VMEM((t, fc), BF16), D],
            4 * t * d * fc, 2 * d * fc)(x0, xo0, x1, xo1, g2, w, du, dg)
        b0 = perm(c0, sib)
        b1 = perm(c1, sib)
        dgs = dg + perm(dg, sib)
        dgs = dgs + perm(dgs, cross)

        u, dw, de = call(
            functools.partial(last_kernel, 2 * vl), 36, [S((k, t, fc), BF16), S((d, fc), F32), S((vl, d), F32)],
            [SMEM] + [VMEM] * 17 + [HBM] * 2, [HBM] * 3,
            [pltpu.VMEM((2 * h, d), F32), pltpu.VMEM((t, d), BF16), pltpu.VMEM((t, fc), BF16), pltpu.VMEM((t, fc), BF16),
             pltpu.VMEM((d // 256, 256, fc), F32), D, D, D],
            4 * t * d * fc, 6 * d * fc, {18: 0, 19: 2})(
                lists, dx0, c0, a0, b0, dx1, c1, a1, b1, oth0, w0, oth1, w1, dwp, ids, g2, w, du, u, de)
        return u, x, de, dw, dgs.reshape(d)

    return jax.shard_map(
        local,
        mesh=mesh,
        in_specs=(P("dp", None), P("tp", None), P(None), P(None, "tp"), P("dp", None, "tp"), P("dp", "tp", None)),
        out_specs=(P("dp", None, "tp"), P("dp", "tp", None), P(("dp", "tp"), None), P(None, ("dp", "tp")), P("dp")),
        check_vma=False,
    )
```

```python
import functools

import jax
import jax.numpy as jnp
from jax import lax
from jax.experimental import pallas as pl
from jax.experimental.pallas import tpu as pltpu
from jax.sharding import PartitionSpec as P


EPS = 1e-6
F32 = jnp.float32
BF16 = jnp.bfloat16
HBM = pl.BlockSpec(memory_space=pltpu.HBM)
VMEM = pl.BlockSpec(memory_space=pltpu.VMEM)
SMEM = pl.BlockSpec(memory_space=pltpu.SMEM)


def call(body, mib, outs, ins, out_specs, scratch, flops, nbytes, aliases=None):
    return pl.pallas_call(
        body,
        out_shape=outs,
        in_specs=ins,
        out_specs=out_specs,
        scratch_shapes=scratch,
        input_output_aliases=aliases or {},
        cost_estimate=pl.CostEstimate(flops=flops, bytes_accessed=nbytes, transcendentals=0),
        compiler_params=pltpu.CompilerParams(vmem_limit_bytes=mib << 20),
    )


def pdn_kernel(du_ref, w_ref, *refs):
    outs = refs[:4]
    dub, dup, wb, ob, dsem, wsem, osem = refs[4:]
    n, d = outs[0].shape
    k, tl = dub.shape[0], dub.shape[1] // 4
    blk = 256
    nb = d // blk
    dc = pltpu.make_async_copy(du_ref, dub, dsem)
    dc.start()
    for i in range(nb):
        pltpu.make_async_copy(w_ref.at[pl.ds(i * blk, blk), :], wb.at[pl.ds(i * blk, blk), :], wsem.at[i]).start()
    r = lax.axis_index("tp")
    dc.wait()
    for a, j in enumerate((2, 3, 1, 0)):
        q = r ^ j
        for m in range(k):
            dup[pl.ds(a * n + m * tl, tl), :] = dub[m, pl.ds(pl.multiple_of(q * tl, tl), tl), :]
    copies = []
    for i in range(nb):
        cols = pl.ds(i * blk, blk)
        pltpu.make_async_copy(w_ref.at[cols, :], wb.at[cols, :], wsem.at[i]).wait()
        p = lax.dot_general(dup[...], wb[i * blk:(i + 1) * blk, :], (((1,), (1,)), ((), ())), preferred_element_type=F32)
        ob[:, i * blk:(i + 1) * blk] = p.astype(BF16)
        for a in range(4):
            c = pltpu.make_async_copy(ob.at[pl.ds(a * n, n), cols], outs[a].at[:, cols], osem)
            c.start()
            copies.append(c)
    for c in copies:
        c.wait()


FILL = ((0, 3), (3, 6), (6, 16))


def zero_start(z, de_ref, lo, hi, sem):
    step = z.shape[0]
    per = de_ref.shape[0] // 16
    for i in range((hi - lo) * per // step):
        pltpu.make_async_copy(z, de_ref.at[pl.ds(lo * per + i * step, step), :], sem).start()


def zero_wait(z, de_ref, lo, hi, sem):
    step = z.shape[0]
    for _ in range((hi - lo) * (de_ref.shape[0] // 16) // step):
        pltpu.make_async_copy(z, de_ref.at[pl.ds(0, step), :], sem).wait()


def zero_kernel(own_ref, de_in, list_ref, de_ref, z, lnxt, tab, sem):
    z[...] = jnp.zeros_like(z)
    zero_start(z, de_ref, *FILL[2], sem)
    n = own_ref[0, own_ref.shape[1] - 1]
    t = lnxt.shape[0] - 8

    def link(i, c):
        v = own_ref[1, i]
        p = tab[v]
        ok = jnp.logical_and(p >= 0, p < i)
        p = jnp.where(ok, p, 0)
        ok = jnp.logical_and(ok, own_ref[1, p] == v)
        lnxt[i] = -1
        lnxt[jnp.where(ok, p, t)] = i
        tab[v] = i
        return c

    lax.fori_loop(0, n, link, 0)

    def lists(i, c):
        nl, nd, nl0, nd0 = c
        x = lnxt[i]
        end = (x < 0).astype(jnp.int32)
        pos = own_ref[0, i]
        list_ref[0, nl] = pos
        list_ref[1, nl] = own_ref[1, i]
        list_ref[2, nd] = pos
        list_ref[3, nd] = own_ref[0, jnp.maximum(x, 0)]
        near = (pos < t // 2).astype(jnp.int32)
        near2 = (list_ref[3, nd] < t // 2).astype(jnp.int32)
        return nl + end, nd + 1 - end, nl0 + end * near, nd0 + (1 - end) * near2

    nl, nd, nl0, nd0 = lax.fori_loop(0, n, lists, (0, 0, 0, 0))
    for a, v in enumerate((nl, nl0, nd, nd0)):
        list_ref[a, list_ref.shape[1] - 1] = v
    zero_wait(z, de_ref, *FILL[2], sem)


def gather_kernel(ids_ref, emb_ref, k0, s0, k1, s1, own_ref, de_ref, buf, tmp, xf, z, lst, sem, zsem):
    k, t = ids_ref.shape
    vl = emb_ref.shape[0]
    h = k0.shape[0]
    tl = t // 4
    r = lax.axis_index("tp")
    z[...] = jnp.zeros_like(z)
    zero_start(z, de_ref, *FILL[0], zsem)
    n = 0
    for c in range(2):
        lo = ((r >> 1) ^ c) * h
        for m in range(k):
            def scan(i, n):
                j = lo + i
                lst[n] = m * t + j
                return n + (lax.shift_right_logical(ids_ref[m, j], vl.bit_length() - 1) == r).astype(jnp.int32)

            n = lax.fori_loop(0, h, scan, n, unroll=16)
    own_ref[0, own_ref.shape[1] - 1] = n

    def start(i, c):
        j = lst[i]
        m = j // t
        v = ids_ref[m, j & (t - 1)] - r * vl
        q = (j & (t - 1)) // tl
        pltpu.make_async_copy(emb_ref.at[pl.ds(pl.multiple_of((v >> 3) << 3, 8), 8), :], buf.at[i], sem).start()
        own_ref[0, i] = ((q ^ r) >> 1) * 2 * h + m * h + ((q ^ r) & 1) * tl + (j & (tl - 1))
        own_ref[1, i] = v
        return c

    lax.fori_loop(0, n, start, 0)
    zero_start(z, de_ref, *FILL[1], zsem)
    for a in range(8):
        own_ref[0, n + a] = k * t
        own_ref[1, n + a] = 0
    xf[...] = jnp.zeros_like(xf)

    def wait(i, c):
        pltpu.make_async_copy(emb_ref.at[pl.ds(0, 8), :], buf.at[0], sem).wait()
        return c

    lax.fori_loop(0, n, wait, 0)

    def take(g, c):
        for a in range(8):
            tmp[a] = buf[g * 8 + a].astype(F32)
        for a in range(8):
            i = g * 8 + a
            xf[pl.ds(own_ref[0, i], 1), :] = tmp[a, pl.ds(own_ref[1, i] & 7, 1), :]
        return c

    lax.fori_loop(0, (n + 7) // 8, take, 0)
    for a, ref in enumerate((k0, s0, k1, s1)):
        for c in range(2):
            ref[c * tl:(c + 1) * tl, :] = xf[c * 2 * h + a * tl:c * 2 * h + (a + 1) * tl, :].astype(BF16)
    zero_wait(z, de_ref, FILL[0][0], FILL[1][1], zsem)


def sum_kernel(k0, y0, k1, y1, a0, t0, a1, t1):
    tl = a0.shape[0]
    for x, y, a, t in ((k0, y0, a0, t0), (k1, y1, a1, t1)):
        a[...] = x[0:tl, :] + y[0:tl, :]
        t[...] = x[tl:2 * tl, :] + y[tl:2 * tl, :]


def chip_mask(ids_ref, m, q, tl, chip_rows):
    t = ids_ref.shape[1]
    row = lax.broadcasted_iota(jnp.int32, (tl, t), 0) + q * tl
    lane = lax.broadcasted_iota(jnp.int32, (tl, t), 1)
    ids = jnp.broadcast_to(ids_ref[m:m + 1, :].astype(F32), (tl, t))
    col = jnp.sum(jnp.where(row == lane, ids, 0.0), axis=1, keepdims=True)
    lo = ((lax.axis_index("tp") >> 1) * chip_rows).astype(F32)
    return jnp.logical_and(col >= lo, col < lo + chip_rows)


def dx_kernel(m, chip_rows, xh_ref, z_ref, p0, p1, p2, p3, dres_ref, g_ref, ids_ref, tok_ref, *refs):
    if m == 1:
        x0_ref, dg0_ref, x_ref, dx_ref, slot_ref, dg_ref, xs_ref = refs
    else:
        x_ref, dx_ref, slot_ref, dg_ref = refs
    tl = dx_ref.shape[0]
    xh = xh_ref[...].astype(F32)
    x = xh + z_ref[...].astype(F32)
    x_ref[...] = x.astype(BF16)
    if m == 1:
        xs_ref[0] = x0_ref[...]
        xs_ref[1] = x.astype(BF16)
    g = g_ref[...].astype(F32)
    rs = lax.rsqrt(jnp.mean(x * x, axis=-1, keepdims=True) + EPS)
    nh = x * rs
    s = slice(m * tl, (m + 1) * tl)
    dn = (p0[s, :].astype(F32) + p1[s, :].astype(F32)) + (p2[s, :].astype(F32) + p3[s, :].astype(F32))
    gdn = g * dn
    mean = jnp.mean(nh * gdn, axis=-1, keepdims=True)
    dxn = rs * (gdn - nh * mean)
    dx = (dres_ref[m].astype(F32) + dxn).astype(BF16)
    dx_ref[...] = dx
    own = chip_mask(ids_ref, m, lax.axis_index("tp"), tl, chip_rows)
    slot_ref[...] = jnp.where(own, xh, dx.astype(F32)).astype(BF16)
    dg = jnp.sum(dn * nh, axis=0, keepdims=True)
    dg_ref[...] = dg if m == 0 else dg + dg0_ref[...]


def norm(x, g_ref):
    rs = lax.rsqrt(jnp.mean(x * x, axis=-1, keepdims=True) + EPS)
    return ((x * rs) * g_ref[...].astype(F32)).astype(BF16)


def umat(n, w_ref, ub, u_ref, q0, q1, sem):
    blk = 256
    for i in range(ub.shape[1] // blk):
        ub[:, i * blk:(i + 1) * blk] = jnp.dot(n, w_ref[:, i * blk:(i + 1) * blk], preferred_element_type=F32).astype(BF16)
    k = u_ref.shape[0]
    tl = u_ref.shape[1] // 4
    copies = []
    for m in range(k):
        for a, q in enumerate((q0, q1)):
            c = pltpu.make_async_copy(ub.at[pl.ds((m * 2 + a) * tl, tl), :],
                                      u_ref.at[m, pl.ds(pl.multiple_of(q * tl, tl), tl), :], sem)
            c.start()
            copies.append(c)
    return copies


def take_du(du_ref, out_ref, tl, order):
    for a, (m, q) in enumerate(order):
        out_ref[a * tl:(a + 1) * tl, :] = du_ref[m, pl.ds(pl.multiple_of(q * tl, tl), tl), :]


def dw_tile(n_ref, du2, i, blk):
    return lax.dot_general(n_ref[:, i * blk:(i + 1) * blk], du2[...], (((0,), (0,)), ((), ())), preferred_element_type=F32)


def u_kernel(x0, y0, x1, y1, g_ref, w_ref, du_ref, tok_ref, u_ref, dwp_ref, n_ref, du2, ub, usem):
    r = lax.axis_index("tp")
    tl = x0.shape[0]
    for a, x in enumerate((x0, y0, x1, y1)):
        n_ref[a * tl:(a + 1) * tl, :] = norm(x[...].astype(F32), g_ref)
    take_du(du_ref, du2, tl, ((0, r), (0, r ^ 1), (1, r), (1, r ^ 1)))
    copies = umat(n_ref[...], w_ref, ub, u_ref, r, r ^ 1, usem)
    blk = 256
    for i in range(dwp_ref.shape[0] // blk):
        dwp_ref[i * blk:(i + 1) * blk, :] = dw_tile(n_ref, du2, i, blk)
    for c in copies:
        c.wait()


def scatter(near, list_ref, xf, de_ref, sem):
    e = list_ref.shape[1] - 1
    split = xf.shape[0] if near else xf.shape[0] // 2

    def add(i, c):
        a = list_ref[2, i]
        b = list_ref[3, i]

        @pl.when((b < split) if near else (b >= split))
        def _():
            xf[pl.ds(b, 1), :] = xf[pl.ds(b, 1), :] + xf[pl.ds(a, 1), :]

        return c

    @pl.when((list_ref[3, e] > 0) if near else (list_ref[2, e] > list_ref[3, e]))
    def _():
        lax.fori_loop(0, list_ref[2, e], add, 0)

    def put(i, c):
        pltpu.make_async_copy(xf.at[pl.ds(list_ref[0, i], 1), :], de_ref.at[pl.ds(list_ref[1, i], 1), :], sem).start()
        return c

    lax.fori_loop(*((0, list_ref[1, e]) if near else (list_ref[1, e], list_ref[0, e])), put, 0)


def scatter_wait(near, list_ref, xf, de_ref, sem):
    e = list_ref.shape[1] - 1

    def wait(i, c):
        pltpu.make_async_copy(xf.at[pl.ds(0, 1), :], de_ref.at[pl.ds(0, 1), :], sem).wait()
        return c

    lax.fori_loop(*((0, list_ref[1, e]) if near else (list_ref[1, e], list_ref[0, e])), wait, 0)


def near_kernel(list_ref, d0, a0, d1, a1, tok_ref, de_in, xn_ref, de_ref, sem):
    tl = d0.shape[0]
    for a, ref in enumerate((d0, a0, d1, a1)):
        xn_ref[a * tl:(a + 1) * tl, :] = ref[...].astype(F32)
    scatter(True, list_ref, xn_ref, de_ref, sem)
    scatter_wait(True, list_ref, xn_ref, de_ref, sem)


def last_kernel(chip_rows, list_ref, xn_ref, c0, b0, c1, b1, t0, w0, t1, w1, dwp_ref, ids_ref, g_ref,
                w_ref, du_ref, u_in, de_in, u_ref, dw_ref, de_ref, xf, n_ref, du2, ub, dwb, usem, wsem, sem):
    d = w_ref.shape[0]
    tl = c0.shape[0]
    r = lax.axis_index("tp")
    h = xn_ref.shape[0]

    @pl.when(list_ref[2, list_ref.shape[1] - 1] > list_ref[3, list_ref.shape[1] - 1])
    def _():
        xf[0:h, :] = xn_ref[...]

    for a, ref in enumerate((c0, b0, c1, b1)):
        xf[h + a * tl:h + (a + 1) * tl, :] = ref[...].astype(F32)
    scatter(False, list_ref, xf, de_ref, sem)
    take_du(du_ref, du2, tl, ((0, r ^ 2), (0, r ^ 3), (1, r ^ 2), (1, r ^ 3)))
    for a, (m, q, own, got) in enumerate(((0, r ^ 2, t0, c0), (0, r ^ 3, w0, b0), (1, r ^ 2, t1, c1), (1, r ^ 3, w1, b1))):
        x = jnp.where(chip_mask(ids_ref, m, q, tl, chip_rows), own[...].astype(F32), got[...].astype(F32))
        n_ref[a * tl:(a + 1) * tl, :] = norm(x, g_ref)
    blk = 256
    copies = []
    for i in range(d // blk):
        dwb[i] = dwp_ref[i * blk:(i + 1) * blk, :] + dw_tile(n_ref, du2, i, blk)
        c = pltpu.make_async_copy(dwb.at[i], dw_ref.at[pl.ds(i * blk, blk), :], wsem)
        c.start()
        copies.append(c)
    copies += umat(n_ref[...], w_ref, ub, u_ref, r ^ 2, r ^ 3, usem)
    scatter_wait(False, list_ref, xf, de_ref, sem)
    for c in copies:
        c.wait()


def solution(mesh):
    groups = mesh.shape["tp"]
    sib = [(i, i ^ 1) for i in range(groups)]
    cross = [(i, i ^ 2) for i in range(groups)]
    diag = [(i, i ^ 3) for i in range(groups)]

    def local(ids, emb, g, w, du, dres):
        k, t = ids.shape
        vl, d = emb.shape
        fc = w.shape[1]
        tl = t // groups
        n = k * tl
        h = 2 * n
        g2 = g.reshape(1, d)
        S = jax.ShapeDtypeStruct
        D = pltpu.SemaphoreType.DMA

        def perm(v, p):
            return lax.ppermute(v, "tp", p)

        p2, p3, p1, p0 = call(
            pdn_kernel, 60, [S((n, d), BF16)] * 4, [HBM] * 2, [HBM] * 4,
            [pltpu.VMEM((k, t, fc), BF16), pltpu.VMEM((4 * n, fc), BF16), pltpu.VMEM((d, fc), BF16), pltpu.VMEM((4 * n, d), BF16),
             D, D((d // 256,)), D], 8 * n * fc * d, 2 * d * fc + 8 * n * (fc + d))(du, w)
        q2 = perm(p2, cross)
        q3 = perm(p3, diag)
        k0, s0, k1, s1, owned, de = call(
            gather_kernel, 36,
            [S((n, d), BF16)] * 4 + [S((2, 2 * h + 16), jnp.int32), S((vl, d), F32)],
            [SMEM, HBM], [VMEM] * 4 + [SMEM, HBM],
            [pltpu.VMEM((2 * h, 8, d), BF16), pltpu.VMEM((8, 8, d), F32), pltpu.VMEM((2 * h + 8, d), F32), pltpu.VMEM((256, d), F32)]
            + [pltpu.SMEM((2 * h + 8,), jnp.int32), D, D],
            500_000_000, 16 * h * d)(ids, emb)
        y0 = perm(s0, sib)
        y1 = perm(s1, sib)
        q1 = perm(p1, sib)
        own0, oth0, own1, oth1 = call(sum_kernel, 16, [S((tl, d), BF16)] * 4, [VMEM] * 4, [VMEM] * 4, [],
                                      8 * tl * d, 24 * tl * d)(k0, y0, k1, y1)
        z0 = perm(oth0, cross)
        z1 = perm(oth1, cross)
        w0 = perm(oth0, sib)
        w1 = perm(oth1, sib)
        lists, de = call(
            zero_kernel, 8, [S((4, 2 * h + 16), jnp.int32), S((vl, d), F32)], [SMEM, HBM], [SMEM, HBM],
            [pltpu.VMEM((256, d), F32), pltpu.SMEM((2 * h + 8,), jnp.int32), pltpu.SMEM((vl,), jnp.int32), D],
            6_000_000_000, 2 * vl * d, {1: 1})(owned, de)

        def dxk(m, xh, z, tok, more):
            outs = [S((tl, d), BF16)] * 3 + [S((1, d), F32)] + ([S((k, tl, d), BF16)] if m else [])
            return call(functools.partial(dx_kernel, m, 2 * vl), 16, outs,
                        [VMEM] * 9 + [SMEM if m else HBM] + [VMEM] * len(more),
                        [VMEM] * len(outs), [], 30 * n * d, 16 * n * d)(
                            xh, z, p0, q1, q2, q3, dres, g2, ids, tok, *more)

        x0, dx0, slot0, dg0 = dxk(0, own0, z0, de, ())
        c0 = perm(slot0, cross)
        x1, dx1, slot1, dg, x = dxk(1, own1, z1, lists, (x0, dg0))
        c1 = perm(slot1, cross)
        xo0 = perm(x0, sib)
        xo1 = perm(x1, sib)
        a0 = perm(dx0, sib)
        a1 = perm(dx1, sib)
        u, dwp = call(
            u_kernel, 32, [S((k, t, fc), BF16), S((d, fc), F32)], [VMEM] * 8, [HBM, VMEM],
            [pltpu.VMEM((t, d), BF16), pltpu.VMEM((t, fc), BF16), pltpu.VMEM((t, fc), BF16), D],
            4 * t * d * fc, 2 * d * fc)(x0, xo0, x1, xo1, g2, w, du, dg)
        xn, de = call(near_kernel, 12, [S((t, d), F32), S((vl, d), F32)], [SMEM] + [VMEM] * 5 + [HBM], [VMEM, HBM],
                      [D], 8 * h * d, 8 * h * d, {6: 1})(lists, dx0, a0, dx1, a1, dg, de)
        b0 = perm(c0, sib)
        b1 = perm(c1, sib)
        dgs = dg + perm(dg, sib)
        dgs = dgs + perm(dgs, cross)

        u, dw, de = call(
            functools.partial(last_kernel, 2 * vl), 36, [S((k, t, fc), BF16), S((d, fc), F32), S((vl, d), F32)],
            [SMEM] + [VMEM] * 14 + [HBM] * 2, [HBM] * 3,
            [pltpu.VMEM((2 * h, d), F32), pltpu.VMEM((t, d), BF16), pltpu.VMEM((t, fc), BF16), pltpu.VMEM((t, fc), BF16),
             pltpu.VMEM((d // 256, 256, fc), F32), D, D, D],
            4 * t * d * fc, 6 * d * fc, {15: 0, 16: 2})(
                lists, xn, c0, b0, c1, b1, oth0, w0, oth1, w1, dwp, ids, g2, w, du, u, de)
        return u, x, de, dw, dgs.reshape(d)

    return jax.shard_map(
        local,
        mesh=mesh,
        in_specs=(P("dp", None), P("tp", None), P(None), P(None, "tp"), P("dp", None, "tp"), P("dp", "tp", None)),
        out_specs=(P("dp", None, "tp"), P("dp", "tp", None), P(("dp", "tp"), None), P(None, ("dp", "tp")), P("dp")),
        check_vma=False,
    )
```

```python
import functools

import jax
import jax.numpy as jnp
from jax import lax
from jax.experimental import pallas as pl
from jax.experimental.pallas import tpu as pltpu
from jax.sharding import PartitionSpec as P


EPS = 1e-6
F32 = jnp.float32
BF16 = jnp.bfloat16
HBM = pl.BlockSpec(memory_space=pltpu.HBM)
VMEM = pl.BlockSpec(memory_space=pltpu.VMEM)
SMEM = pl.BlockSpec(memory_space=pltpu.SMEM)


def call(body, mib, outs, ins, out_specs, scratch, flops, nbytes, aliases=None):
    return pl.pallas_call(
        body,
        out_shape=outs,
        in_specs=ins,
        out_specs=out_specs,
        scratch_shapes=scratch,
        input_output_aliases=aliases or {},
        cost_estimate=pl.CostEstimate(flops=flops, bytes_accessed=nbytes, transcendentals=0),
        compiler_params=pltpu.CompilerParams(vmem_limit_bytes=mib << 20),
    )


def pdn_kernel(du_ref, w_ref, *refs):
    outs = refs[:4]
    dub, dup, wb, ob, dsem, wsem, osem = refs[4:]
    n, d = outs[0].shape
    k, tl = dub.shape[0], dub.shape[1] // 4
    blk = 256
    nb = d // blk
    dc = pltpu.make_async_copy(du_ref, dub, dsem)
    dc.start()
    for i in range(nb):
        pltpu.make_async_copy(w_ref.at[pl.ds(i * blk, blk), :], wb.at[pl.ds(i * blk, blk), :], wsem.at[i]).start()
    r = lax.axis_index("tp")
    dc.wait()
    for a, j in enumerate((2, 3, 1, 0)):
        q = r ^ j
        for m in range(k):
            dup[pl.ds(a * n + m * tl, tl), :] = dub[m, pl.ds(pl.multiple_of(q * tl, tl), tl), :]

    def tile(i, c):
        cols = pl.ds(pl.multiple_of(i * blk, blk), blk)
        pltpu.make_async_copy(w_ref.at[cols, :], wb.at[cols, :], wsem.at[i]).wait()
        p = lax.dot_general(dup[...], wb[cols, :], (((1,), (1,)), ((), ())), preferred_element_type=F32)
        ob[:, cols] = p.astype(BF16)
        for a in range(4):
            pltpu.make_async_copy(ob.at[pl.ds(a * n, n), cols], outs[a].at[:, cols], osem).start()
        return c

    lax.fori_loop(0, nb, tile, 0)
    for a in range(4):
        pltpu.make_async_copy(ob.at[pl.ds(a * n, n), :], outs[a], osem).wait()


FILL = ((0, 3), (3, 6), (6, 16))


def zero_start(z, de_ref, lo, hi, sem):
    step = z.shape[0]
    per = de_ref.shape[0] // 16
    for i in range((hi - lo) * per // step):
        pltpu.make_async_copy(z, de_ref.at[pl.ds(lo * per + i * step, step), :], sem).start()


def zero_wait(z, de_ref, lo, hi, sem):
    step = z.shape[0]
    for _ in range((hi - lo) * (de_ref.shape[0] // 16) // step):
        pltpu.make_async_copy(z, de_ref.at[pl.ds(0, step), :], sem).wait()


def zero_kernel(own_ref, de_in, list_ref, de_ref, z, lnxt, tab, sem):
    z[...] = jnp.zeros_like(z)
    zero_start(z, de_ref, *FILL[2], sem)
    n = own_ref[0, own_ref.shape[1] - 1]
    t = lnxt.shape[0] - 8

    def link(i, c):
        v = own_ref[1, i]
        p = tab[v]
        ok = jnp.logical_and(p >= 0, p < i)
        p = jnp.where(ok, p, 0)
        ok = jnp.logical_and(ok, own_ref[1, p] == v)
        lnxt[i] = -1
        lnxt[jnp.where(ok, p, t)] = i
        tab[v] = i
        return c

    lax.fori_loop(0, n, link, 0)

    def lists(i, c):
        nl, nd, nl0, nd0 = c
        x = lnxt[i]
        end = (x < 0).astype(jnp.int32)
        pos = own_ref[0, i]
        list_ref[0, nl] = pos
        list_ref[1, nl] = own_ref[1, i]
        list_ref[2, nd] = pos
        list_ref[3, nd] = own_ref[0, jnp.maximum(x, 0)]
        near = (pos < t // 2).astype(jnp.int32)
        near2 = (list_ref[3, nd] < t // 2).astype(jnp.int32)
        return nl + end, nd + 1 - end, nl0 + end * near, nd0 + (1 - end) * near2

    nl, nd, nl0, nd0 = lax.fori_loop(0, n, lists, (0, 0, 0, 0))
    for a, v in enumerate((nl, nl0, nd, nd0)):
        list_ref[a, list_ref.shape[1] - 1] = v
    zero_wait(z, de_ref, *FILL[2], sem)


def gather_kernel(ids_ref, emb_ref, k0, s0, k1, s1, own_ref, de_ref, buf, tmp, xf, z, lst, sem, zsem):
    k, t = ids_ref.shape
    vl = emb_ref.shape[0]
    h = k0.shape[0]
    tl = t // 4
    r = lax.axis_index("tp")
    z[...] = jnp.zeros_like(z)
    zero_start(z, de_ref, *FILL[0], zsem)
    n = 0
    for c in range(2):
        lo = ((r >> 1) ^ c) * h
        for m in range(k):
            def scan(i, n):
                j = lo + i
                lst[n] = m * t + j
                return n + (lax.shift_right_logical(ids_ref[m, j], vl.bit_length() - 1) == r).astype(jnp.int32)

            n = lax.fori_loop(0, h, scan, n, unroll=16)
    own_ref[0, own_ref.shape[1] - 1] = n

    def start(i, c):
        j = lst[i]
        m = j // t
        v = ids_ref[m, j & (t - 1)] - r * vl
        q = (j & (t - 1)) // tl
        pltpu.make_async_copy(emb_ref.at[pl.ds(pl.multiple_of((v >> 3) << 3, 8), 8), :], buf.at[i], sem).start()
        own_ref[0, i] = ((q ^ r) >> 1) * 2 * h + m * h + ((q ^ r) & 1) * tl + (j & (tl - 1))
        own_ref[1, i] = v
        return c

    lax.fori_loop(0, n, start, 0)
    zero_start(z, de_ref, *FILL[1], zsem)
    for a in range(8):
        own_ref[0, n + a] = k * t
        own_ref[1, n + a] = 0
    xf[...] = jnp.zeros_like(xf)

    def wait(i, c):
        pltpu.make_async_copy(emb_ref.at[pl.ds(0, 8), :], buf.at[0], sem).wait()
        return c

    lax.fori_loop(0, n, wait, 0)

    def take(g, c):
        for a in range(8):
            tmp[a] = buf[g * 8 + a].astype(F32)
        for a in range(8):
            i = g * 8 + a
            xf[pl.ds(own_ref[0, i], 1), :] = tmp[a, pl.ds(own_ref[1, i] & 7, 1), :]
        return c

    lax.fori_loop(0, (n + 7) // 8, take, 0)
    for a, ref in enumerate((k0, s0, k1, s1)):
        for c in range(2):
            ref[c * tl:(c + 1) * tl, :] = xf[c * 2 * h + a * tl:c * 2 * h + (a + 1) * tl, :].astype(BF16)
    zero_wait(z, de_ref, FILL[0][0], FILL[1][1], zsem)


def sum_kernel(k0, y0, k1, y1, a0, t0, a1, t1):
    tl = a0.shape[0]
    for x, y, a, t in ((k0, y0, a0, t0), (k1, y1, a1, t1)):
        a[...] = x[0:tl, :] + y[0:tl, :]
        t[...] = x[tl:2 * tl, :] + y[tl:2 * tl, :]


def chip_mask(ids_ref, m, q, tl, chip_rows):
    t = ids_ref.shape[1]
    row = lax.broadcasted_iota(jnp.int32, (tl, t), 0) + q * tl
    lane = lax.broadcasted_iota(jnp.int32, (tl, t), 1)
    ids = jnp.broadcast_to(ids_ref[m:m + 1, :].astype(F32), (tl, t))
    col = jnp.sum(jnp.where(row == lane, ids, 0.0), axis=1, keepdims=True)
    lo = ((lax.axis_index("tp") >> 1) * chip_rows).astype(F32)
    return jnp.logical_and(col >= lo, col < lo + chip_rows)


def dx_kernel(m, chip_rows, xh_ref, z_ref, p0, p1, p2, p3, dres_ref, g_ref, ids_ref, tok_ref, *refs):
    if m == 1:
        both0_ref, dg0_ref, both_ref, slot_ref, dg_ref, xs_ref = refs
    else:
        both_ref, slot_ref, dg_ref = refs
    tl = slot_ref.shape[0]
    xh = xh_ref[...].astype(F32)
    x = xh + z_ref[...].astype(F32)
    both_ref[0:tl, :] = x.astype(BF16)
    if m == 1:
        xs_ref[0] = both0_ref[0:tl, :]
        xs_ref[1] = x.astype(BF16)
    g = g_ref[...].astype(F32)
    rs = lax.rsqrt(jnp.mean(x * x, axis=-1, keepdims=True) + EPS)
    nh = x * rs
    s = slice(m * tl, (m + 1) * tl)
    dn = (p0[s, :].astype(F32) + p1[s, :].astype(F32)) + (p2[s, :].astype(F32) + p3[s, :].astype(F32))
    gdn = g * dn
    mean = jnp.mean(nh * gdn, axis=-1, keepdims=True)
    dxn = rs * (gdn - nh * mean)
    dx = (dres_ref[m].astype(F32) + dxn).astype(BF16)
    both_ref[tl:2 * tl, :] = dx
    own = chip_mask(ids_ref, m, lax.axis_index("tp"), tl, chip_rows)
    slot_ref[...] = jnp.where(own, xh, dx.astype(F32)).astype(BF16)
    dg = jnp.sum(dn * nh, axis=0, keepdims=True)
    dg_ref[...] = dg if m == 0 else dg + dg0_ref[...]


def norm(x, g_ref):
    rs = lax.rsqrt(jnp.mean(x * x, axis=-1, keepdims=True) + EPS)
    return ((x * rs) * g_ref[...].astype(F32)).astype(BF16)


def umat(n_ref, w_ref, ub, u_ref, q0, q1, sem):
    blk = 256

    def tile(i, c):
        cols = pl.ds(pl.multiple_of(i * blk, blk), blk)
        ub[:, cols] = jnp.dot(n_ref[...], w_ref[:, cols], preferred_element_type=F32).astype(BF16)
        return c

    lax.fori_loop(0, ub.shape[1] // blk, tile, 0)
    k = u_ref.shape[0]
    tl = u_ref.shape[1] // 4
    copies = []
    for m in range(k):
        for a, q in enumerate((q0, q1)):
            c = pltpu.make_async_copy(ub.at[pl.ds((m * 2 + a) * tl, tl), :],
                                      u_ref.at[m, pl.ds(pl.multiple_of(q * tl, tl), tl), :], sem)
            c.start()
            copies.append(c)
    return copies


def take_du(du_ref, out_ref, tl, order):
    for a, (m, q) in enumerate(order):
        out_ref[a * tl:(a + 1) * tl, :] = du_ref[m, pl.ds(pl.multiple_of(q * tl, tl), tl), :]


def dw_tile(n_ref, du2, i, blk):
    return lax.dot_general(n_ref[:, pl.ds(pl.multiple_of(i * blk, blk), blk)], du2[...], (((0,), (0,)), ((), ())), preferred_element_type=F32)


def u_kernel(x0, y0, x1, y1, g_ref, w_ref, du_ref, tok_ref, u_ref, dwp_ref, n_ref, du2, ub, usem):
    r = lax.axis_index("tp")
    tl = x0.shape[0] // 2
    for a, x in enumerate((x0, y0, x1, y1)):
        n_ref[a * tl:(a + 1) * tl, :] = norm(x[0:tl, :].astype(F32), g_ref)
    take_du(du_ref, du2, tl, ((0, r), (0, r ^ 1), (1, r), (1, r ^ 1)))
    copies = umat(n_ref, w_ref, ub, u_ref, r, r ^ 1, usem)
    blk = 256

    def tile(i, c):
        dwp_ref[pl.ds(pl.multiple_of(i * blk, blk), blk), :] = dw_tile(n_ref, du2, i, blk)
        return c

    lax.fori_loop(0, dwp_ref.shape[0] // blk, tile, 0)
    for c in copies:
        c.wait()


def scatter(near, list_ref, xf, de_ref, sem):
    e = list_ref.shape[1] - 1
    split = xf.shape[0] if near else xf.shape[0] // 2

    def add(i, c):
        a = list_ref[2, i]
        b = list_ref[3, i]

        @pl.when((b < split) if near else (b >= split))
        def _():
            xf[pl.ds(b, 1), :] = xf[pl.ds(b, 1), :] + xf[pl.ds(a, 1), :]

        return c

    @pl.when((list_ref[3, e] > 0) if near else (list_ref[2, e] > list_ref[3, e]))
    def _():
        lax.fori_loop(0, list_ref[2, e], add, 0)

    def put(i, c):
        pltpu.make_async_copy(xf.at[pl.ds(list_ref[0, i], 1), :], de_ref.at[pl.ds(list_ref[1, i], 1), :], sem).start()
        return c

    lax.fori_loop(*((0, list_ref[1, e]) if near else (list_ref[1, e], list_ref[0, e])), put, 0)


def scatter_wait(near, list_ref, xf, de_ref, sem):
    e = list_ref.shape[1] - 1

    def wait(i, c):
        pltpu.make_async_copy(xf.at[pl.ds(0, 1), :], de_ref.at[pl.ds(0, 1), :], sem).wait()
        return c

    lax.fori_loop(*((0, list_ref[1, e]) if near else (list_ref[1, e], list_ref[0, e])), wait, 0)


def near_kernel(list_ref, d0, a0, d1, a1, tok_ref, de_in, xn_ref, de_ref, sem):
    tl = d0.shape[0] // 2
    for a, ref in enumerate((d0, a0, d1, a1)):
        xn_ref[a * tl:(a + 1) * tl, :] = ref[tl:2 * tl, :].astype(F32)
    scatter(True, list_ref, xn_ref, de_ref, sem)
    scatter_wait(True, list_ref, xn_ref, de_ref, sem)


def last_kernel(chip_rows, list_ref, xn_ref, c0, b0, c1, b1, t0, w0, t1, w1, dwp_ref, ids_ref, g_ref,
                w_ref, du_ref, u_in, de_in, u_ref, dw_ref, de_ref, xf, n_ref, du2, ub, dwb, usem, wsem, sem):
    d = w_ref.shape[0]
    tl = c0.shape[0]
    r = lax.axis_index("tp")
    h = xn_ref.shape[0]

    @pl.when(list_ref[2, list_ref.shape[1] - 1] > list_ref[3, list_ref.shape[1] - 1])
    def _():
        xf[0:h, :] = xn_ref[...]

    for a, ref in enumerate((c0, b0, c1, b1)):
        xf[h + a * tl:h + (a + 1) * tl, :] = ref[...].astype(F32)
    scatter(False, list_ref, xf, de_ref, sem)
    take_du(du_ref, du2, tl, ((0, r ^ 2), (0, r ^ 3), (1, r ^ 2), (1, r ^ 3)))
    for a, (m, q, own, got) in enumerate(((0, r ^ 2, t0, c0), (0, r ^ 3, w0, b0), (1, r ^ 2, t1, c1), (1, r ^ 3, w1, b1))):
        x = jnp.where(chip_mask(ids_ref, m, q, tl, chip_rows), own[...].astype(F32), got[...].astype(F32))
        n_ref[a * tl:(a + 1) * tl, :] = norm(x, g_ref)
    blk = 256

    def tile(i, c):
        rows = pl.ds(pl.multiple_of(i * blk, blk), blk)
        dwb[rows, :] = dwp_ref[rows, :] + dw_tile(n_ref, du2, i, blk)
        pltpu.make_async_copy(dwb.at[rows, :], dw_ref.at[rows, :], wsem).start()
        return c

    lax.fori_loop(0, d // blk, tile, 0)
    copies = umat(n_ref, w_ref, ub, u_ref, r ^ 2, r ^ 3, usem)
    scatter_wait(False, list_ref, xf, de_ref, sem)
    pltpu.make_async_copy(dwb, dw_ref, wsem).wait()
    for c in copies:
        c.wait()


def solution(mesh):
    groups = mesh.shape["tp"]
    sib = [(i, i ^ 1) for i in range(groups)]
    cross = [(i, i ^ 2) for i in range(groups)]
    diag = [(i, i ^ 3) for i in range(groups)]

    def local(ids, emb, g, w, du, dres):
        k, t = ids.shape
        vl, d = emb.shape
        fc = w.shape[1]
        tl = t // groups
        n = k * tl
        h = 2 * n
        g2 = g.reshape(1, d)
        S = jax.ShapeDtypeStruct
        D = pltpu.SemaphoreType.DMA

        def perm(v, p):
            return lax.ppermute(v, "tp", p)

        p2, p3, p1, p0 = call(
            pdn_kernel, 60, [S((n, d), BF16)] * 4, [HBM] * 2, [HBM] * 4,
            [pltpu.VMEM((k, t, fc), BF16), pltpu.VMEM((4 * n, fc), BF16), pltpu.VMEM((d, fc), BF16), pltpu.VMEM((4 * n, d), BF16),
             D, D((d // 256,)), D], 8 * n * fc * d, 2 * d * fc + 8 * n * (fc + d))(du, w)
        q2 = perm(p2, cross)
        q3 = perm(p3, diag)
        k0, s0, k1, s1, owned, de = call(
            gather_kernel, 36,
            [S((n, d), BF16)] * 4 + [S((2, 2 * h + 16), jnp.int32), S((vl, d), F32)],
            [SMEM, HBM], [VMEM] * 4 + [SMEM, HBM],
            [pltpu.VMEM((2 * h, 8, d), BF16), pltpu.VMEM((8, 8, d), F32), pltpu.VMEM((2 * h + 8, d), F32), pltpu.VMEM((256, d), F32)]
            + [pltpu.SMEM((2 * h + 8,), jnp.int32), D, D],
            500_000_000, 16 * h * d)(ids, emb)
        y0 = perm(s0, sib)
        y1 = perm(s1, sib)
        q1 = perm(p1, sib)
        own0, oth0, own1, oth1 = call(sum_kernel, 16, [S((tl, d), BF16)] * 4, [VMEM] * 4, [VMEM] * 4, [],
                                      8 * tl * d, 24 * tl * d)(k0, y0, k1, y1)
        z0 = perm(oth0, cross)
        z1 = perm(oth1, cross)
        w0 = perm(oth0, sib)
        w1 = perm(oth1, sib)
        lists, de = call(
            zero_kernel, 8, [S((4, 2 * h + 16), jnp.int32), S((vl, d), F32)], [SMEM, HBM], [SMEM, HBM],
            [pltpu.VMEM((256, d), F32), pltpu.SMEM((2 * h + 8,), jnp.int32), pltpu.SMEM((vl,), jnp.int32), D],
            6_000_000_000, 2 * vl * d, {1: 1})(owned, de)

        def dxk(m, xh, z, tok, more):
            outs = [S((n, d), BF16), S((tl, d), BF16), S((1, d), F32)] + ([S((k, tl, d), BF16)] if m else [])
            return call(functools.partial(dx_kernel, m, 2 * vl), 16, outs,
                        [VMEM] * 9 + [SMEM if m else HBM] + [VMEM] * len(more),
                        [VMEM] * len(outs), [], 30 * n * d, 16 * n * d)(
                            xh, z, p0, q1, q2, q3, dres, g2, ids, tok, *more)

        mine0, slot0, dg0 = dxk(0, own0, z0, de, ())
        c0 = perm(slot0, cross)
        next0 = perm(mine0, sib)
        mine1, slot1, dg, x = dxk(1, own1, z1, lists, (mine0, dg0))
        c1 = perm(slot1, cross)
        next1 = perm(mine1, sib)
        u, dwp = call(
            u_kernel, 32, [S((k, t, fc), BF16), S((d, fc), F32)], [VMEM] * 8, [HBM, VMEM],
            [pltpu.VMEM((t, d), BF16), pltpu.VMEM((t, fc), BF16), pltpu.VMEM((t, fc), BF16), D],
            4 * t * d * fc, 2 * d * fc)(mine0, next0, mine1, next1, g2, w, du, dg)
        xn, de = call(near_kernel, 8, [S((t, d), F32), S((vl, d), F32)], [SMEM] + [VMEM] * 5 + [HBM], [VMEM, HBM],
                      [D], 8 * h * d, 8 * h * d, {6: 1})(lists, mine0, next0, mine1, next1, dg, de)
        b0 = perm(c0, sib)
        b1 = perm(c1, sib)
        dgs = dg + perm(dg, sib)
        dgs = dgs + perm(dgs, cross)

        u, dw, de = call(
            functools.partial(last_kernel, 2 * vl), 20, [S((k, t, fc), BF16), S((d, fc), F32), S((vl, d), F32)],
            [SMEM] + [VMEM] * 14 + [HBM] * 2, [HBM] * 3,
            [pltpu.VMEM((2 * h, d), F32), pltpu.VMEM((t, d), BF16), pltpu.VMEM((t, fc), BF16), pltpu.VMEM((t, fc), BF16),
             pltpu.VMEM((d, fc), F32), D, D, D],
            4 * t * d * fc, 6 * d * fc, {15: 0, 16: 2})(
                lists, xn, c0, b0, c1, b1, oth0, w0, oth1, w1, dwp, ids, g2, w, du, u, de)
        return u, x, de, dw, dgs.reshape(d)

    return jax.shard_map(
        local,
        mesh=mesh,
        in_specs=(P("dp", None), P("tp", None), P(None), P(None, "tp"), P("dp", None, "tp"), P("dp", "tp", None)),
        out_specs=(P("dp", None, "tp"), P("dp", "tp", None), P(("dp", "tp"), None), P(None, ("dp", "tp")), P("dp")),
        check_vma=False,
    )
```

```python
import functools

import jax
import jax.numpy as jnp
from jax import lax
from jax.experimental import pallas as pl
from jax.experimental.pallas import tpu as pltpu
from jax.sharding import PartitionSpec as P


EPS = 1e-6
F32 = jnp.float32
BF16 = jnp.bfloat16
HBM = pl.BlockSpec(memory_space=pltpu.HBM)
VMEM = pl.BlockSpec(memory_space=pltpu.VMEM)
SMEM = pl.BlockSpec(memory_space=pltpu.SMEM)


def call(body, mib, outs, ins, out_specs, scratch, flops, nbytes, aliases=None):
    return pl.pallas_call(
        body,
        out_shape=outs,
        in_specs=ins,
        out_specs=out_specs,
        scratch_shapes=scratch,
        input_output_aliases=aliases or {},
        cost_estimate=pl.CostEstimate(flops=flops, bytes_accessed=nbytes, transcendentals=0),
        compiler_params=pltpu.CompilerParams(vmem_limit_bytes=mib << 20),
    )


def pdn_kernel(du_ref, w_ref, *refs):
    outs = refs[:4]
    dub, dup, wb, ob, dsem, wsem, osem = refs[4:]
    n, d = outs[0].shape
    k, tl = dub.shape[0], dub.shape[1] // 4
    blk = 256
    nb = d // blk
    dc = pltpu.make_async_copy(du_ref, dub, dsem)
    dc.start()
    for i in range(nb):
        pltpu.make_async_copy(w_ref.at[pl.ds(i * blk, blk), :], wb.at[pl.ds(i * blk, blk), :], wsem.at[i]).start()
    r = lax.axis_index("tp")
    dc.wait()
    for a, j in enumerate((2, 3, 1, 0)):
        q = r ^ j
        for m in range(k):
            dup[pl.ds(a * n + m * tl, tl), :] = dub[m, pl.ds(pl.multiple_of(q * tl, tl), tl), :]

    def tile(i, c):
        cols = pl.ds(pl.multiple_of(i * blk, blk), blk)
        pltpu.make_async_copy(w_ref.at[cols, :], wb.at[cols, :], wsem.at[i]).wait()
        p = lax.dot_general(dup[...], wb[cols, :], (((1,), (1,)), ((), ())), preferred_element_type=F32)
        ob[:, cols] = p.astype(BF16)
        for a in range(4):
            pltpu.make_async_copy(ob.at[pl.ds(a * n, n), cols], outs[a].at[:, cols], osem).start()
        return c

    lax.fori_loop(0, nb, tile, 0)
    for a in range(4):
        pltpu.make_async_copy(ob.at[pl.ds(a * n, n), :], outs[a], osem).wait()


FILL = ((0, 3), (3, 6), (6, 16))


def zero_start(z, de_ref, lo, hi, sem):
    step = z.shape[0]
    per = de_ref.shape[0] // 16
    for i in range((hi - lo) * per // step):
        pltpu.make_async_copy(z, de_ref.at[pl.ds(lo * per + i * step, step), :], sem).start()


def zero_wait(z, de_ref, lo, hi, sem):
    step = z.shape[0]
    for _ in range((hi - lo) * (de_ref.shape[0] // 16) // step):
        pltpu.make_async_copy(z, de_ref.at[pl.ds(0, step), :], sem).wait()


def zero_kernel(own_ref, de_in, list_ref, de_ref, z, lnxt, tab, sem):
    z[...] = jnp.zeros_like(z)
    zero_start(z, de_ref, *FILL[2], sem)
    n = own_ref[0, own_ref.shape[1] - 1]
    t = lnxt.shape[0] - 8

    def link(i, c):
        v = own_ref[1, i]
        p = tab[v]
        ok = jnp.logical_and(p >= 0, p < i)
        p = jnp.where(ok, p, 0)
        ok = jnp.logical_and(ok, own_ref[1, p] == v)
        lnxt[i] = -1
        lnxt[jnp.where(ok, p, t)] = i
        tab[v] = i
        return c

    lax.fori_loop(0, n, link, 0)

    def lists(i, c):
        nl, nd, nl0, nd0 = c
        x = lnxt[i]
        end = (x < 0).astype(jnp.int32)
        pos = own_ref[0, i]
        list_ref[0, nl] = pos
        list_ref[1, nl] = own_ref[1, i]
        list_ref[2, nd] = pos
        list_ref[3, nd] = own_ref[0, jnp.maximum(x, 0)]
        near = (pos < t // 2).astype(jnp.int32)
        near2 = (list_ref[3, nd] < t // 2).astype(jnp.int32)
        return nl + end, nd + 1 - end, nl0 + end * near, nd0 + (1 - end) * near2

    nl, nd, nl0, nd0 = lax.fori_loop(0, n, lists, (0, 0, 0, 0))
    for a, v in enumerate((nl, nl0, nd, nd0)):
        list_ref[a, list_ref.shape[1] - 1] = v
    zero_wait(z, de_ref, *FILL[2], sem)


def gather_kernel(ids_ref, emb_ref, k0, s0, k1, s1, own_ref, de_ref, buf, tmp, xf, z, lst, sem, zsem):
    k, t = ids_ref.shape
    vl = emb_ref.shape[0]
    h = k0.shape[0]
    tl = t // 4
    r = lax.axis_index("tp")
    z[...] = jnp.zeros_like(z)
    zero_start(z, de_ref, *FILL[0], zsem)
    n = 0
    for c in range(2):
        lo = ((r >> 1) ^ c) * h
        for m in range(k):
            def scan(i, n):
                j = lo + i
                lst[n] = m * t + j
                return n + (lax.shift_right_logical(ids_ref[m, j], vl.bit_length() - 1) == r).astype(jnp.int32)

            n = lax.fori_loop(0, h, scan, n, unroll=16)
    own_ref[0, own_ref.shape[1] - 1] = n

    def start(i, c):
        j = lst[i]
        m = j // t
        v = ids_ref[m, j & (t - 1)] - r * vl
        q = (j & (t - 1)) // tl
        pltpu.make_async_copy(emb_ref.at[pl.ds(pl.multiple_of((v >> 3) << 3, 8), 8), :], buf.at[i], sem).start()
        own_ref[0, i] = ((q ^ r) >> 1) * 2 * h + m * h + ((q ^ r) & 1) * tl + (j & (tl - 1))
        own_ref[1, i] = v
        return c

    lax.fori_loop(0, n, start, 0)
    zero_start(z, de_ref, *FILL[1], zsem)
    for a in range(8):
        own_ref[0, n + a] = k * t
        own_ref[1, n + a] = 0
    xf[...] = jnp.zeros_like(xf)

    def wait(i, c):
        pltpu.make_async_copy(emb_ref.at[pl.ds(0, 8), :], buf.at[0], sem).wait()
        return c

    lax.fori_loop(0, n, wait, 0)

    def take(g, c):
        for a in range(8):
            tmp[a] = buf[g * 8 + a].astype(F32)
        for a in range(8):
            i = g * 8 + a
            xf[pl.ds(own_ref[0, i], 1), :] = tmp[a, pl.ds(own_ref[1, i] & 7, 1), :]
        return c

    lax.fori_loop(0, (n + 7) // 8, take, 0)
    for a, ref in enumerate((k0, s0, k1, s1)):
        for c in range(2):
            ref[c * tl:(c + 1) * tl, :] = xf[c * 2 * h + a * tl:c * 2 * h + (a + 1) * tl, :].astype(BF16)
    zero_wait(z, de_ref, FILL[0][0], FILL[1][1], zsem)


def sum_kernel(k0, y0, k1, y1, a0, t0, a1, t1):
    tl = a0.shape[0]
    for x, y, a, t in ((k0, y0, a0, t0), (k1, y1, a1, t1)):
        a[...] = x[0:tl, :] + y[0:tl, :]
        t[...] = x[tl:2 * tl, :] + y[tl:2 * tl, :]


def chip_mask(ids_ref, m, q, tl, chip_rows):
    t = ids_ref.shape[1]
    row = lax.broadcasted_iota(jnp.int32, (tl, t), 0) + q * tl
    lane = lax.broadcasted_iota(jnp.int32, (tl, t), 1)
    ids = jnp.broadcast_to(ids_ref[m:m + 1, :].astype(F32), (tl, t))
    col = jnp.sum(jnp.where(row == lane, ids, 0.0), axis=1, keepdims=True)
    lo = ((lax.axis_index("tp") >> 1) * chip_rows).astype(F32)
    return jnp.logical_and(col >= lo, col < lo + chip_rows)


def dx_kernel(m, chip_rows, xh_ref, z_ref, p0, p1, p2, p3, dres_ref, g_ref, ids_ref, tok_ref, *refs):
    if m == 1:
        both0_ref, dg0_ref, both_ref, slot_ref, dg_ref, xs_ref = refs
    else:
        both_ref, slot_ref, dg_ref = refs
    tl = slot_ref.shape[0]
    xh = xh_ref[...].astype(F32)
    x = xh + z_ref[...].astype(F32)
    both_ref[0:tl, :] = x.astype(BF16)
    if m == 1:
        xs_ref[0] = both0_ref[0:tl, :]
        xs_ref[1] = x.astype(BF16)
    g = g_ref[...].astype(F32)
    rs = lax.rsqrt(jnp.mean(x * x, axis=-1, keepdims=True) + EPS)
    nh = x * rs
    s = slice(m * tl, (m + 1) * tl)
    dn = (p0[s, :].astype(F32) + p1[s, :].astype(F32)) + (p2[s, :].astype(F32) + p3[s, :].astype(F32))
    gdn = g * dn
    mean = jnp.mean(nh * gdn, axis=-1, keepdims=True)
    dxn = rs * (gdn - nh * mean)
    dx = (dres_ref[m].astype(F32) + dxn).astype(BF16)
    both_ref[tl:2 * tl, :] = dx
    own = chip_mask(ids_ref, m, lax.axis_index("tp"), tl, chip_rows)
    slot_ref[...] = jnp.where(own, xh, dx.astype(F32)).astype(BF16)
    dg = jnp.sum(dn * nh, axis=0, keepdims=True)
    dg_ref[...] = dg if m == 0 else dg + dg0_ref[...]


def norm(x, g_ref):
    rs = lax.rsqrt(jnp.mean(x * x, axis=-1, keepdims=True) + EPS)
    return ((x * rs) * g_ref[...].astype(F32)).astype(BF16)


def umat(n_ref, w_ref, ub, u_ref, q0, q1, sem):
    blk = 256
    for i in range(ub.shape[1] // blk):
        ub[:, i * blk:(i + 1) * blk] = jnp.dot(
            n_ref[...], w_ref[:, i * blk:(i + 1) * blk], preferred_element_type=F32).astype(BF16)
    k = u_ref.shape[0]
    tl = u_ref.shape[1] // 4
    copies = []
    for m in range(k):
        for a, q in enumerate((q0, q1)):
            c = pltpu.make_async_copy(ub.at[pl.ds((m * 2 + a) * tl, tl), :],
                                      u_ref.at[m, pl.ds(pl.multiple_of(q * tl, tl), tl), :], sem)
            c.start()
            copies.append(c)
    return copies


def take_du(du_ref, out_ref, tl, order):
    for a, (m, q) in enumerate(order):
        out_ref[a * tl:(a + 1) * tl, :] = du_ref[m, pl.ds(pl.multiple_of(q * tl, tl), tl), :]


def dw_tile(n_ref, du2, i, blk):
    return lax.dot_general(n_ref[:, i * blk:(i + 1) * blk], du2[...], (((0,), (0,)), ((), ())), preferred_element_type=F32)


def u_kernel(x0, y0, x1, y1, g_ref, w_ref, du_ref, tok_ref, u_ref, dwp_ref, n_ref, du2, ub, usem):
    r = lax.axis_index("tp")
    tl = x0.shape[0] // 2
    for a, x in enumerate((x0, y0, x1, y1)):
        n_ref[a * tl:(a + 1) * tl, :] = norm(x[0:tl, :].astype(F32), g_ref)
    take_du(du_ref, du2, tl, ((0, r), (0, r ^ 1), (1, r), (1, r ^ 1)))
    copies = umat(n_ref, w_ref, ub, u_ref, r, r ^ 1, usem)
    blk = 256
    for i in range(dwp_ref.shape[0] // blk):
        dwp_ref[i * blk:(i + 1) * blk, :] = dw_tile(n_ref, du2, i, blk)
    for c in copies:
        c.wait()


def scatter(near, list_ref, xf, de_ref, sem):
    e = list_ref.shape[1] - 1
    split = xf.shape[0] if near else xf.shape[0] // 2

    def add(i, c):
        a = list_ref[2, i]
        b = list_ref[3, i]

        @pl.when((b < split) if near else (b >= split))
        def _():
            xf[pl.ds(b, 1), :] = xf[pl.ds(b, 1), :] + xf[pl.ds(a, 1), :]

        return c

    @pl.when((list_ref[3, e] > 0) if near else (list_ref[2, e] > list_ref[3, e]))
    def _():
        lax.fori_loop(0, list_ref[2, e], add, 0)

    def put(i, c):
        pltpu.make_async_copy(xf.at[pl.ds(list_ref[0, i], 1), :], de_ref.at[pl.ds(list_ref[1, i], 1), :], sem).start()
        return c

    lax.fori_loop(*((0, list_ref[1, e]) if near else (list_ref[1, e], list_ref[0, e])), put, 0)


def scatter_wait(near, list_ref, xf, de_ref, sem):
    e = list_ref.shape[1] - 1

    def wait(i, c):
        pltpu.make_async_copy(xf.at[pl.ds(0, 1), :], de_ref.at[pl.ds(0, 1), :], sem).wait()
        return c

    lax.fori_loop(*((0, list_ref[1, e]) if near else (list_ref[1, e], list_ref[0, e])), wait, 0)


def near_kernel(list_ref, d0, a0, d1, a1, tok_ref, de_in, xn_ref, de_ref, sem):
    tl = d0.shape[0] // 2
    for a, ref in enumerate((d0, a0, d1, a1)):
        xn_ref[a * tl:(a + 1) * tl, :] = ref[tl:2 * tl, :].astype(F32)
    scatter(True, list_ref, xn_ref, de_ref, sem)
    scatter_wait(True, list_ref, xn_ref, de_ref, sem)


def last_kernel(chip_rows, list_ref, xn_ref, c0, b0, c1, b1, t0, w0, t1, w1, dwp_ref, ids_ref, g_ref,
                w_ref, du_ref, u_in, de_in, u_ref, dw_ref, de_ref, xf, n_ref, du2, ub, dwb, usem, wsem, sem):
    d = w_ref.shape[0]
    tl = c0.shape[0]
    r = lax.axis_index("tp")
    h = xn_ref.shape[0]

    @pl.when(list_ref[2, list_ref.shape[1] - 1] > list_ref[3, list_ref.shape[1] - 1])
    def _():
        xf[0:h, :] = xn_ref[...]

    for a, ref in enumerate((c0, b0, c1, b1)):
        xf[h + a * tl:h + (a + 1) * tl, :] = ref[...].astype(F32)
    scatter(False, list_ref, xf, de_ref, sem)
    take_du(du_ref, du2, tl, ((0, r ^ 2), (0, r ^ 3), (1, r ^ 2), (1, r ^ 3)))
    for a, (m, q, own, got) in enumerate(((0, r ^ 2, t0, c0), (0, r ^ 3, w0, b0), (1, r ^ 2, t1, c1), (1, r ^ 3, w1, b1))):
        x = jnp.where(chip_mask(ids_ref, m, q, tl, chip_rows), own[...].astype(F32), got[...].astype(F32))
        n_ref[a * tl:(a + 1) * tl, :] = norm(x, g_ref)
    blk = 256
    for i in range(d // blk):
        rows = slice(i * blk, (i + 1) * blk)
        dwb[rows, :] = dwp_ref[rows, :] + dw_tile(n_ref, du2, i, blk)
        pltpu.make_async_copy(dwb.at[pl.ds(i * blk, blk), :], dw_ref.at[pl.ds(i * blk, blk), :], wsem).start()
    copies = umat(n_ref, w_ref, ub, u_ref, r ^ 2, r ^ 3, usem)
    scatter_wait(False, list_ref, xf, de_ref, sem)
    pltpu.make_async_copy(dwb, dw_ref, wsem).wait()
    for c in copies:
        c.wait()


def solution(mesh):
    groups = mesh.shape["tp"]
    sib = [(i, i ^ 1) for i in range(groups)]
    cross = [(i, i ^ 2) for i in range(groups)]
    diag = [(i, i ^ 3) for i in range(groups)]

    def local(ids, emb, g, w, du, dres):
        k, t = ids.shape
        vl, d = emb.shape
        fc = w.shape[1]
        tl = t // groups
        n = k * tl
        h = 2 * n
        g2 = g.reshape(1, d)
        S = jax.ShapeDtypeStruct
        D = pltpu.SemaphoreType.DMA

        def perm(v, p):
            return lax.ppermute(v, "tp", p)

        p2, p3, p1, p0 = call(
            pdn_kernel, 60, [S((n, d), BF16)] * 4, [HBM] * 2, [HBM] * 4,
            [pltpu.VMEM((k, t, fc), BF16), pltpu.VMEM((4 * n, fc), BF16), pltpu.VMEM((d, fc), BF16), pltpu.VMEM((4 * n, d), BF16),
             D, D((d // 256,)), D], 8 * n * fc * d, 2 * d * fc + 8 * n * (fc + d))(du, w)
        q2 = perm(p2, cross)
        q3 = perm(p3, diag)
        k0, s0, k1, s1, owned, de = call(
            gather_kernel, 36,
            [S((n, d), BF16)] * 4 + [S((2, 2 * h + 16), jnp.int32), S((vl, d), F32)],
            [SMEM, HBM], [VMEM] * 4 + [SMEM, HBM],
            [pltpu.VMEM((2 * h, 8, d), BF16), pltpu.VMEM((8, 8, d), F32), pltpu.VMEM((2 * h + 8, d), F32), pltpu.VMEM((256, d), F32)]
            + [pltpu.SMEM((2 * h + 8,), jnp.int32), D, D],
            500_000_000, 16 * h * d)(ids, emb)
        y0 = perm(s0, sib)
        y1 = perm(s1, sib)
        q1 = perm(p1, sib)
        own0, oth0, own1, oth1 = call(sum_kernel, 16, [S((tl, d), BF16)] * 4, [VMEM] * 4, [VMEM] * 4, [],
                                      8 * tl * d, 24 * tl * d)(k0, y0, k1, y1)
        z0 = perm(oth0, cross)
        z1 = perm(oth1, cross)
        w0 = perm(oth0, sib)
        w1 = perm(oth1, sib)
        lists, de = call(
            zero_kernel, 8, [S((4, 2 * h + 16), jnp.int32), S((vl, d), F32)], [SMEM, HBM], [SMEM, HBM],
            [pltpu.VMEM((256, d), F32), pltpu.SMEM((2 * h + 8,), jnp.int32), pltpu.SMEM((vl,), jnp.int32), D],
            6_000_000_000, 2 * vl * d, {1: 1})(owned, de)

        def dxk(m, xh, z, tok, more):
            outs = [S((n, d), BF16), S((tl, d), BF16), S((1, d), F32)] + ([S((k, tl, d), BF16)] if m else [])
            return call(functools.partial(dx_kernel, m, 2 * vl), 16, outs,
                        [VMEM] * 9 + [SMEM if m else HBM] + [VMEM] * len(more),
                        [VMEM] * len(outs), [], 30 * n * d, 16 * n * d)(
                            xh, z, p0, q1, q2, q3, dres, g2, ids, tok, *more)

        mine0, slot0, dg0 = dxk(0, own0, z0, de, ())
        c0 = perm(slot0, cross)
        next0 = perm(mine0, sib)
        mine1, slot1, dg, x = dxk(1, own1, z1, lists, (mine0, dg0))
        c1 = perm(slot1, cross)
        next1 = perm(mine1, sib)
        u, dwp = call(
            u_kernel, 32, [S((k, t, fc), BF16), S((d, fc), F32)], [VMEM] * 8, [HBM, VMEM],
            [pltpu.VMEM((t, d), BF16), pltpu.VMEM((t, fc), BF16), pltpu.VMEM((t, fc), BF16), D],
            4 * t * d * fc, 2 * d * fc)(mine0, next0, mine1, next1, g2, w, du, dg)
        xn, de = call(near_kernel, 8, [S((t, d), F32), S((vl, d), F32)], [SMEM] + [VMEM] * 5 + [HBM], [VMEM, HBM],
                      [D], 8 * h * d, 8 * h * d, {6: 1})(lists, mine0, next0, mine1, next1, dg, de)
        b0 = perm(c0, sib)
        b1 = perm(c1, sib)
        dgs = dg + perm(dg, sib)
        dgs = dgs + perm(dgs, cross)

        u, dw, de = call(
            functools.partial(last_kernel, 2 * vl), 20, [S((k, t, fc), BF16), S((d, fc), F32), S((vl, d), F32)],
            [SMEM] + [VMEM] * 14 + [HBM] * 2, [HBM] * 3,
            [pltpu.VMEM((2 * h, d), F32), pltpu.VMEM((t, d), BF16), pltpu.VMEM((t, fc), BF16), pltpu.VMEM((t, fc), BF16),
             pltpu.VMEM((d, fc), F32), D, D, D],
            4 * t * d * fc, 6 * d * fc, {15: 0, 16: 2})(
                lists, xn, c0, b0, c1, b1, oth0, w0, oth1, w1, dwp, ids, g2, w, du, u, de)
        return u, x, de, dw, dgs.reshape(d)

    return jax.shard_map(
        local,
        mesh=mesh,
        in_specs=(P("dp", None), P("tp", None), P(None), P(None, "tp"), P("dp", None, "tp"), P("dp", "tp", None)),
        out_specs=(P("dp", None, "tp"), P("dp", "tp", None), P(("dp", "tp"), None), P(None, ("dp", "tp")), P("dp")),
        check_vma=False,
    )
```

```python
import functools

import jax
import jax.numpy as jnp
from jax import lax
from jax.experimental import pallas as pl
from jax.experimental.pallas import tpu as pltpu
from jax.sharding import PartitionSpec as P


EPS = 1e-6
F32 = jnp.float32
BF16 = jnp.bfloat16
HBM = pl.BlockSpec(memory_space=pltpu.HBM)
VMEM = pl.BlockSpec(memory_space=pltpu.VMEM)
SMEM = pl.BlockSpec(memory_space=pltpu.SMEM)


def call(body, mib, outs, ins, out_specs, scratch, flops, nbytes, aliases=None):
    return pl.pallas_call(
        body,
        out_shape=outs,
        in_specs=ins,
        out_specs=out_specs,
        scratch_shapes=scratch,
        input_output_aliases=aliases or {},
        cost_estimate=pl.CostEstimate(flops=flops, bytes_accessed=nbytes, transcendentals=0),
        compiler_params=pltpu.CompilerParams(vmem_limit_bytes=mib << 20),
    )


def pdn_kernel(lo, fill, du_ref, w_ref, *refs):
    refs = refs[fill:]
    outs = refs[:4]
    if fill:
        de_ref, z, zsem = refs[4], refs[-2], refs[-1]
    dub, dup, wb, ob, dsem, wsem, osem = refs[5:12]
    n, width = outs[0].shape
    k, tl = dub.shape[0], dub.shape[1] // 4
    blk = 256
    nb = width // blk
    dc = pltpu.make_async_copy(du_ref, dub, dsem)
    dc.start()
    for i in range(nb):
        pltpu.make_async_copy(w_ref.at[pl.ds(lo + i * blk, blk), :], wb.at[pl.ds(i * blk, blk), :], wsem.at[i]).start()
    if fill:
        z[...] = jnp.zeros_like(z)
        zero_start(z, de_ref, *FILL[0], zsem)
    else:
        refs[4][0] = 0
    r = lax.axis_index("tp")
    dc.wait()
    for a, j in enumerate((2, 3, 1, 0)):
        q = r ^ j
        for m in range(k):
            dup[pl.ds(a * n + m * tl, tl), :] = dub[m, pl.ds(pl.multiple_of(q * tl, tl), tl), :]

    def tile(i, c):
        cols = pl.ds(pl.multiple_of(i * blk, blk), blk)
        pltpu.make_async_copy(w_ref.at[cols, :], wb.at[cols, :], wsem.at[i]).wait()
        p = lax.dot_general(dup[...], wb[cols, :], (((1,), (1,)), ((), ())), preferred_element_type=F32)
        ob[:, cols] = p.astype(BF16)
        for a in range(4):
            pltpu.make_async_copy(ob.at[pl.ds(a * n, n), cols], outs[a].at[:, cols], osem).start()
        return c

    lax.fori_loop(0, nb, tile, 0)
    for a in range(4):
        pltpu.make_async_copy(ob.at[pl.ds(a * n, n), :], outs[a], osem).wait()
    if fill:
        zero_wait(z, de_ref, *FILL[0], zsem)


FILL = ((0, 3), (3, 6), (6, 9), (9, 13), (13, 16))


def zero_start(z, de_ref, lo, hi, sem):
    step = z.shape[0]
    per = de_ref.shape[0] // 16
    for i in range((hi - lo) * per // step):
        pltpu.make_async_copy(z, de_ref.at[pl.ds(lo * per + i * step, step), :], sem).start()


def zero_wait(z, de_ref, lo, hi, sem):
    step = z.shape[0]
    for _ in range((hi - lo) * (de_ref.shape[0] // 16) // step):
        pltpu.make_async_copy(z, de_ref.at[pl.ds(0, step), :], sem).wait()


def zero_kernel(own_ref, de_in, list_ref, de_ref, z, lnxt, tab, sem):
    z[...] = jnp.zeros_like(z)
    zero_start(z, de_ref, *FILL[3], sem)
    n = own_ref[0, own_ref.shape[1] - 1]
    t = lnxt.shape[0] - 8

    def link(i, c):
        v = own_ref[1, i]
        p = tab[v]
        ok = jnp.logical_and(p >= 0, p < i)
        p = jnp.where(ok, p, 0)
        ok = jnp.logical_and(ok, own_ref[1, p] == v)
        lnxt[i] = -1
        lnxt[jnp.where(ok, p, t)] = i
        tab[v] = i
        return c

    lax.fori_loop(0, n, link, 0)

    def lists(i, c):
        nl, nd, nl0, nd0 = c
        x = lnxt[i]
        end = (x < 0).astype(jnp.int32)
        pos = own_ref[0, i]
        list_ref[0, nl] = pos
        list_ref[1, nl] = own_ref[1, i]
        list_ref[2, nd] = pos
        list_ref[3, nd] = own_ref[0, jnp.maximum(x, 0)]
        near = (pos < t // 2).astype(jnp.int32)
        near2 = (list_ref[3, nd] < t // 2).astype(jnp.int32)
        return nl + end, nd + 1 - end, nl0 + end * near, nd0 + (1 - end) * near2

    nl, nd, nl0, nd0 = lax.fori_loop(0, n, lists, (0, 0, 0, 0))
    for a, v in enumerate((nl, nl0, nd, nd0)):
        list_ref[a, list_ref.shape[1] - 1] = v
    zero_wait(z, de_ref, *FILL[3], sem)


def zero2_kernel(tok_ref, de_in, de_ref, z, sem):
    z[...] = jnp.zeros_like(z)
    zero_start(z, de_ref, *FILL[4], sem)
    zero_wait(z, de_ref, *FILL[4], sem)


def gather_kernel(ids_ref, emb_ref, de_in, k0, s0, k1, s1, own_ref, de_ref, buf, tmp, xf, z, lst, sem, zsem):
    k, t = ids_ref.shape
    vl = emb_ref.shape[0]
    h = k0.shape[0]
    tl = t // 4
    r = lax.axis_index("tp")
    z[...] = jnp.zeros_like(z)
    zero_start(z, de_ref, *FILL[1], zsem)
    n = 0
    for c in range(2):
        lo = ((r >> 1) ^ c) * h
        for m in range(k):
            def scan(i, n):
                j = lo + i
                lst[n] = m * t + j
                return n + (lax.shift_right_logical(ids_ref[m, j], vl.bit_length() - 1) == r).astype(jnp.int32)

            n = lax.fori_loop(0, h, scan, n, unroll=16)
    own_ref[0, own_ref.shape[1] - 1] = n

    def start(i, c):
        j = lst[i]
        m = j // t
        v = ids_ref[m, j & (t - 1)] - r * vl
        q = (j & (t - 1)) // tl
        pltpu.make_async_copy(emb_ref.at[pl.ds(pl.multiple_of((v >> 3) << 3, 8), 8), :], buf.at[i], sem).start()
        own_ref[0, i] = ((q ^ r) >> 1) * 2 * h + m * h + ((q ^ r) & 1) * tl + (j & (tl - 1))
        own_ref[1, i] = v
        return c

    lax.fori_loop(0, n, start, 0)
    zero_start(z, de_ref, *FILL[2], zsem)
    for a in range(8):
        own_ref[0, n + a] = k * t
        own_ref[1, n + a] = 0
    xf[...] = jnp.zeros_like(xf)

    def wait(i, c):
        pltpu.make_async_copy(emb_ref.at[pl.ds(0, 8), :], buf.at[0], sem).wait()
        return c

    lax.fori_loop(0, n, wait, 0)

    def take(g, c):
        for a in range(8):
            tmp[a] = buf[g * 8 + a].astype(F32)
        for a in range(8):
            i = g * 8 + a
            xf[pl.ds(own_ref[0, i], 1), :] = tmp[a, pl.ds(own_ref[1, i] & 7, 1), :]
        return c

    lax.fori_loop(0, (n + 7) // 8, take, 0)
    for a, ref in enumerate((k0, s0, k1, s1)):
        for c in range(2):
            ref[c * tl:(c + 1) * tl, :] = xf[c * 2 * h + a * tl:c * 2 * h + (a + 1) * tl, :].astype(BF16)
    zero_wait(z, de_ref, FILL[1][0], FILL[2][1], zsem)


def sum_kernel(k0, y0, k1, y1, a0, t0, a1, t1):
    tl = a0.shape[0]
    for x, y, a, t in ((k0, y0, a0, t0), (k1, y1, a1, t1)):
        a[...] = x[0:tl, :] + y[0:tl, :]
        t[...] = x[tl:2 * tl, :] + y[tl:2 * tl, :]


def chip_mask(ids_ref, m, q, tl, chip_rows):
    t = ids_ref.shape[1]
    row = lax.broadcasted_iota(jnp.int32, (tl, t), 0) + q * tl
    lane = lax.broadcasted_iota(jnp.int32, (tl, t), 1)
    ids = jnp.broadcast_to(ids_ref[m:m + 1, :].astype(F32), (tl, t))
    col = jnp.sum(jnp.where(row == lane, ids, 0.0), axis=1, keepdims=True)
    lo = ((lax.axis_index("tp") >> 1) * chip_rows).astype(F32)
    return jnp.logical_and(col >= lo, col < lo + chip_rows)


def dx_kernel(m, chip_rows, xh_ref, z_ref, p0, p1, p2, p3, r0, r1, r2, r3, dres_ref, g_ref, ids_ref, tok_ref, *refs):
    if m == 1:
        both0_ref, dg0_ref, both_ref, slot_ref, dg_ref, xs_ref = refs
    else:
        both_ref, slot_ref, dg_ref = refs
    tl = slot_ref.shape[0]
    xh = xh_ref[...].astype(F32)
    x = xh + z_ref[...].astype(F32)
    both_ref[0:tl, :] = x.astype(BF16)
    if m == 1:
        xs_ref[0] = both0_ref[0:tl, :]
        xs_ref[1] = x.astype(BF16)
    g = g_ref[...].astype(F32)
    rs = lax.rsqrt(jnp.mean(x * x, axis=-1, keepdims=True) + EPS)
    nh = x * rs
    s = slice(m * tl, (m + 1) * tl)
    dn = jnp.concatenate([
        (a[s, :].astype(F32) + b[s, :].astype(F32)) + (c[s, :].astype(F32) + e[s, :].astype(F32))
        for a, b, c, e in ((p0, p1, p2, p3), (r0, r1, r2, r3))], axis=1)
    gdn = g * dn
    mean = jnp.mean(nh * gdn, axis=-1, keepdims=True)
    dxn = rs * (gdn - nh * mean)
    dx = (dres_ref[m].astype(F32) + dxn).astype(BF16)
    both_ref[tl:2 * tl, :] = dx
    own = chip_mask(ids_ref, m, lax.axis_index("tp"), tl, chip_rows)
    slot_ref[...] = jnp.where(own, xh, dx.astype(F32)).astype(BF16)
    dg = jnp.sum(dn * nh, axis=0, keepdims=True)
    dg_ref[...] = dg if m == 0 else dg + dg0_ref[...]


def norm(x, g_ref):
    rs = lax.rsqrt(jnp.mean(x * x, axis=-1, keepdims=True) + EPS)
    return ((x * rs) * g_ref[...].astype(F32)).astype(BF16)


def umat(n_ref, w_ref, ub, u_ref, q0, q1, sem):
    blk = 256
    for i in range(ub.shape[1] // blk):
        ub[:, i * blk:(i + 1) * blk] = jnp.dot(
            n_ref[...], w_ref[:, i * blk:(i + 1) * blk], preferred_element_type=F32).astype(BF16)
    k = u_ref.shape[0]
    tl = u_ref.shape[1] // 4
    copies = []
    for m in range(k):
        for a, q in enumerate((q0, q1)):
            c = pltpu.make_async_copy(ub.at[pl.ds((m * 2 + a) * tl, tl), :],
                                      u_ref.at[m, pl.ds(pl.multiple_of(q * tl, tl), tl), :], sem)
            c.start()
            copies.append(c)
    return copies


def take_du(du_ref, out_ref, tl, order):
    for a, (m, q) in enumerate(order):
        out_ref[a * tl:(a + 1) * tl, :] = du_ref[m, pl.ds(pl.multiple_of(q * tl, tl), tl), :]


def dw_tile(n_ref, du2, i, blk):
    return lax.dot_general(n_ref[:, i * blk:(i + 1) * blk], du2[...], (((0,), (0,)), ((), ())), preferred_element_type=F32)


def u_kernel(x0, y0, x1, y1, g_ref, w_ref, du_ref, tok_ref, u_ref, dwp_ref, n_ref, du2, ub, usem):
    r = lax.axis_index("tp")
    tl = x0.shape[0] // 2
    for a, x in enumerate((x0, y0, x1, y1)):
        n_ref[a * tl:(a + 1) * tl, :] = norm(x[0:tl, :].astype(F32), g_ref)
    take_du(du_ref, du2, tl, ((0, r), (0, r ^ 1), (1, r), (1, r ^ 1)))
    copies = umat(n_ref, w_ref, ub, u_ref, r, r ^ 1, usem)
    blk = 256
    for i in range(dwp_ref.shape[0] // blk):
        dwp_ref[i * blk:(i + 1) * blk, :] = dw_tile(n_ref, du2, i, blk)
    for c in copies:
        c.wait()


def scatter(near, list_ref, xf, de_ref, sem):
    e = list_ref.shape[1] - 1
    split = xf.shape[0] if near else xf.shape[0] // 2

    def add(i, c):
        a = list_ref[2, i]
        b = list_ref[3, i]

        @pl.when((b < split) if near else (b >= split))
        def _():
            xf[pl.ds(b, 1), :] = xf[pl.ds(b, 1), :] + xf[pl.ds(a, 1), :]

        return c

    @pl.when((list_ref[3, e] > 0) if near else (list_ref[2, e] > list_ref[3, e]))
    def _():
        lax.fori_loop(0, list_ref[2, e], add, 0)

    def put(i, c):
        pltpu.make_async_copy(xf.at[pl.ds(list_ref[0, i], 1), :], de_ref.at[pl.ds(list_ref[1, i], 1), :], sem).start()
        return c

    lax.fori_loop(*((0, list_ref[1, e]) if near else (list_ref[1, e], list_ref[0, e])), put, 0)


def scatter_wait(near, list_ref, xf, de_ref, sem):
    e = list_ref.shape[1] - 1

    def wait(i, c):
        pltpu.make_async_copy(xf.at[pl.ds(0, 1), :], de_ref.at[pl.ds(0, 1), :], sem).wait()
        return c

    lax.fori_loop(*((0, list_ref[1, e]) if near else (list_ref[1, e], list_ref[0, e])), wait, 0)


def near_kernel(list_ref, d0, a0, d1, a1, tok_ref, de_in, xn_ref, de_ref, sem):
    tl = d0.shape[0] // 2
    for a, ref in enumerate((d0, a0, d1, a1)):
        xn_ref[a * tl:(a + 1) * tl, :] = ref[tl:2 * tl, :].astype(F32)
    scatter(True, list_ref, xn_ref, de_ref, sem)
    scatter_wait(True, list_ref, xn_ref, de_ref, sem)


def last_kernel(chip_rows, list_ref, xn_ref, c0, b0, c1, b1, t0, w0, t1, w1, dwp_ref, ids_ref, g_ref,
                w_ref, du_ref, u_in, de_in, u_ref, dw_ref, de_ref, xf, n_ref, du2, ub, dwb, usem, wsem, sem):
    d = w_ref.shape[0]
    tl = c0.shape[0]
    r = lax.axis_index("tp")
    h = xn_ref.shape[0]

    @pl.when(list_ref[2, list_ref.shape[1] - 1] > list_ref[3, list_ref.shape[1] - 1])
    def _():
        xf[0:h, :] = xn_ref[...]

    for a, ref in enumerate((c0, b0, c1, b1)):
        xf[h + a * tl:h + (a + 1) * tl, :] = ref[...].astype(F32)
    scatter(False, list_ref, xf, de_ref, sem)
    take_du(du_ref, du2, tl, ((0, r ^ 2), (0, r ^ 3), (1, r ^ 2), (1, r ^ 3)))
    for a, (m, q, own, got) in enumerate(((0, r ^ 2, t0, c0), (0, r ^ 3, w0, b0), (1, r ^ 2, t1, c1), (1, r ^ 3, w1, b1))):
        x = jnp.where(chip_mask(ids_ref, m, q, tl, chip_rows), own[...].astype(F32), got[...].astype(F32))
        n_ref[a * tl:(a + 1) * tl, :] = norm(x, g_ref)
    blk = 256
    for i in range(d // blk):
        rows = slice(i * blk, (i + 1) * blk)
        dwb[rows, :] = dwp_ref[rows, :] + dw_tile(n_ref, du2, i, blk)
        pltpu.make_async_copy(dwb.at[pl.ds(i * blk, blk), :], dw_ref.at[pl.ds(i * blk, blk), :], wsem).start()
    copies = umat(n_ref, w_ref, ub, u_ref, r ^ 2, r ^ 3, usem)
    scatter_wait(False, list_ref, xf, de_ref, sem)
    pltpu.make_async_copy(dwb, dw_ref, wsem).wait()
    for c in copies:
        c.wait()


def solution(mesh):
    groups = mesh.shape["tp"]
    sib = [(i, i ^ 1) for i in range(groups)]
    cross = [(i, i ^ 2) for i in range(groups)]
    diag = [(i, i ^ 3) for i in range(groups)]

    def local(ids, emb, g, w, du, dres):
        k, t = ids.shape
        vl, d = emb.shape
        fc = w.shape[1]
        tl = t // groups
        n = k * tl
        h = 2 * n
        g2 = g.reshape(1, d)
        S = jax.ShapeDtypeStruct
        D = pltpu.SemaphoreType.DMA

        def perm(v, p):
            return lax.ppermute(v, "tp", p)

        d1 = 4 * 256
        d2 = d - d1

        def pdn(lo, width, fill, *tok):
            extra = S((vl, d), F32) if fill else S((8,), jnp.int32)
            return call(
                functools.partial(pdn_kernel, lo, fill), 60, [S((n, width), BF16)] * 4 + [extra],
                [HBM] * 2 + [SMEM] * len(tok), [HBM] * 4 + [HBM if fill else SMEM],
                [pltpu.VMEM((k, t, fc), BF16), pltpu.VMEM((4 * n, fc), BF16), pltpu.VMEM((width, fc), BF16),
                 pltpu.VMEM((4 * n, width), BF16), D, D((width // 256,)), D]
                + ([pltpu.VMEM((256, d), F32), D] if fill else []),
                8 * n * fc * width, 2 * width * fc + 8 * n * (fc + width))(du, w, *tok)

        p2, p3, p1, p0, first = pdn(0, d1, False)
        q2 = perm(p2, cross)
        q3 = perm(p3, diag)
        r2, r3, r1, r0, de = pdn(d1, d2, True, first)
        v2 = perm(r2, cross)
        v3 = perm(r3, diag)
        k0, s0, k1, s1, owned, de = call(
            gather_kernel, 36,
            [S((n, d), BF16)] * 4 + [S((2, 2 * h + 16), jnp.int32), S((vl, d), F32)],
            [SMEM, HBM, HBM], [VMEM] * 4 + [SMEM, HBM],
            [pltpu.VMEM((2 * h, 8, d), BF16), pltpu.VMEM((8, 8, d), F32), pltpu.VMEM((2 * h + 8, d), F32), pltpu.VMEM((256, d), F32)]
            + [pltpu.SMEM((2 * h + 8,), jnp.int32), D, D],
            500_000_000, 16 * h * d, {2: 5})(ids, emb, de)
        y0 = perm(s0, sib)
        y1 = perm(s1, sib)
        q1 = perm(p1, sib)
        v1 = perm(r1, sib)
        own0, oth0, own1, oth1 = call(sum_kernel, 16, [S((tl, d), BF16)] * 4, [VMEM] * 4, [VMEM] * 4, [],
                                      8 * tl * d, 24 * tl * d)(k0, y0, k1, y1)
        z0 = perm(oth0, cross)
        z1 = perm(oth1, cross)
        w0 = perm(oth0, sib)
        w1 = perm(oth1, sib)
        lists, de = call(
            zero_kernel, 8, [S((4, 2 * h + 16), jnp.int32), S((vl, d), F32)], [SMEM, HBM], [SMEM, HBM],
            [pltpu.VMEM((256, d), F32), pltpu.SMEM((2 * h + 8,), jnp.int32), pltpu.SMEM((vl,), jnp.int32), D],
            6_000_000_000, 2 * vl * d, {1: 1})(owned, de)

        def dxk(m, xh, z, tok, more):
            outs = [S((n, d), BF16), S((tl, d), BF16), S((1, d), F32)] + ([S((k, tl, d), BF16)] if m else [])
            return call(functools.partial(dx_kernel, m, 2 * vl), 16, outs,
                        [VMEM] * 13 + [HBM] + [VMEM] * len(more),
                        [VMEM] * len(outs), [], 30 * n * d, 16 * n * d)(
                            xh, z, p0, q1, q2, q3, r0, v1, v2, v3, dres, g2, ids, tok, *more)

        mine0, slot0, dg0 = dxk(0, own0, z0, de, ())
        c0 = perm(slot0, cross)
        next0 = perm(mine0, sib)
        de = call(zero2_kernel, 8, S((vl, d), F32), [VMEM, HBM], HBM, [pltpu.VMEM((256, d), F32), D],
                  2_000_000_000, vl * d, {1: 0})(dg0, de)
        mine1, slot1, dg, x = dxk(1, own1, z1, de, (mine0, dg0))
        c1 = perm(slot1, cross)
        next1 = perm(mine1, sib)
        u, dwp = call(
            u_kernel, 32, [S((k, t, fc), BF16), S((d, fc), F32)], [VMEM] * 8, [HBM, VMEM],
            [pltpu.VMEM((t, d), BF16), pltpu.VMEM((t, fc), BF16), pltpu.VMEM((t, fc), BF16), D],
            4 * t * d * fc, 2 * d * fc)(mine0, next0, mine1, next1, g2, w, du, dg)
        xn, de = call(near_kernel, 8, [S((t, d), F32), S((vl, d), F32)], [SMEM] + [VMEM] * 5 + [HBM], [VMEM, HBM],
                      [D], 8 * h * d, 8 * h * d, {6: 1})(lists, mine0, next0, mine1, next1, dg, de)
        b0 = perm(c0, sib)
        b1 = perm(c1, sib)
        dgs = dg + perm(dg, sib)
        dgs = dgs + perm(dgs, cross)

        u, dw, de = call(
            functools.partial(last_kernel, 2 * vl), 20, [S((k, t, fc), BF16), S((d, fc), F32), S((vl, d), F32)],
            [SMEM] + [VMEM] * 14 + [HBM] * 2, [HBM] * 3,
            [pltpu.VMEM((2 * h, d), F32), pltpu.VMEM((t, d), BF16), pltpu.VMEM((t, fc), BF16), pltpu.VMEM((t, fc), BF16),
             pltpu.VMEM((d, fc), F32), D, D, D],
            4 * t * d * fc, 6 * d * fc, {15: 0, 16: 2})(
                lists, xn, c0, b0, c1, b1, oth0, w0, oth1, w1, dwp, ids, g2, w, du, u, de)
        return u, x, de, dw, dgs.reshape(d)

    return jax.shard_map(
        local,
        mesh=mesh,
        in_specs=(P("dp", None), P("tp", None), P(None), P(None, "tp"), P("dp", None, "tp"), P("dp", "tp", None)),
        out_specs=(P("dp", None, "tp"), P("dp", "tp", None), P(("dp", "tp"), None), P(None, ("dp", "tp")), P("dp")),
        check_vma=False,
    )
```

```python
import functools

import jax
import jax.numpy as jnp
from jax import lax
from jax.experimental import pallas as pl
from jax.experimental.pallas import tpu as pltpu
from jax.sharding import PartitionSpec as P


EPS = 1e-6
F32 = jnp.float32
BF16 = jnp.bfloat16
HBM = pl.BlockSpec(memory_space=pltpu.HBM)
VMEM = pl.BlockSpec(memory_space=pltpu.VMEM)
SMEM = pl.BlockSpec(memory_space=pltpu.SMEM)


def call(body, mib, outs, ins, out_specs, scratch, flops, nbytes, aliases=None):
    return pl.pallas_call(
        body,
        out_shape=outs,
        in_specs=ins,
        out_specs=out_specs,
        scratch_shapes=scratch,
        input_output_aliases=aliases or {},
        cost_estimate=pl.CostEstimate(flops=flops, bytes_accessed=nbytes, transcendentals=0),
        compiler_params=pltpu.CompilerParams(vmem_limit_bytes=mib << 20),
    )


def pdn_kernel(du_ref, w_ref, *refs):
    outs = refs[:4]
    dub, dup, wb, ob, dsem, wsem, osem = refs[4:]
    n, d = outs[0].shape
    k, tl = dub.shape[0], dub.shape[1] // 4
    blk = 256
    nb = d // blk
    dc = pltpu.make_async_copy(du_ref, dub, dsem)
    dc.start()
    for i in range(nb):
        pltpu.make_async_copy(w_ref.at[pl.ds(i * blk, blk), :], wb.at[pl.ds(i * blk, blk), :], wsem.at[i]).start()
    r = lax.axis_index("tp")
    dc.wait()
    for a, j in enumerate((2, 3, 1, 0)):
        q = r ^ j
        for m in range(k):
            dup[pl.ds(a * n + m * tl, tl), :] = dub[m, pl.ds(pl.multiple_of(q * tl, tl), tl), :]

    def tile(i, c):
        cols = pl.ds(pl.multiple_of(i * blk, blk), blk)
        pltpu.make_async_copy(w_ref.at[cols, :], wb.at[cols, :], wsem.at[i]).wait()
        p = lax.dot_general(dup[...], wb[cols, :], (((1,), (1,)), ((), ())), preferred_element_type=F32)
        ob[:, cols] = p.astype(BF16)
        for a in range(4):
            pltpu.make_async_copy(ob.at[pl.ds(a * n, n), cols], outs[a].at[:, cols], osem).start()
        return c

    lax.fori_loop(0, nb, tile, 0)
    for a in range(4):
        pltpu.make_async_copy(ob.at[pl.ds(a * n, n), :], outs[a], osem).wait()


FILL = ((0, 3), (3, 6), (6, 16))


def zero_start(z, de_ref, lo, hi, sem):
    step = z.shape[0]
    per = de_ref.shape[0] // 16
    for i in range((hi - lo) * per // step):
        pltpu.make_async_copy(z, de_ref.at[pl.ds(lo * per + i * step, step), :], sem).start()


def zero_wait(z, de_ref, lo, hi, sem):
    step = z.shape[0]
    for _ in range((hi - lo) * (de_ref.shape[0] // 16) // step):
        pltpu.make_async_copy(z, de_ref.at[pl.ds(0, step), :], sem).wait()


def zero_kernel(own_ref, de_in, list_ref, de_ref, z, lnxt, tab, sem):
    z[...] = jnp.zeros_like(z)
    zero_start(z, de_ref, *FILL[2], sem)
    n = own_ref[0, own_ref.shape[1] - 1]
    t = lnxt.shape[0] - 8

    def link(i, c):
        v = own_ref[1, i]
        p = tab[v]
        ok = jnp.logical_and(p >= 0, p < i)
        p = jnp.where(ok, p, 0)
        ok = jnp.logical_and(ok, own_ref[1, p] == v)
        lnxt[i] = -1
        lnxt[jnp.where(ok, p, t)] = i
        tab[v] = i
        return c

    lax.fori_loop(0, n, link, 0)

    def lists(i, c):
        nl, nd, nl0, nd0, nl1, nd1 = c
        x = lnxt[i]
        end = (x < 0).astype(jnp.int32)
        pos = own_ref[0, i]
        list_ref[0, nl] = pos
        list_ref[1, nl] = own_ref[1, i]
        list_ref[2, nd] = pos
        list_ref[3, nd] = own_ref[0, jnp.maximum(x, 0)]
        to = list_ref[3, nd]
        dup = 1 - end
        return (nl + end, nd + dup, nl0 + end * (pos < SEG[1]).astype(jnp.int32), nd0 + dup * (to < SEG[1]).astype(jnp.int32),
                nl1 + end * (pos < SEG[2]).astype(jnp.int32), nd1 + dup * (to < SEG[2]).astype(jnp.int32))

    nl, nd, nl0, nd0, nl1, nd1 = lax.fori_loop(0, n, lists, (0,) * 6)
    e = list_ref.shape[1]
    for a, v in enumerate((0, nl0, nl1, nl)):
        list_ref[a, e - 1] = v
    for a, v in enumerate((0, nd0, nd1, nd)):
        list_ref[a, e - 2] = v
    zero_wait(z, de_ref, *FILL[2], sem)


def gather_kernel(ids_ref, emb_ref, k0, s0, k1, s1, own_ref, de_ref, buf, tmp, xf, z, lst, sem, zsem):
    k, t = ids_ref.shape
    vl = emb_ref.shape[0]
    h = k0.shape[0]
    tl = t // 4
    r = lax.axis_index("tp")
    z[...] = jnp.zeros_like(z)
    zero_start(z, de_ref, *FILL[0], zsem)
    n = 0
    for m, q in ((0, r), (0, r ^ 1), (1, r), (1, r ^ 1), (0, r ^ 2), (0, r ^ 3), (1, r ^ 2), (1, r ^ 3)):
        def scan(i, n):
            j = q * tl + i
            lst[n] = m * t + j
            return n + (lax.shift_right_logical(ids_ref[m, j], vl.bit_length() - 1) == r).astype(jnp.int32)

        n = lax.fori_loop(0, tl, scan, n, unroll=16)
    own_ref[0, own_ref.shape[1] - 1] = n

    def start(i, c):
        j = lst[i]
        m = j // t
        v = ids_ref[m, j & (t - 1)] - r * vl
        q = (j & (t - 1)) // tl
        pltpu.make_async_copy(emb_ref.at[pl.ds(pl.multiple_of((v >> 3) << 3, 8), 8), :], buf.at[i], sem).start()
        own_ref[0, i] = ((q ^ r) >> 1) * 2 * h + m * h + ((q ^ r) & 1) * tl + (j & (tl - 1))
        own_ref[1, i] = v
        return c

    lax.fori_loop(0, n, start, 0)
    zero_start(z, de_ref, *FILL[1], zsem)
    for a in range(8):
        own_ref[0, n + a] = k * t
        own_ref[1, n + a] = 0
    xf[...] = jnp.zeros_like(xf)

    def wait(i, c):
        pltpu.make_async_copy(emb_ref.at[pl.ds(0, 8), :], buf.at[0], sem).wait()
        return c

    lax.fori_loop(0, n, wait, 0)

    def take(g, c):
        for a in range(8):
            tmp[a] = buf[g * 8 + a].astype(F32)
        for a in range(8):
            i = g * 8 + a
            xf[pl.ds(own_ref[0, i], 1), :] = tmp[a, pl.ds(own_ref[1, i] & 7, 1), :]
        return c

    lax.fori_loop(0, (n + 7) // 8, take, 0)
    for a, ref in enumerate((k0, s0, k1, s1)):
        for c in range(2):
            ref[c * tl:(c + 1) * tl, :] = xf[c * 2 * h + a * tl:c * 2 * h + (a + 1) * tl, :].astype(BF16)
    zero_wait(z, de_ref, FILL[0][0], FILL[1][1], zsem)


def sum_kernel(k0, y0, k1, y1, a0, t0, a1, t1):
    tl = a0.shape[0]
    for x, y, a, t in ((k0, y0, a0, t0), (k1, y1, a1, t1)):
        a[...] = x[0:tl, :] + y[0:tl, :]
        t[...] = x[tl:2 * tl, :] + y[tl:2 * tl, :]


def chip_mask(ids_ref, m, q, tl, chip_rows):
    t = ids_ref.shape[1]
    row = lax.broadcasted_iota(jnp.int32, (tl, t), 0) + q * tl
    lane = lax.broadcasted_iota(jnp.int32, (tl, t), 1)
    ids = jnp.broadcast_to(ids_ref[m:m + 1, :].astype(F32), (tl, t))
    col = jnp.sum(jnp.where(row == lane, ids, 0.0), axis=1, keepdims=True)
    lo = ((lax.axis_index("tp") >> 1) * chip_rows).astype(F32)
    return jnp.logical_and(col >= lo, col < lo + chip_rows)


def dx_kernel(m, chip_rows, xh_ref, z_ref, p0, p1, p2, p3, dres_ref, g_ref, ids_ref, tok_ref, *refs):
    if m == 1:
        both0_ref, dg0_ref, both_ref, slot_ref, dg_ref, xs_ref = refs
    else:
        both_ref, slot_ref, dg_ref = refs
    tl = slot_ref.shape[0]
    xh = xh_ref[...].astype(F32)
    x = xh + z_ref[...].astype(F32)
    both_ref[0:tl, :] = x.astype(BF16)
    if m == 1:
        xs_ref[0] = both0_ref[0:tl, :]
        xs_ref[1] = x.astype(BF16)
    g = g_ref[...].astype(F32)
    rs = lax.rsqrt(jnp.mean(x * x, axis=-1, keepdims=True) + EPS)
    nh = x * rs
    s = slice(m * tl, (m + 1) * tl)
    dn = (p0[s, :].astype(F32) + p1[s, :].astype(F32)) + (p2[s, :].astype(F32) + p3[s, :].astype(F32))
    gdn = g * dn
    mean = jnp.mean(nh * gdn, axis=-1, keepdims=True)
    dxn = rs * (gdn - nh * mean)
    dx = (dres_ref[m].astype(F32) + dxn).astype(BF16)
    both_ref[tl:2 * tl, :] = dx
    own = chip_mask(ids_ref, m, lax.axis_index("tp"), tl, chip_rows)
    slot_ref[...] = jnp.where(own, xh, dx.astype(F32)).astype(BF16)
    dg = jnp.sum(dn * nh, axis=0, keepdims=True)
    dg_ref[...] = dg if m == 0 else dg + dg0_ref[...]


def norm(x, g_ref):
    rs = lax.rsqrt(jnp.mean(x * x, axis=-1, keepdims=True) + EPS)
    return ((x * rs) * g_ref[...].astype(F32)).astype(BF16)


def umat(n_ref, w_ref, ub, u_ref, q0, q1, sem):
    blk = 256
    for i in range(ub.shape[1] // blk):
        ub[:, i * blk:(i + 1) * blk] = jnp.dot(
            n_ref[...], w_ref[:, i * blk:(i + 1) * blk], preferred_element_type=F32).astype(BF16)
    k = u_ref.shape[0]
    tl = u_ref.shape[1] // 4
    copies = []
    for m in range(k):
        for a, q in enumerate((q0, q1)):
            c = pltpu.make_async_copy(ub.at[pl.ds((m * 2 + a) * tl, tl), :],
                                      u_ref.at[m, pl.ds(pl.multiple_of(q * tl, tl), tl), :], sem)
            c.start()
            copies.append(c)
    return copies


def take_du(du_ref, out_ref, tl, order):
    for a, (m, q) in enumerate(order):
        out_ref[a * tl:(a + 1) * tl, :] = du_ref[m, pl.ds(pl.multiple_of(q * tl, tl), tl), :]


def dw_tile(n_ref, du2, i, blk):
    return lax.dot_general(n_ref[:, i * blk:(i + 1) * blk], du2[...], (((0,), (0,)), ((), ())), preferred_element_type=F32)


def u_kernel(x0, y0, x1, y1, g_ref, w_ref, du_ref, tok_ref, u_ref, dwp_ref, n_ref, du2, ub, usem):
    r = lax.axis_index("tp")
    tl = x0.shape[0] // 2
    for a, x in enumerate((x0, y0, x1, y1)):
        n_ref[a * tl:(a + 1) * tl, :] = norm(x[0:tl, :].astype(F32), g_ref)
    take_du(du_ref, du2, tl, ((0, r), (0, r ^ 1), (1, r), (1, r ^ 1)))
    copies = umat(n_ref, w_ref, ub, u_ref, r, r ^ 1, usem)
    blk = 256
    for i in range(dwp_ref.shape[0] // blk):
        dwp_ref[i * blk:(i + 1) * blk, :] = dw_tile(n_ref, du2, i, blk)
    for c in copies:
        c.wait()


SEG = (0, 256, 448, 512)


def scatter(p, list_ref, xf, de_ref, sem):
    e = list_ref.shape[1]

    def add(i, c):
        a = list_ref[2, i]
        b = list_ref[3, i]

        @pl.when(jnp.logical_and(b >= SEG[p], b < SEG[p + 1]))
        def _():
            xf[pl.ds(b, 1), :] = xf[pl.ds(b, 1), :] + xf[pl.ds(a, 1), :]

        return c

    @pl.when(repeats(p, list_ref))
    def _():
        lax.fori_loop(0, list_ref[3, e - 2], add, 0)

    def put(i, c):
        pltpu.make_async_copy(xf.at[pl.ds(list_ref[0, i], 1), :], de_ref.at[pl.ds(list_ref[1, i], 1), :], sem).start()
        return c

    lax.fori_loop(list_ref[p, e - 1], list_ref[p + 1, e - 1], put, 0)


def repeats(p, list_ref):
    e = list_ref.shape[1]
    return list_ref[p + 1, e - 2] > list_ref[p, e - 2]


def scatter_wait(p, list_ref, xf, de_ref, sem):
    e = list_ref.shape[1]

    def wait(i, c):
        pltpu.make_async_copy(xf.at[pl.ds(0, 1), :], de_ref.at[pl.ds(0, 1), :], sem).wait()
        return c

    lax.fori_loop(list_ref[p, e - 1], list_ref[p + 1, e - 1], wait, 0)


def near_kernel(list_ref, d0, a0, d1, a1, tok_ref, de_in, xn_ref, de_ref, sem):
    tl = d0.shape[0] // 2
    for a, ref in enumerate((d0, a0, d1, a1)):
        xn_ref[a * tl:(a + 1) * tl, :] = ref[tl:2 * tl, :].astype(F32)
    scatter(0, list_ref, xn_ref, de_ref, sem)
    scatter_wait(0, list_ref, xn_ref, de_ref, sem)


def far_n(ids_ref, m, q, own, got, g_ref, chip_rows):
    own_x = chip_mask(ids_ref, m, q, got.shape[0], chip_rows)
    return norm(jnp.where(own_x, own[...].astype(F32), got[...].astype(F32)), g_ref)


def mid_kernel(chip_rows, list_ref, xn_ref, c0, b0, c1, t0, w0, t1, ids_ref, g_ref, de_in, n_ref, xm_ref, de_ref, xf, sem):
    tl = c0.shape[0]
    h = xn_ref.shape[0]
    r = lax.axis_index("tp")

    @pl.when(repeats(1, list_ref))
    def _():
        xf[0:h, :] = xn_ref[...]

    for a, ref in enumerate((c0, b0, c1)):
        xf[h + a * tl:h + (a + 1) * tl, :] = ref[...].astype(F32)
    scatter(1, list_ref, xf, de_ref, sem)
    for a, (m, q, own, got) in enumerate(((0, r ^ 2, t0, c0), (0, r ^ 3, w0, b0), (1, r ^ 2, t1, c1))):
        n_ref[a * tl:(a + 1) * tl, :] = far_n(ids_ref, m, q, own, got, g_ref, chip_rows)
    xm_ref[...] = xf[h:h + 3 * tl, :]
    scatter_wait(1, list_ref, xf, de_ref, sem)


def last_kernel(chip_rows, list_ref, xn_ref, xm_ref, nm_ref, b1, w1, dwp_ref, ids_ref, g_ref,
                w_ref, du_ref, u_in, de_in, u_ref, dw_ref, de_ref, xf, n_ref, du2, ub, dwb, usem, wsem, sem):
    d = w_ref.shape[0]
    tl = b1.shape[0]
    r = lax.axis_index("tp")
    h = xn_ref.shape[0]

    @pl.when(repeats(2, list_ref))
    def _():
        xf[0:h, :] = xn_ref[...]
        xf[h:h + 3 * tl, :] = xm_ref[...]

    xf[h + 3 * tl:h + 4 * tl, :] = b1[...].astype(F32)
    scatter(2, list_ref, xf, de_ref, sem)
    take_du(du_ref, du2, tl, ((0, r ^ 2), (0, r ^ 3), (1, r ^ 2), (1, r ^ 3)))
    n_ref[0:3 * tl, :] = nm_ref[...]
    n_ref[3 * tl:4 * tl, :] = far_n(ids_ref, 1, r ^ 3, w1, b1, g_ref, chip_rows)
    blk = 256
    for i in range(d // blk):
        rows = slice(i * blk, (i + 1) * blk)
        dwb[rows, :] = dwp_ref[rows, :] + dw_tile(n_ref, du2, i, blk)
        pltpu.make_async_copy(dwb.at[pl.ds(i * blk, blk), :], dw_ref.at[pl.ds(i * blk, blk), :], wsem).start()
    copies = umat(n_ref, w_ref, ub, u_ref, r ^ 2, r ^ 3, usem)
    scatter_wait(2, list_ref, xf, de_ref, sem)
    pltpu.make_async_copy(dwb, dw_ref, wsem).wait()
    for c in copies:
        c.wait()


def solution(mesh):
    groups = mesh.shape["tp"]
    sib = [(i, i ^ 1) for i in range(groups)]
    cross = [(i, i ^ 2) for i in range(groups)]
    diag = [(i, i ^ 3) for i in range(groups)]

    def local(ids, emb, g, w, du, dres):
        k, t = ids.shape
        vl, d = emb.shape
        fc = w.shape[1]
        tl = t // groups
        n = k * tl
        h = 2 * n
        g2 = g.reshape(1, d)
        S = jax.ShapeDtypeStruct
        D = pltpu.SemaphoreType.DMA

        def perm(v, p):
            return lax.ppermute(v, "tp", p)

        p2, p3, p1, p0 = call(
            pdn_kernel, 60, [S((n, d), BF16)] * 4, [HBM] * 2, [HBM] * 4,
            [pltpu.VMEM((k, t, fc), BF16), pltpu.VMEM((4 * n, fc), BF16), pltpu.VMEM((d, fc), BF16), pltpu.VMEM((4 * n, d), BF16),
             D, D((d // 256,)), D], 8 * n * fc * d, 2 * d * fc + 8 * n * (fc + d))(du, w)
        q2 = perm(p2, cross)
        q3 = perm(p3, diag)
        k0, s0, k1, s1, owned, de = call(
            gather_kernel, 36,
            [S((n, d), BF16)] * 4 + [S((2, 2 * h + 16), jnp.int32), S((vl, d), F32)],
            [SMEM, HBM], [VMEM] * 4 + [SMEM, HBM],
            [pltpu.VMEM((2 * h, 8, d), BF16), pltpu.VMEM((8, 8, d), F32), pltpu.VMEM((2 * h + 8, d), F32), pltpu.VMEM((256, d), F32)]
            + [pltpu.SMEM((2 * h + 8,), jnp.int32), D, D],
            500_000_000, 16 * h * d)(ids, emb)
        y0 = perm(s0, sib)
        y1 = perm(s1, sib)
        q1 = perm(p1, sib)
        own0, oth0, own1, oth1 = call(sum_kernel, 16, [S((tl, d), BF16)] * 4, [VMEM] * 4, [VMEM] * 4, [],
                                      8 * tl * d, 24 * tl * d)(k0, y0, k1, y1)
        z0 = perm(oth0, cross)
        z1 = perm(oth1, cross)
        w0 = perm(oth0, sib)
        w1 = perm(oth1, sib)
        lists, de = call(
            zero_kernel, 8, [S((4, 2 * h + 16), jnp.int32), S((vl, d), F32)], [SMEM, HBM], [SMEM, HBM],
            [pltpu.VMEM((256, d), F32), pltpu.SMEM((2 * h + 8,), jnp.int32), pltpu.SMEM((vl,), jnp.int32), D],
            6_000_000_000, 2 * vl * d, {1: 1})(owned, de)

        def dxk(m, xh, z, tok, more):
            outs = [S((n, d), BF16), S((tl, d), BF16), S((1, d), F32)] + ([S((k, tl, d), BF16)] if m else [])
            return call(functools.partial(dx_kernel, m, 2 * vl), 16, outs,
                        [VMEM] * 9 + [HBM] + [VMEM] * len(more),
                        [VMEM] * len(outs), [], 30 * n * d, 16 * n * d)(
                            xh, z, p0, q1, q2, q3, dres, g2, ids, tok, *more)

        mine0, slot0, dg0 = dxk(0, own0, z0, de, ())
        c0 = perm(slot0, cross)
        next0 = perm(mine0, sib)
        mine1, slot1, dg, x = dxk(1, own1, z1, de, (mine0, dg0))
        c1 = perm(slot1, cross)
        next1 = perm(mine1, sib)
        u, dwp = call(
            u_kernel, 32, [S((k, t, fc), BF16), S((d, fc), F32)], [VMEM] * 8, [HBM, VMEM],
            [pltpu.VMEM((t, d), BF16), pltpu.VMEM((t, fc), BF16), pltpu.VMEM((t, fc), BF16), D],
            4 * t * d * fc, 2 * d * fc)(mine0, next0, mine1, next1, g2, w, du, dg)
        xn, de = call(near_kernel, 8, [S((t, d), F32), S((vl, d), F32)], [SMEM] + [VMEM] * 5 + [HBM], [VMEM, HBM],
                      [D], 8 * h * d, 8 * h * d, {6: 1})(lists, mine0, next0, mine1, next1, dg, de)
        b0 = perm(c0, sib)
        b1 = perm(c1, sib)
        dgs = dg + perm(dg, sib)
        dgs = dgs + perm(dgs, cross)

        nm, xm, de = call(
            functools.partial(mid_kernel, 2 * vl), 16, [S((3 * tl, d), BF16), S((3 * tl, d), F32), S((vl, d), F32)],
            [SMEM] + [VMEM] * 9 + [HBM], [VMEM, VMEM, HBM], [pltpu.VMEM((t + 3 * tl, d), F32), D],
            8 * h * d, 8 * h * d, {10: 2})(lists, xn, c0, b0, c1, oth0, w0, oth1, ids, g2, de)
        u, dw, de = call(
            functools.partial(last_kernel, 2 * vl), 20, [S((k, t, fc), BF16), S((d, fc), F32), S((vl, d), F32)],
            [SMEM] + [VMEM] * 10 + [HBM] * 2, [HBM] * 3,
            [pltpu.VMEM((2 * h, d), F32), pltpu.VMEM((t, d), BF16), pltpu.VMEM((t, fc), BF16), pltpu.VMEM((t, fc), BF16),
             pltpu.VMEM((d, fc), F32), D, D, D],
            4 * t * d * fc, 6 * d * fc, {11: 0, 12: 2})(
                lists, xn, xm, nm, b1, w1, dwp, ids, g2, w, du, u, de)
        return u, x, de, dw, dgs.reshape(d)

    return jax.shard_map(
        local,
        mesh=mesh,
        in_specs=(P("dp", None), P("tp", None), P(None), P(None, "tp"), P("dp", None, "tp"), P("dp", "tp", None)),
        out_specs=(P("dp", None, "tp"), P("dp", "tp", None), P(("dp", "tp"), None), P(None, ("dp", "tp")), P("dp")),
        check_vma=False,
    )
```

```python
import functools

import jax
import jax.numpy as jnp
from jax import lax
from jax.experimental import pallas as pl
from jax.experimental.pallas import tpu as pltpu
from jax.sharding import PartitionSpec as P


EPS = 1e-6
F32 = jnp.float32
BF16 = jnp.bfloat16
HBM = pl.BlockSpec(memory_space=pltpu.HBM)
VMEM = pl.BlockSpec(memory_space=pltpu.VMEM)
SMEM = pl.BlockSpec(memory_space=pltpu.SMEM)


def call(body, mib, outs, ins, out_specs, scratch, flops, nbytes, aliases=None):
    return pl.pallas_call(
        body,
        out_shape=outs,
        in_specs=ins,
        out_specs=out_specs,
        scratch_shapes=scratch,
        input_output_aliases=aliases or {},
        cost_estimate=pl.CostEstimate(flops=flops, bytes_accessed=nbytes, transcendentals=0),
        compiler_params=pltpu.CompilerParams(vmem_limit_bytes=mib << 20),
    )


def pdn_kernel(du_ref, w_ref, *refs):
    outs = refs[:4]
    dub, dup, wb, ob, dsem, wsem, osem = refs[4:]
    n, d = outs[0].shape
    k, tl = dub.shape[0], dub.shape[1] // 4
    blk = 768
    nb = d // blk
    dc = pltpu.make_async_copy(du_ref, dub, dsem)
    dc.start()
    for i in range(nb):
        pltpu.make_async_copy(w_ref.at[pl.ds(i * blk, blk), :], wb.at[pl.ds(i * blk, blk), :], wsem.at[i]).start()
    r = lax.axis_index("tp")
    dc.wait()
    for a, j in enumerate((2, 3, 1, 0)):
        q = r ^ j
        for m in range(k):
            dup[pl.ds(a * n + m * tl, tl), :] = dub[m, pl.ds(pl.multiple_of(q * tl, tl), tl), :]

    def tile(i, c):
        cols = pl.ds(pl.multiple_of(i * blk, blk), blk)
        pltpu.make_async_copy(w_ref.at[cols, :], wb.at[cols, :], wsem.at[i]).wait()
        p = lax.dot_general(dup[...], wb[cols, :], (((1,), (1,)), ((), ())), preferred_element_type=F32)
        ob[:, cols] = p.astype(BF16)
        for a in range(4):
            pltpu.make_async_copy(ob.at[pl.ds(a * n, n), cols], outs[a].at[:, cols], osem).start()
        return c

    lax.fori_loop(0, nb, tile, 0)
    for a in range(4):
        pltpu.make_async_copy(ob.at[pl.ds(a * n, n), :], outs[a], osem).wait()


FILL = ((0, 3), (3, 6), (6, 16))


def zero_start(z, de_ref, lo, hi, sem):
    step = z.shape[0]
    per = de_ref.shape[0] // 16
    for i in range((hi - lo) * per // step):
        pltpu.make_async_copy(z, de_ref.at[pl.ds(lo * per + i * step, step), :], sem).start()


def zero_wait(z, de_ref, lo, hi, sem):
    step = z.shape[0]
    for _ in range((hi - lo) * (de_ref.shape[0] // 16) // step):
        pltpu.make_async_copy(z, de_ref.at[pl.ds(0, step), :], sem).wait()


def zero_kernel(own_ref, de_in, list_ref, de_ref, z, lnxt, tab, sem):
    z[...] = jnp.zeros_like(z)
    zero_start(z, de_ref, *FILL[2], sem)
    n = own_ref[0, own_ref.shape[1] - 1]
    t = lnxt.shape[0] - 8

    def link(i, c):
        v = own_ref[1, i]
        p = tab[v]
        ok = jnp.logical_and(p >= 0, p < i)
        p = jnp.where(ok, p, 0)
        ok = jnp.logical_and(ok, own_ref[1, p] == v)
        lnxt[i] = -1
        lnxt[jnp.where(ok, p, t)] = i
        tab[v] = i
        return c

    lax.fori_loop(0, n, link, 0)

    def lists(i, c):
        nl, nd, nl0, nd0, nl1, nd1 = c
        x = lnxt[i]
        end = (x < 0).astype(jnp.int32)
        pos = own_ref[0, i]
        list_ref[0, nl] = pos
        list_ref[1, nl] = own_ref[1, i]
        list_ref[2, nd] = pos
        list_ref[3, nd] = own_ref[0, jnp.maximum(x, 0)]
        to = list_ref[3, nd]
        dup = 1 - end
        return (nl + end, nd + dup, nl0 + end * (pos < SEG[1]).astype(jnp.int32), nd0 + dup * (to < SEG[1]).astype(jnp.int32),
                nl1 + end * (pos < SEG[2]).astype(jnp.int32), nd1 + dup * (to < SEG[2]).astype(jnp.int32))

    nl, nd, nl0, nd0, nl1, nd1 = lax.fori_loop(0, n, lists, (0,) * 6)
    e = list_ref.shape[1]
    for a, v in enumerate((0, nl0, nl1, nl)):
        list_ref[a, e - 1] = v
    for a, v in enumerate((0, nd0, nd1, nd)):
        list_ref[a, e - 2] = v
    zero_wait(z, de_ref, *FILL[2], sem)


def gather_kernel(ids_ref, emb_ref, k0, s0, k1, s1, own_ref, de_ref, buf, tmp, xf, z, lst, sem, zsem):
    k, t = ids_ref.shape
    vl = emb_ref.shape[0]
    h = k0.shape[0]
    tl = t // 4
    r = lax.axis_index("tp")
    z[...] = jnp.zeros_like(z)
    zero_start(z, de_ref, *FILL[0], zsem)
    n = 0
    for m, q in ((0, r), (0, r ^ 1), (1, r), (1, r ^ 1), (0, r ^ 2), (0, r ^ 3), (1, r ^ 2), (1, r ^ 3)):
        def scan(i, n):
            j = q * tl + i
            lst[n] = m * t + j
            return n + (lax.shift_right_logical(ids_ref[m, j], vl.bit_length() - 1) == r).astype(jnp.int32)

        n = lax.fori_loop(0, tl, scan, n, unroll=16)
    own_ref[0, own_ref.shape[1] - 1] = n

    def start(i, c):
        j = lst[i]
        m = j // t
        v = ids_ref[m, j & (t - 1)] - r * vl
        q = (j & (t - 1)) // tl
        pltpu.make_async_copy(emb_ref.at[pl.ds(pl.multiple_of((v >> 3) << 3, 8), 8), :], buf.at[i], sem).start()
        own_ref[0, i] = ((q ^ r) >> 1) * 2 * h + m * h + ((q ^ r) & 1) * tl + (j & (tl - 1))
        own_ref[1, i] = v
        return c

    lax.fori_loop(0, n, start, 0)
    zero_start(z, de_ref, *FILL[1], zsem)
    for a in range(8):
        own_ref[0, n + a] = k * t
        own_ref[1, n + a] = 0
    xf[...] = jnp.zeros_like(xf)

    def wait(i, c):
        pltpu.make_async_copy(emb_ref.at[pl.ds(0, 8), :], buf.at[0], sem).wait()
        return c

    lax.fori_loop(0, n, wait, 0)

    def take(g, c):
        for a in range(8):
            tmp[a] = buf[g * 8 + a].astype(F32)
        for a in range(8):
            i = g * 8 + a
            xf[pl.ds(own_ref[0, i], 1), :] = tmp[a, pl.ds(own_ref[1, i] & 7, 1), :]
        return c

    lax.fori_loop(0, (n + 7) // 8, take, 0)
    for a, ref in enumerate((k0, s0, k1, s1)):
        for c in range(2):
            ref[c * tl:(c + 1) * tl, :] = xf[c * 2 * h + a * tl:c * 2 * h + (a + 1) * tl, :].astype(BF16)
    zero_wait(z, de_ref, FILL[0][0], FILL[1][1], zsem)


def sum_kernel(k0, y0, k1, y1, a0, t0, a1, t1):
    tl = a0.shape[0]
    for x, y, a, t in ((k0, y0, a0, t0), (k1, y1, a1, t1)):
        a[...] = x[0:tl, :] + y[0:tl, :]
        t[...] = x[tl:2 * tl, :] + y[tl:2 * tl, :]


def chip_mask(ids_ref, m, q, tl, chip_rows):
    t = ids_ref.shape[1]
    row = lax.broadcasted_iota(jnp.int32, (tl, t), 0) + q * tl
    lane = lax.broadcasted_iota(jnp.int32, (tl, t), 1)
    ids = jnp.broadcast_to(ids_ref[m:m + 1, :].astype(F32), (tl, t))
    col = jnp.sum(jnp.where(row == lane, ids, 0.0), axis=1, keepdims=True)
    lo = ((lax.axis_index("tp") >> 1) * chip_rows).astype(F32)
    return jnp.logical_and(col >= lo, col < lo + chip_rows)


def dx_kernel(m, chip_rows, xh_ref, z_ref, p0, p1, p2, p3, dres_ref, g_ref, ids_ref, tok_ref, *refs):
    if m == 1:
        both0_ref, dg0_ref, both_ref, slot_ref, dg_ref, xs_ref = refs
    else:
        both_ref, slot_ref, dg_ref = refs
    tl = slot_ref.shape[0]
    xh = xh_ref[...].astype(F32)
    x = xh + z_ref[...].astype(F32)
    both_ref[0:tl, :] = x.astype(BF16)
    if m == 1:
        xs_ref[0] = both0_ref[0:tl, :]
        xs_ref[1] = x.astype(BF16)
    g = g_ref[...].astype(F32)
    rs = lax.rsqrt(jnp.mean(x * x, axis=-1, keepdims=True) + EPS)
    nh = x * rs
    s = slice(m * tl, (m + 1) * tl)
    dn = (p0[s, :].astype(F32) + p1[s, :].astype(F32)) + (p2[s, :].astype(F32) + p3[s, :].astype(F32))
    gdn = g * dn
    mean = jnp.mean(nh * gdn, axis=-1, keepdims=True)
    dxn = rs * (gdn - nh * mean)
    dx = (dres_ref[m].astype(F32) + dxn).astype(BF16)
    both_ref[tl:2 * tl, :] = dx
    own = chip_mask(ids_ref, m, lax.axis_index("tp"), tl, chip_rows)
    slot_ref[...] = jnp.where(own, xh, dx.astype(F32)).astype(BF16)
    dg = jnp.sum(dn * nh, axis=0, keepdims=True)
    dg_ref[...] = dg if m == 0 else dg + dg0_ref[...]


def norm(x, g_ref):
    rs = lax.rsqrt(jnp.mean(x * x, axis=-1, keepdims=True) + EPS)
    return ((x * rs) * g_ref[...].astype(F32)).astype(BF16)


def umat(n_ref, w_ref, ub, u_ref, q0, q1, sem):
    blk = 256
    for i in range(ub.shape[1] // blk):
        ub[:, i * blk:(i + 1) * blk] = jnp.dot(
            n_ref[...], w_ref[:, i * blk:(i + 1) * blk], preferred_element_type=F32).astype(BF16)
    k = u_ref.shape[0]
    tl = u_ref.shape[1] // 4
    copies = []
    for m in range(k):
        for a, q in enumerate((q0, q1)):
            c = pltpu.make_async_copy(ub.at[pl.ds((m * 2 + a) * tl, tl), :],
                                      u_ref.at[m, pl.ds(pl.multiple_of(q * tl, tl), tl), :], sem)
            c.start()
            copies.append(c)
    return copies


def take_du(du_ref, out_ref, tl, order):
    for a, (m, q) in enumerate(order):
        out_ref[a * tl:(a + 1) * tl, :] = du_ref[m, pl.ds(pl.multiple_of(q * tl, tl), tl), :]


def dw_tile(n_ref, du2, i, blk):
    return lax.dot_general(n_ref[:, i * blk:(i + 1) * blk], du2[...], (((0,), (0,)), ((), ())), preferred_element_type=F32)


def u_kernel(x0, y0, x1, y1, g_ref, w_ref, du_ref, tok_ref, u_ref, dwp_ref, n_ref, du2, ub, usem):
    r = lax.axis_index("tp")
    tl = x0.shape[0] // 2
    for a, x in enumerate((x0, y0, x1, y1)):
        n_ref[a * tl:(a + 1) * tl, :] = norm(x[0:tl, :].astype(F32), g_ref)
    take_du(du_ref, du2, tl, ((0, r), (0, r ^ 1), (1, r), (1, r ^ 1)))
    copies = umat(n_ref, w_ref, ub, u_ref, r, r ^ 1, usem)
    blk = 256
    for i in range(dwp_ref.shape[0] // blk):
        dwp_ref[i * blk:(i + 1) * blk, :] = dw_tile(n_ref, du2, i, blk)
    for c in copies:
        c.wait()


SEG = (0, 256, 448, 512)


def scatter(p, list_ref, xf, de_ref, sem):
    e = list_ref.shape[1]

    def add(i, c):
        a = list_ref[2, i]
        b = list_ref[3, i]

        @pl.when(jnp.logical_and(b >= SEG[p], b < SEG[p + 1]))
        def _():
            xf[pl.ds(b, 1), :] = xf[pl.ds(b, 1), :] + xf[pl.ds(a, 1), :]

        return c

    @pl.when(repeats(p, list_ref))
    def _():
        lax.fori_loop(0, list_ref[3, e - 2], add, 0)

    def put(i, c):
        pltpu.make_async_copy(xf.at[pl.ds(list_ref[0, i], 1), :], de_ref.at[pl.ds(list_ref[1, i], 1), :], sem).start()
        return c

    lax.fori_loop(list_ref[p, e - 1], list_ref[p + 1, e - 1], put, 0)


def repeats(p, list_ref):
    e = list_ref.shape[1]
    return list_ref[p + 1, e - 2] > list_ref[p, e - 2]


def scatter_wait(p, list_ref, xf, de_ref, sem):
    e = list_ref.shape[1]

    def wait(i, c):
        pltpu.make_async_copy(xf.at[pl.ds(0, 1), :], de_ref.at[pl.ds(0, 1), :], sem).wait()
        return c

    lax.fori_loop(list_ref[p, e - 1], list_ref[p + 1, e - 1], wait, 0)


def near_kernel(list_ref, d0, a0, d1, a1, tok_ref, de_in, xn_ref, de_ref, sem):
    tl = d0.shape[0] // 2
    for a, ref in enumerate((d0, a0, d1, a1)):
        xn_ref[a * tl:(a + 1) * tl, :] = ref[tl:2 * tl, :].astype(F32)
    scatter(0, list_ref, xn_ref, de_ref, sem)
    scatter_wait(0, list_ref, xn_ref, de_ref, sem)


def far_n(ids_ref, m, q, own, got, g_ref, chip_rows):
    own_x = chip_mask(ids_ref, m, q, got.shape[0], chip_rows)
    return norm(jnp.where(own_x, own[...].astype(F32), got[...].astype(F32)), g_ref)


def mid_kernel(chip_rows, list_ref, xn_ref, c0, b0, c1, t0, w0, t1, ids_ref, g_ref, de_in, n_ref, xm_ref, de_ref, xf, sem):
    tl = c0.shape[0]
    h = xn_ref.shape[0]
    r = lax.axis_index("tp")

    @pl.when(repeats(1, list_ref))
    def _():
        xf[0:h, :] = xn_ref[...]

    for a, ref in enumerate((c0, b0, c1)):
        xf[h + a * tl:h + (a + 1) * tl, :] = ref[...].astype(F32)
    scatter(1, list_ref, xf, de_ref, sem)
    for a, (m, q, own, got) in enumerate(((0, r ^ 2, t0, c0), (0, r ^ 3, w0, b0), (1, r ^ 2, t1, c1))):
        n_ref[a * tl:(a + 1) * tl, :] = far_n(ids_ref, m, q, own, got, g_ref, chip_rows)
    xm_ref[...] = xf[h:h + 3 * tl, :]
    scatter_wait(1, list_ref, xf, de_ref, sem)


def last_kernel(chip_rows, list_ref, xn_ref, xm_ref, nm_ref, b1, w1, dwp_ref, ids_ref, g_ref,
                w_ref, du_ref, u_in, de_in, u_ref, dw_ref, de_ref, xf, n_ref, du2, ub, dwb, usem, wsem, sem):
    d = w_ref.shape[0]
    tl = b1.shape[0]
    r = lax.axis_index("tp")
    h = xn_ref.shape[0]

    @pl.when(repeats(2, list_ref))
    def _():
        xf[0:h, :] = xn_ref[...]
        xf[h:h + 3 * tl, :] = xm_ref[...]

    xf[h + 3 * tl:h + 4 * tl, :] = b1[...].astype(F32)
    scatter(2, list_ref, xf, de_ref, sem)
    take_du(du_ref, du2, tl, ((0, r ^ 2), (0, r ^ 3), (1, r ^ 2), (1, r ^ 3)))
    n_ref[0:3 * tl, :] = nm_ref[...]
    n_ref[3 * tl:4 * tl, :] = far_n(ids_ref, 1, r ^ 3, w1, b1, g_ref, chip_rows)
    blk = 256
    for i in range(d // blk):
        rows = slice(i * blk, (i + 1) * blk)
        dwb[rows, :] = dwp_ref[rows, :] + dw_tile(n_ref, du2, i, blk)
        pltpu.make_async_copy(dwb.at[pl.ds(i * blk, blk), :], dw_ref.at[pl.ds(i * blk, blk), :], wsem).start()
    copies = umat(n_ref, w_ref, ub, u_ref, r ^ 2, r ^ 3, usem)
    scatter_wait(2, list_ref, xf, de_ref, sem)
    pltpu.make_async_copy(dwb, dw_ref, wsem).wait()
    for c in copies:
        c.wait()


def solution(mesh):
    groups = mesh.shape["tp"]
    sib = [(i, i ^ 1) for i in range(groups)]
    cross = [(i, i ^ 2) for i in range(groups)]
    diag = [(i, i ^ 3) for i in range(groups)]

    def local(ids, emb, g, w, du, dres):
        k, t = ids.shape
        vl, d = emb.shape
        fc = w.shape[1]
        tl = t // groups
        n = k * tl
        h = 2 * n
        g2 = g.reshape(1, d)
        S = jax.ShapeDtypeStruct
        D = pltpu.SemaphoreType.DMA

        def perm(v, p):
            return lax.ppermute(v, "tp", p)

        p2, p3, p1, p0 = call(
            pdn_kernel, 60, [S((n, d), BF16)] * 4, [HBM] * 2, [HBM] * 4,
            [pltpu.VMEM((k, t, fc), BF16), pltpu.VMEM((4 * n, fc), BF16), pltpu.VMEM((d, fc), BF16), pltpu.VMEM((4 * n, d), BF16),
             D, D((d // 768,)), D], 8 * n * fc * d, 2 * d * fc + 8 * n * (fc + d))(du, w)
        q2 = perm(p2, cross)
        q3 = perm(p3, diag)
        k0, s0, k1, s1, owned, de = call(
            gather_kernel, 36,
            [S((n, d), BF16)] * 4 + [S((2, 2 * h + 16), jnp.int32), S((vl, d), F32)],
            [SMEM, HBM], [VMEM] * 4 + [SMEM, HBM],
            [pltpu.VMEM((2 * h, 8, d), BF16), pltpu.VMEM((8, 8, d), F32), pltpu.VMEM((2 * h + 8, d), F32), pltpu.VMEM((256, d), F32)]
            + [pltpu.SMEM((2 * h + 8,), jnp.int32), D, D],
            500_000_000, 16 * h * d)(ids, emb)
        y0 = perm(s0, sib)
        y1 = perm(s1, sib)
        q1 = perm(p1, sib)
        own0, oth0, own1, oth1 = call(sum_kernel, 16, [S((tl, d), BF16)] * 4, [VMEM] * 4, [VMEM] * 4, [],
                                      8 * tl * d, 24 * tl * d)(k0, y0, k1, y1)
        z0 = perm(oth0, cross)
        z1 = perm(oth1, cross)
        w0 = perm(oth0, sib)
        w1 = perm(oth1, sib)
        lists, de = call(
            zero_kernel, 8, [S((4, 2 * h + 16), jnp.int32), S((vl, d), F32)], [SMEM, HBM], [SMEM, HBM],
            [pltpu.VMEM((256, d), F32), pltpu.SMEM((2 * h + 8,), jnp.int32), pltpu.SMEM((vl,), jnp.int32), D],
            6_000_000_000, 2 * vl * d, {1: 1})(owned, de)

        def dxk(m, xh, z, tok, more):
            outs = [S((n, d), BF16), S((tl, d), BF16), S((1, d), F32)] + ([S((k, tl, d), BF16)] if m else [])
            return call(functools.partial(dx_kernel, m, 2 * vl), 16, outs,
                        [VMEM] * 9 + [HBM] + [VMEM] * len(more),
                        [VMEM] * len(outs), [], 30 * n * d, 16 * n * d)(
                            xh, z, p0, q1, q2, q3, dres, g2, ids, tok, *more)

        mine0, slot0, dg0 = dxk(0, own0, z0, de, ())
        c0 = perm(slot0, cross)
        next0 = perm(mine0, sib)
        mine1, slot1, dg, x = dxk(1, own1, z1, de, (mine0, dg0))
        c1 = perm(slot1, cross)
        next1 = perm(mine1, sib)
        u, dwp = call(
            u_kernel, 32, [S((k, t, fc), BF16), S((d, fc), F32)], [VMEM] * 8, [HBM, VMEM],
            [pltpu.VMEM((t, d), BF16), pltpu.VMEM((t, fc), BF16), pltpu.VMEM((t, fc), BF16), D],
            4 * t * d * fc, 2 * d * fc)(mine0, next0, mine1, next1, g2, w, du, dg)
        xn, de = call(near_kernel, 8, [S((t, d), F32), S((vl, d), F32)], [SMEM] + [VMEM] * 5 + [HBM], [VMEM, HBM],
                      [D], 8 * h * d, 8 * h * d, {6: 1})(lists, mine0, next0, mine1, next1, dg, de)
        b0 = perm(c0, sib)
        b1 = perm(c1, sib)
        dgs = dg + perm(dg, cross)
        dgs = dgs + perm(dgs, sib)

        nm, xm, de = call(
            functools.partial(mid_kernel, 2 * vl), 16, [S((3 * tl, d), BF16), S((3 * tl, d), F32), S((vl, d), F32)],
            [SMEM] + [VMEM] * 9 + [HBM], [VMEM, VMEM, HBM], [pltpu.VMEM((t + 3 * tl, d), F32), D],
            8 * h * d, 8 * h * d, {10: 2})(lists, xn, c0, b0, c1, oth0, w0, oth1, ids, g2, de)
        u, dw, de = call(
            functools.partial(last_kernel, 2 * vl), 20, [S((k, t, fc), BF16), S((d, fc), F32), S((vl, d), F32)],
            [SMEM] + [VMEM] * 10 + [HBM] * 2, [HBM] * 3,
            [pltpu.VMEM((2 * h, d), F32), pltpu.VMEM((t, d), BF16), pltpu.VMEM((t, fc), BF16), pltpu.VMEM((t, fc), BF16),
             pltpu.VMEM((d, fc), F32), D, D, D],
            4 * t * d * fc, 6 * d * fc, {11: 0, 12: 2})(
                lists, xn, xm, nm, b1, w1, dwp, ids, g2, w, du, u, de)
        return u, x, de, dw, dgs.reshape(d)

    return jax.shard_map(
        local,
        mesh=mesh,
        in_specs=(P("dp", None), P("tp", None), P(None), P(None, "tp"), P("dp", None, "tp"), P("dp", "tp", None)),
        out_specs=(P("dp", None, "tp"), P("dp", "tp", None), P(("dp", "tp"), None), P(None, ("dp", "tp")), P("dp")),
        check_vma=False,
    )
```

```python
import functools

import jax
import jax.numpy as jnp
from jax import lax
from jax.experimental import pallas as pl
from jax.experimental.pallas import tpu as pltpu
from jax.sharding import PartitionSpec as P


EPS = 1e-6
F32 = jnp.float32
BF16 = jnp.bfloat16
HBM = pl.BlockSpec(memory_space=pltpu.HBM)
VMEM = pl.BlockSpec(memory_space=pltpu.VMEM)
SMEM = pl.BlockSpec(memory_space=pltpu.SMEM)


def call(body, mib, outs, ins, out_specs, scratch, flops, nbytes, aliases=None):
    return pl.pallas_call(
        body,
        out_shape=outs,
        in_specs=ins,
        out_specs=out_specs,
        scratch_shapes=scratch,
        input_output_aliases=aliases or {},
        cost_estimate=pl.CostEstimate(flops=flops, bytes_accessed=nbytes, transcendentals=0),
        compiler_params=pltpu.CompilerParams(vmem_limit_bytes=mib << 20),
    )


def pdn_kernel(du_ref, w_ref, *refs):
    outs = refs[:4]
    dub, dup, wb, ob, dsem, wsem, osem = refs[4:]
    n, d = outs[0].shape
    k, tl = dub.shape[0], dub.shape[1] // 4
    blk = 768
    nb = d // blk
    dc = pltpu.make_async_copy(du_ref, dub, dsem)
    dc.start()
    for i in range(nb):
        pltpu.make_async_copy(w_ref.at[pl.ds(i * blk, blk), :], wb.at[pl.ds(i * blk, blk), :], wsem.at[i]).start()
    r = lax.axis_index("tp")
    dc.wait()
    for a, j in enumerate((2, 3, 1, 0)):
        q = r ^ j
        for m in range(k):
            dup[pl.ds(a * n + m * tl, tl), :] = dub[m, pl.ds(pl.multiple_of(q * tl, tl), tl), :]

    def tile(i, c):
        cols = pl.ds(pl.multiple_of(i * blk, blk), blk)
        pltpu.make_async_copy(w_ref.at[cols, :], wb.at[cols, :], wsem.at[i]).wait()
        p = lax.dot_general(dup[...], wb[cols, :], (((1,), (1,)), ((), ())), preferred_element_type=F32)
        ob[:, cols] = p.astype(BF16)
        for a in range(4):
            pltpu.make_async_copy(ob.at[pl.ds(a * n, n), cols], outs[a].at[:, cols], osem).start()
        return c

    lax.fori_loop(0, nb, tile, 0)
    for a in range(4):
        pltpu.make_async_copy(ob.at[pl.ds(a * n, n), :], outs[a], osem).wait()


FILL = ((0, 3), (3, 6), (6, 16))


def zero_start(z, de_ref, lo, hi, sem):
    step = z.shape[0]
    per = de_ref.shape[0] // 16
    for i in range((hi - lo) * per // step):
        pltpu.make_async_copy(z, de_ref.at[pl.ds(lo * per + i * step, step), :], sem).start()


def zero_wait(z, de_ref, lo, hi, sem):
    step = z.shape[0]
    for _ in range((hi - lo) * (de_ref.shape[0] // 16) // step):
        pltpu.make_async_copy(z, de_ref.at[pl.ds(0, step), :], sem).wait()


def zero_kernel(own_ref, de_in, list_ref, de_ref, z, lnxt, tab, sem):
    z[...] = jnp.zeros_like(z)
    zero_start(z, de_ref, *FILL[2], sem)
    n = own_ref[0, own_ref.shape[1] - 1]
    t = lnxt.shape[0] - 8

    def link(i, c):
        v = own_ref[1, i]
        p = tab[v]
        ok = jnp.logical_and(p >= 0, p < i)
        p = jnp.where(ok, p, 0)
        ok = jnp.logical_and(ok, own_ref[1, p] == v)
        lnxt[i] = -1
        lnxt[jnp.where(ok, p, t)] = i
        tab[v] = i
        return c

    lax.fori_loop(0, n, link, 0)

    def lists(i, c):
        nl, nd, nl0, nd0 = c
        x = lnxt[i]
        end = (x < 0).astype(jnp.int32)
        pos = own_ref[0, i]
        list_ref[0, nl] = pos
        list_ref[1, nl] = own_ref[1, i]
        list_ref[2, nd] = pos
        list_ref[3, nd] = own_ref[0, jnp.maximum(x, 0)]
        to = list_ref[3, nd]
        dup = 1 - end
        return nl + end, nd + dup, nl0 + end * (pos < SEG[1]).astype(jnp.int32), nd0 + dup * (to < SEG[1]).astype(jnp.int32)

    nl, nd, nl0, nd0 = lax.fori_loop(0, n, lists, (0,) * 4)
    e = list_ref.shape[1]
    for a, (v, x) in enumerate(((0, 0), (nl0, nd0), (nl, nd))):
        list_ref[a, e - 1] = v
        list_ref[a, e - 2] = x
    zero_wait(z, de_ref, *FILL[2], sem)


def gather_kernel(ids_ref, emb_ref, k0, s0, k1, s1, own_ref, de_ref, buf, tmp, xf, z, lst, sem, zsem):
    k, t = ids_ref.shape
    vl = emb_ref.shape[0]
    h = k0.shape[0]
    tl = t // 4
    r = lax.axis_index("tp")
    z[...] = jnp.zeros_like(z)
    zero_start(z, de_ref, *FILL[0], zsem)
    n = 0
    for m, q in ((0, r), (0, r ^ 1), (1, r), (1, r ^ 1), (0, r ^ 2), (0, r ^ 3), (1, r ^ 2), (1, r ^ 3)):
        def scan(i, n):
            j = q * tl + i
            lst[n] = m * t + j
            return n + (lax.shift_right_logical(ids_ref[m, j], vl.bit_length() - 1) == r).astype(jnp.int32)

        n = lax.fori_loop(0, tl, scan, n, unroll=16)
    own_ref[0, own_ref.shape[1] - 1] = n

    def start(i, c):
        j = lst[i]
        m = j // t
        v = ids_ref[m, j & (t - 1)] - r * vl
        q = (j & (t - 1)) // tl
        pltpu.make_async_copy(emb_ref.at[pl.ds(pl.multiple_of((v >> 3) << 3, 8), 8), :], buf.at[i], sem).start()
        own_ref[0, i] = ((q ^ r) >> 1) * 2 * h + m * h + ((q ^ r) & 1) * tl + (j & (tl - 1))
        own_ref[1, i] = v
        return c

    lax.fori_loop(0, n, start, 0)
    zero_start(z, de_ref, *FILL[1], zsem)
    for a in range(8):
        own_ref[0, n + a] = k * t
        own_ref[1, n + a] = 0
    xf[...] = jnp.zeros_like(xf)

    def wait(i, c):
        pltpu.make_async_copy(emb_ref.at[pl.ds(0, 8), :], buf.at[0], sem).wait()
        return c

    lax.fori_loop(0, n, wait, 0)

    def take(g, c):
        for a in range(8):
            tmp[a] = buf[g * 8 + a].astype(F32)
        for a in range(8):
            i = g * 8 + a
            xf[pl.ds(own_ref[0, i], 1), :] = tmp[a, pl.ds(own_ref[1, i] & 7, 1), :]
        return c

    lax.fori_loop(0, (n + 7) // 8, take, 0)
    for a, ref in enumerate((k0, s0, k1, s1)):
        for c in range(2):
            ref[c * tl:(c + 1) * tl, :] = xf[c * 2 * h + a * tl:c * 2 * h + (a + 1) * tl, :].astype(BF16)
    zero_wait(z, de_ref, FILL[0][0], FILL[1][1], zsem)


def sum_kernel(k0, y0, k1, y1, a0, t0, a1, t1):
    tl = a0.shape[0]
    for x, y, a, t in ((k0, y0, a0, t0), (k1, y1, a1, t1)):
        a[...] = x[0:tl, :] + y[0:tl, :]
        t[...] = x[tl:2 * tl, :] + y[tl:2 * tl, :]


def chip_mask(ids_ref, m, q, tl, chip_rows):
    t = ids_ref.shape[1]
    row = lax.broadcasted_iota(jnp.int32, (tl, t), 0) + q * tl
    lane = lax.broadcasted_iota(jnp.int32, (tl, t), 1)
    ids = jnp.broadcast_to(ids_ref[m:m + 1, :].astype(F32), (tl, t))
    col = jnp.sum(jnp.where(row == lane, ids, 0.0), axis=1, keepdims=True)
    lo = ((lax.axis_index("tp") >> 1) * chip_rows).astype(F32)
    return jnp.logical_and(col >= lo, col < lo + chip_rows)


def dx_kernel(m, chip_rows, xh_ref, z_ref, p0, p1, p2, p3, dres_ref, g_ref, ids_ref, tok_ref, *refs):
    if m == 1:
        both0_ref, dg0_ref, both_ref, slot_ref, dg_ref, xs_ref = refs
    else:
        both_ref, slot_ref, dg_ref = refs
    tl = slot_ref.shape[0]
    xh = xh_ref[...].astype(F32)
    x = xh + z_ref[...].astype(F32)
    both_ref[0:tl, :] = x.astype(BF16)
    if m == 1:
        xs_ref[0] = both0_ref[0:tl, :]
        xs_ref[1] = x.astype(BF16)
    g = g_ref[...].astype(F32)
    rs = lax.rsqrt(jnp.mean(x * x, axis=-1, keepdims=True) + EPS)
    nh = x * rs
    s = slice(m * tl, (m + 1) * tl)
    dn = (p0[s, :].astype(F32) + p1[s, :].astype(F32)) + (p2[s, :].astype(F32) + p3[s, :].astype(F32))
    gdn = g * dn
    mean = jnp.mean(nh * gdn, axis=-1, keepdims=True)
    dxn = rs * (gdn - nh * mean)
    dx = (dres_ref[m].astype(F32) + dxn).astype(BF16)
    both_ref[tl:2 * tl, :] = dx
    own = chip_mask(ids_ref, m, lax.axis_index("tp"), tl, chip_rows)
    slot_ref[...] = jnp.where(own, xh, dx.astype(F32)).astype(BF16)
    dg = jnp.sum(dn * nh, axis=0, keepdims=True)
    dg_ref[...] = dg if m == 0 else dg + dg0_ref[...]


def norm(x, g_ref):
    rs = lax.rsqrt(jnp.mean(x * x, axis=-1, keepdims=True) + EPS)
    return ((x * rs) * g_ref[...].astype(F32)).astype(BF16)


def umat(n_ref, w_ref, ub, u_ref, q0, q1, sem):
    blk = 256
    for i in range(ub.shape[1] // blk):
        ub[:, i * blk:(i + 1) * blk] = jnp.dot(
            n_ref[...], w_ref[:, i * blk:(i + 1) * blk], preferred_element_type=F32).astype(BF16)
    k = u_ref.shape[0]
    tl = u_ref.shape[1] // 4
    copies = []
    for m in range(k):
        for a, q in enumerate((q0, q1)):
            c = pltpu.make_async_copy(ub.at[pl.ds((m * 2 + a) * tl, tl), :],
                                      u_ref.at[m, pl.ds(pl.multiple_of(q * tl, tl), tl), :], sem)
            c.start()
            copies.append(c)
    return copies


def take_du(du_ref, out_ref, tl, order):
    for a, (m, q) in enumerate(order):
        out_ref[a * tl:(a + 1) * tl, :] = du_ref[m, pl.ds(pl.multiple_of(q * tl, tl), tl), :]


def dw_tile(n_ref, du2, i, blk):
    return lax.dot_general(n_ref[:, i * blk:(i + 1) * blk], du2[...], (((0,), (0,)), ((), ())), preferred_element_type=F32)


def u_kernel(x0, y0, x1, y1, g_ref, w_ref, du_ref, tok_ref, u_ref, dwp_ref, n_ref, du2, ub, usem):
    r = lax.axis_index("tp")
    tl = x0.shape[0] // 2
    for a, x in enumerate((x0, y0, x1, y1)):
        n_ref[a * tl:(a + 1) * tl, :] = norm(x[0:tl, :].astype(F32), g_ref)
    take_du(du_ref, du2, tl, ((0, r), (0, r ^ 1), (1, r), (1, r ^ 1)))
    copies = umat(n_ref, w_ref, ub, u_ref, r, r ^ 1, usem)
    blk = 256
    for i in range(dwp_ref.shape[0] // blk):
        dwp_ref[i * blk:(i + 1) * blk, :] = dw_tile(n_ref, du2, i, blk)
    for c in copies:
        c.wait()


SEG = (0, 256, 512)


def scatter(p, list_ref, xf, de_ref, sem):
    e = list_ref.shape[1]

    def add(i, c):
        a = list_ref[2, i]
        b = list_ref[3, i]

        @pl.when(jnp.logical_and(b >= SEG[p], b < SEG[p + 1]))
        def _():
            xf[pl.ds(b, 1), :] = xf[pl.ds(b, 1), :] + xf[pl.ds(a, 1), :]

        return c

    @pl.when(repeats(p, list_ref))
    def _():
        lax.fori_loop(0, list_ref[2, e - 2], add, 0)

    def put(i, c):
        pltpu.make_async_copy(xf.at[pl.ds(list_ref[0, i], 1), :], de_ref.at[pl.ds(list_ref[1, i], 1), :], sem).start()
        return c

    lax.fori_loop(list_ref[p, e - 1], list_ref[p + 1, e - 1], put, 0)


def repeats(p, list_ref):
    e = list_ref.shape[1]
    return list_ref[p + 1, e - 2] > list_ref[p, e - 2]


def scatter_wait(p, list_ref, xf, de_ref, sem):
    e = list_ref.shape[1]

    def wait(i, c):
        pltpu.make_async_copy(xf.at[pl.ds(0, 1), :], de_ref.at[pl.ds(0, 1), :], sem).wait()
        return c

    lax.fori_loop(list_ref[p, e - 1], list_ref[p + 1, e - 1], wait, 0)


def near_kernel(list_ref, d0, a0, d1, a1, tok_ref, de_in, xn_ref, de_ref, sem):
    tl = d0.shape[0] // 2
    for a, ref in enumerate((d0, a0, d1, a1)):
        xn_ref[a * tl:(a + 1) * tl, :] = ref[tl:2 * tl, :].astype(F32)
    scatter(0, list_ref, xn_ref, de_ref, sem)
    scatter_wait(0, list_ref, xn_ref, de_ref, sem)


def far_n(ids_ref, m, q, own, got, g_ref, chip_rows):
    own_x = chip_mask(ids_ref, m, q, got.shape[0], chip_rows)
    return norm(jnp.where(own_x, own[...].astype(F32), got[...].astype(F32)), g_ref)


def last_kernel(chip_rows, list_ref, xn_ref, c0, b0, c1, b1, t0, w0, t1, w1, dwp_ref, ids_ref, g_ref,
                w_ref, du_ref, u_in, de_in, u_ref, dw_ref, de_ref, xf, n_ref, du2, ub, dwb, usem, wsem, sem):
    d = w_ref.shape[0]
    tl = c0.shape[0]
    r = lax.axis_index("tp")
    h = xn_ref.shape[0]
    take_du(du_ref, du2, tl, ((0, r ^ 2), (0, r ^ 3), (1, r ^ 2), (1, r ^ 3)))
    for a, (m, q, own, got) in enumerate(((0, r ^ 2, t0, c0), (0, r ^ 3, w0, b0), (1, r ^ 2, t1, c1), (1, r ^ 3, w1, b1))):
        n_ref[a * tl:(a + 1) * tl, :] = far_n(ids_ref, m, q, own, got, g_ref, chip_rows)
    blk = 256
    for i in range(d // blk):
        rows = slice(i * blk, (i + 1) * blk)
        dwb[rows, :] = dwp_ref[rows, :] + dw_tile(n_ref, du2, i, blk)
        pltpu.make_async_copy(dwb.at[pl.ds(i * blk, blk), :], dw_ref.at[pl.ds(i * blk, blk), :], wsem).start()

    @pl.when(repeats(1, list_ref))
    def _():
        xf[0:h, :] = xn_ref[...]

    for a, ref in enumerate((c0, b0, c1, b1)):
        xf[h + a * tl:h + (a + 1) * tl, :] = ref[...].astype(F32)
    scatter(1, list_ref, xf, de_ref, sem)
    copies = umat(n_ref, w_ref, ub, u_ref, r ^ 2, r ^ 3, usem)
    scatter_wait(1, list_ref, xf, de_ref, sem)
    pltpu.make_async_copy(dwb, dw_ref, wsem).wait()
    for c in copies:
        c.wait()


def solution(mesh):
    groups = mesh.shape["tp"]
    sib = [(i, i ^ 1) for i in range(groups)]
    cross = [(i, i ^ 2) for i in range(groups)]
    diag = [(i, i ^ 3) for i in range(groups)]

    def local(ids, emb, g, w, du, dres):
        k, t = ids.shape
        vl, d = emb.shape
        fc = w.shape[1]
        tl = t // groups
        n = k * tl
        h = 2 * n
        g2 = g.reshape(1, d)
        S = jax.ShapeDtypeStruct
        D = pltpu.SemaphoreType.DMA

        def perm(v, p):
            return lax.ppermute(v, "tp", p)

        p2, p3, p1, p0 = call(
            pdn_kernel, 60, [S((n, d), BF16)] * 4, [HBM] * 2, [HBM] * 4,
            [pltpu.VMEM((k, t, fc), BF16), pltpu.VMEM((4 * n, fc), BF16), pltpu.VMEM((d, fc), BF16), pltpu.VMEM((4 * n, d), BF16),
             D, D((d // 768,)), D], 8 * n * fc * d, 2 * d * fc + 8 * n * (fc + d))(du, w)
        q2 = perm(p2, cross)
        q3 = perm(p3, diag)
        k0, s0, k1, s1, owned, de = call(
            gather_kernel, 36,
            [S((n, d), BF16)] * 4 + [S((2, 2 * h + 16), jnp.int32), S((vl, d), F32)],
            [SMEM, HBM], [VMEM] * 4 + [SMEM, HBM],
            [pltpu.VMEM((2 * h, 8, d), BF16), pltpu.VMEM((8, 8, d), F32), pltpu.VMEM((2 * h + 8, d), F32), pltpu.VMEM((256, d), F32)]
            + [pltpu.SMEM((2 * h + 8,), jnp.int32), D, D],
            500_000_000, 16 * h * d)(ids, emb)
        y0 = perm(s0, sib)
        y1 = perm(s1, sib)
        q1 = perm(p1, sib)
        own0, oth0, own1, oth1 = call(sum_kernel, 16, [S((tl, d), BF16)] * 4, [VMEM] * 4, [VMEM] * 4, [],
                                      8 * tl * d, 24 * tl * d)(k0, y0, k1, y1)
        z0 = perm(oth0, cross)
        z1 = perm(oth1, cross)
        w0 = perm(oth0, sib)
        w1 = perm(oth1, sib)
        lists, de = call(
            zero_kernel, 8, [S((4, 2 * h + 16), jnp.int32), S((vl, d), F32)], [SMEM, HBM], [SMEM, HBM],
            [pltpu.VMEM((256, d), F32), pltpu.SMEM((2 * h + 8,), jnp.int32), pltpu.SMEM((vl,), jnp.int32), D],
            6_000_000_000, 2 * vl * d, {1: 1})(owned, de)

        def dxk(m, xh, z, tok, more):
            outs = [S((n, d), BF16), S((tl, d), BF16), S((1, d), F32)] + ([S((k, tl, d), BF16)] if m else [])
            return call(functools.partial(dx_kernel, m, 2 * vl), 16, outs,
                        [VMEM] * 9 + [HBM] + [VMEM] * len(more),
                        [VMEM] * len(outs), [], 30 * n * d, 16 * n * d)(
                            xh, z, p0, q1, q2, q3, dres, g2, ids, tok, *more)

        mine0, slot0, dg0 = dxk(0, own0, z0, de, ())
        c0 = perm(slot0, cross)
        next0 = perm(mine0, sib)
        mine1, slot1, dg, x = dxk(1, own1, z1, de, (mine0, dg0))
        c1 = perm(slot1, cross)
        next1 = perm(mine1, sib)
        u, dwp = call(
            u_kernel, 32, [S((k, t, fc), BF16), S((d, fc), F32)], [VMEM] * 8, [HBM, VMEM],
            [pltpu.VMEM((t, d), BF16), pltpu.VMEM((t, fc), BF16), pltpu.VMEM((t, fc), BF16), D],
            4 * t * d * fc, 2 * d * fc)(mine0, next0, mine1, next1, g2, w, du, dg)
        xn, de = call(near_kernel, 8, [S((t, d), F32), S((vl, d), F32)], [SMEM] + [VMEM] * 5 + [HBM], [VMEM, HBM],
                      [D], 8 * h * d, 8 * h * d, {6: 1})(lists, mine0, next0, mine1, next1, dg, de)
        b0 = perm(c0, sib)
        b1 = perm(c1, sib)
        dgs = dg + perm(dg, cross)
        dgs = dgs + perm(dgs, sib)

        u, dw, de = call(
            functools.partial(last_kernel, 2 * vl), 20, [S((k, t, fc), BF16), S((d, fc), F32), S((vl, d), F32)],
            [SMEM] + [VMEM] * 14 + [HBM] * 2, [HBM] * 3,
            [pltpu.VMEM((2 * h, d), F32), pltpu.VMEM((t, d), BF16), pltpu.VMEM((t, fc), BF16), pltpu.VMEM((t, fc), BF16),
             pltpu.VMEM((d, fc), F32), D, D, D],
            4 * t * d * fc, 6 * d * fc, {15: 0, 16: 2})(
                lists, xn, c0, b0, c1, b1, oth0, w0, oth1, w1, dwp, ids, g2, w, du, u, de)
        return u, x, de, dw, dgs.reshape(d)

    return jax.shard_map(
        local,
        mesh=mesh,
        in_specs=(P("dp", None), P("tp", None), P(None), P(None, "tp"), P("dp", None, "tp"), P("dp", "tp", None)),
        out_specs=(P("dp", None, "tp"), P("dp", "tp", None), P(("dp", "tp"), None), P(None, ("dp", "tp")), P("dp")),
        check_vma=False,
    )
```

```python
import functools

import jax
import jax.numpy as jnp
from jax import lax
from jax.experimental import pallas as pl
from jax.experimental.pallas import tpu as pltpu
from jax.sharding import PartitionSpec as P


EPS = 1e-6
F32 = jnp.float32
BF16 = jnp.bfloat16
HBM = pl.BlockSpec(memory_space=pltpu.HBM)
VMEM = pl.BlockSpec(memory_space=pltpu.VMEM)
SMEM = pl.BlockSpec(memory_space=pltpu.SMEM)


def call(body, mib, outs, ins, out_specs, scratch, flops, nbytes, aliases=None):
    return pl.pallas_call(
        body,
        out_shape=outs,
        in_specs=ins,
        out_specs=out_specs,
        scratch_shapes=scratch,
        input_output_aliases=aliases or {},
        cost_estimate=pl.CostEstimate(flops=flops, bytes_accessed=nbytes, transcendentals=0),
        compiler_params=pltpu.CompilerParams(vmem_limit_bytes=mib << 20),
    )


def pdn_kernel(du_ref, w_ref, *refs):
    outs = refs[:4]
    dub, dup, wb, ob, dsem, wsem, osem = refs[4:]
    n, d = outs[0].shape
    k, tl = dub.shape[0], dub.shape[1] // 4
    blk = 768
    nb = d // blk
    dc = pltpu.make_async_copy(du_ref, dub, dsem)
    dc.start()
    for i in range(nb):
        pltpu.make_async_copy(w_ref.at[pl.ds(i * blk, blk), :], wb.at[pl.ds(i * blk, blk), :], wsem.at[i]).start()
    r = lax.axis_index("tp")
    dc.wait()
    for a, j in enumerate((2, 3, 1, 0)):
        q = r ^ j
        for m in range(k):
            dup[pl.ds(a * n + m * tl, tl), :] = dub[m, pl.ds(pl.multiple_of(q * tl, tl), tl), :]

    def tile(i, c):
        cols = pl.ds(pl.multiple_of(i * blk, blk), blk)
        pltpu.make_async_copy(w_ref.at[cols, :], wb.at[cols, :], wsem.at[i]).wait()
        p = lax.dot_general(dup[...], wb[cols, :], (((1,), (1,)), ((), ())), preferred_element_type=F32)
        ob[:, cols] = p.astype(BF16)
        for a in range(4):
            pltpu.make_async_copy(ob.at[pl.ds(a * n, n), cols], outs[a].at[:, cols], osem).start()
        return c

    lax.fori_loop(0, nb, tile, 0)
    for a in range(4):
        pltpu.make_async_copy(ob.at[pl.ds(a * n, n), :], outs[a], osem).wait()


FILL = ((0, 3), (3, 6), (6, 16))


def zero_start(z, de_ref, lo, hi, sem):
    step = z.shape[0]
    per = de_ref.shape[0] // 16
    for i in range((hi - lo) * per // step):
        pltpu.make_async_copy(z, de_ref.at[pl.ds(lo * per + i * step, step), :], sem).start()


def zero_wait(z, de_ref, lo, hi, sem):
    step = z.shape[0]
    for _ in range((hi - lo) * (de_ref.shape[0] // 16) // step):
        pltpu.make_async_copy(z, de_ref.at[pl.ds(0, step), :], sem).wait()


def zero_kernel(own_ref, de_in, list_ref, de_ref, z, lnxt, tab, sem):
    z[...] = jnp.zeros_like(z)
    zero_start(z, de_ref, *FILL[2], sem)
    n = own_ref[0, own_ref.shape[1] - 1]
    t = lnxt.shape[0] - 8

    def link(i, c):
        v = own_ref[1, i]
        p = tab[v]
        ok = jnp.logical_and(p >= 0, p < i)
        p = jnp.where(ok, p, 0)
        ok = jnp.logical_and(ok, own_ref[1, p] == v)
        lnxt[i] = -1
        lnxt[jnp.where(ok, p, t)] = i
        tab[v] = i
        return c

    lax.fori_loop(0, n, link, 0)

    def lists(i, c):
        nl, nd, nl0, nd0 = c
        x = lnxt[i]
        end = (x < 0).astype(jnp.int32)
        pos = own_ref[0, i]
        list_ref[0, nl] = pos
        list_ref[1, nl] = own_ref[1, i]
        list_ref[2, nd] = pos
        list_ref[3, nd] = own_ref[0, jnp.maximum(x, 0)]
        to = list_ref[3, nd]
        dup = 1 - end
        return nl + end, nd + dup, nl0 + end * (pos < SEG[1]).astype(jnp.int32), nd0 + dup * (to < SEG[1]).astype(jnp.int32)

    nl, nd, nl0, nd0 = lax.fori_loop(0, n, lists, (0,) * 4)
    e = list_ref.shape[1]
    for a, (v, x) in enumerate(((0, 0), (nl0, nd0), (nl, nd))):
        list_ref[a, e - 1] = v
        list_ref[a, e - 2] = x
    zero_wait(z, de_ref, *FILL[2], sem)


def gather_kernel(ids_ref, emb_ref, k0, s0, k1, s1, own_ref, de_ref, buf, tmp, xf, z, lst, sem, zsem):
    k, t = ids_ref.shape
    vl = emb_ref.shape[0]
    h = k0.shape[0]
    tl = t // 4
    r = lax.axis_index("tp")
    z[...] = jnp.zeros_like(z)
    zero_start(z, de_ref, *FILL[0], zsem)
    n = 0
    for m, q in ((0, r), (0, r ^ 1), (1, r), (1, r ^ 1), (0, r ^ 2), (0, r ^ 3), (1, r ^ 2), (1, r ^ 3)):
        def scan(i, n):
            j = q * tl + i
            lst[n] = m * t + j
            return n + (lax.shift_right_logical(ids_ref[m, j], vl.bit_length() - 1) == r).astype(jnp.int32)

        n = lax.fori_loop(0, tl, scan, n, unroll=16)
    own_ref[0, own_ref.shape[1] - 1] = n

    def start(i, c):
        j = lst[i]
        m = j // t
        v = ids_ref[m, j & (t - 1)] - r * vl
        q = (j & (t - 1)) // tl
        pltpu.make_async_copy(emb_ref.at[pl.ds(pl.multiple_of((v >> 3) << 3, 8), 8), :], buf.at[i], sem).start()
        own_ref[0, i] = ((q ^ r) >> 1) * 2 * h + m * h + ((q ^ r) & 1) * tl + (j & (tl - 1))
        own_ref[1, i] = v
        return c

    lax.fori_loop(0, n, start, 0)
    zero_start(z, de_ref, *FILL[1], zsem)
    for a in range(8):
        own_ref[0, n + a] = k * t
        own_ref[1, n + a] = 0
    xf[...] = jnp.zeros_like(xf)

    def wait(i, c):
        pltpu.make_async_copy(emb_ref.at[pl.ds(0, 8), :], buf.at[0], sem).wait()
        return c

    lax.fori_loop(0, n, wait, 0)

    def take(g, c):
        for a in range(8):
            tmp[a] = buf[g * 8 + a].astype(F32)
        for a in range(8):
            i = g * 8 + a
            xf[pl.ds(own_ref[0, i], 1), :] = tmp[a, pl.ds(own_ref[1, i] & 7, 1), :]
        return c

    lax.fori_loop(0, (n + 7) // 8, take, 0)
    for a, ref in enumerate((k0, s0, k1, s1)):
        for c in range(2):
            ref[c * tl:(c + 1) * tl, :] = xf[c * 2 * h + a * tl:c * 2 * h + (a + 1) * tl, :].astype(BF16)
    zero_wait(z, de_ref, FILL[0][0], FILL[1][1], zsem)


def sum_kernel(k0, y0, k1, y1, a0, t0, a1, t1):
    tl = a0.shape[0]
    for x, y, a, t in ((k0, y0, a0, t0), (k1, y1, a1, t1)):
        a[...] = x[0:tl, :] + y[0:tl, :]
        t[...] = x[tl:2 * tl, :] + y[tl:2 * tl, :]


def chip_mask(ids_ref, m, q, tl, chip_rows):
    t = ids_ref.shape[1]
    row = lax.broadcasted_iota(jnp.int32, (tl, t), 0) + q * tl
    lane = lax.broadcasted_iota(jnp.int32, (tl, t), 1)
    ids = jnp.broadcast_to(ids_ref[m:m + 1, :].astype(F32), (tl, t))
    col = jnp.sum(jnp.where(row == lane, ids, 0.0), axis=1, keepdims=True)
    lo = ((lax.axis_index("tp") >> 1) * chip_rows).astype(F32)
    return jnp.logical_and(col >= lo, col < lo + chip_rows)


def dx_kernel(m, chip_rows, xh_ref, z_ref, p0, p1, p2, p3, dres_ref, g_ref, ids_ref, tok_ref, *refs):
    if m == 1:
        both0_ref, dg0_ref, both_ref, slot_ref, dg_ref, xs_ref = refs
    else:
        both_ref, slot_ref, dg_ref = refs
    tl = slot_ref.shape[0]
    xh = xh_ref[...].astype(F32)
    x = xh + z_ref[...].astype(F32)
    both_ref[0:tl, :] = x.astype(BF16)
    if m == 1:
        xs_ref[0] = both0_ref[0:tl, :]
        xs_ref[1] = x.astype(BF16)
    g = g_ref[...].astype(F32)
    rs = lax.rsqrt(jnp.mean(x * x, axis=-1, keepdims=True) + EPS)
    nh = x * rs
    s = slice(m * tl, (m + 1) * tl)
    dn = (p0[s, :].astype(F32) + p1[s, :].astype(F32)) + (p2[s, :].astype(F32) + p3[s, :].astype(F32))
    gdn = g * dn
    mean = jnp.mean(nh * gdn, axis=-1, keepdims=True)
    dxn = rs * (gdn - nh * mean)
    dx = (dres_ref[m].astype(F32) + dxn).astype(BF16)
    both_ref[tl:2 * tl, :] = dx
    own = chip_mask(ids_ref, m, lax.axis_index("tp"), tl, chip_rows)
    slot_ref[...] = jnp.where(own, xh, dx.astype(F32)).astype(BF16)
    dg = jnp.sum(dn * nh, axis=0, keepdims=True)
    dg_ref[...] = dg if m == 0 else dg + dg0_ref[...]


def norm(x, g_ref):
    rs = lax.rsqrt(jnp.mean(x * x, axis=-1, keepdims=True) + EPS)
    return ((x * rs) * g_ref[...].astype(F32)).astype(BF16)


def umat(n_ref, row, w_ref, ub, u_ref, order, sem):
    blk = 256
    tl = u_ref.shape[1] // 4
    rows = len(order) * tl
    for i in range(ub.shape[1] // blk):
        ub[:, i * blk:(i + 1) * blk] = jnp.dot(
            n_ref[row:row + rows, :], w_ref[:, i * blk:(i + 1) * blk], preferred_element_type=F32).astype(BF16)
    copies = []
    for a, (m, q) in enumerate(order):
        c = pltpu.make_async_copy(ub.at[pl.ds(a * tl, tl), :], u_ref.at[m, pl.ds(pl.multiple_of(q * tl, tl), tl), :], sem)
        c.start()
        copies.append(c)
    return copies


def take_du(du_ref, out_ref, tl, order):
    for a, (m, q) in enumerate(order):
        out_ref[a * tl:(a + 1) * tl, :] = du_ref[m, pl.ds(pl.multiple_of(q * tl, tl), tl), :]


def dw_tile(n_ref, du2, i, blk):
    return lax.dot_general(n_ref[:, i * blk:(i + 1) * blk], du2[...], (((0,), (0,)), ((), ())), preferred_element_type=F32)


def u_kernel(x0, y0, x1, y1, g_ref, w_ref, du_ref, tok_ref, u_ref, dwp_ref, n_ref, du2, ub, usem):
    r = lax.axis_index("tp")
    tl = x0.shape[0] // 2
    for a, x in enumerate((x0, y0, x1, y1)):
        n_ref[a * tl:(a + 1) * tl, :] = norm(x[0:tl, :].astype(F32), g_ref)
    order = ((0, r), (0, r ^ 1), (1, r), (1, r ^ 1))
    take_du(du_ref, du2, tl, order)
    copies = umat(n_ref, 0, w_ref, ub, u_ref, order, usem)
    blk = 256
    for i in range(dwp_ref.shape[0] // blk):
        dwp_ref[i * blk:(i + 1) * blk, :] = dw_tile(n_ref, du2, i, blk)
    for c in copies:
        c.wait()


SEG = (0, 256, 512)


def scatter(p, list_ref, xf, de_ref, sem):
    e = list_ref.shape[1]

    def add(i, c):
        a = list_ref[2, i]
        b = list_ref[3, i]

        @pl.when(jnp.logical_and(b >= SEG[p], b < SEG[p + 1]))
        def _():
            xf[pl.ds(b, 1), :] = xf[pl.ds(b, 1), :] + xf[pl.ds(a, 1), :]

        return c

    @pl.when(repeats(p, list_ref))
    def _():
        lax.fori_loop(0, list_ref[2, e - 2], add, 0)

    def put(i, c):
        pltpu.make_async_copy(xf.at[pl.ds(list_ref[0, i], 1), :], de_ref.at[pl.ds(list_ref[1, i], 1), :], sem).start()
        return c

    lax.fori_loop(list_ref[p, e - 1], list_ref[p + 1, e - 1], put, 0)


def repeats(p, list_ref):
    e = list_ref.shape[1]
    return list_ref[p + 1, e - 2] > list_ref[p, e - 2]


def scatter_wait(p, list_ref, xf, de_ref, sem):
    e = list_ref.shape[1]

    def wait(i, c):
        pltpu.make_async_copy(xf.at[pl.ds(0, 1), :], de_ref.at[pl.ds(0, 1), :], sem).wait()
        return c

    lax.fori_loop(list_ref[p, e - 1], list_ref[p + 1, e - 1], wait, 0)


def near_kernel(list_ref, d0, a0, d1, a1, tok_ref, de_in, xn_ref, de_ref, sem):
    tl = d0.shape[0] // 2
    for a, ref in enumerate((d0, a0, d1, a1)):
        xn_ref[a * tl:(a + 1) * tl, :] = ref[tl:2 * tl, :].astype(F32)
    scatter(0, list_ref, xn_ref, de_ref, sem)
    scatter_wait(0, list_ref, xn_ref, de_ref, sem)


def far_n(ids_ref, m, q, own, got, g_ref, chip_rows):
    own_x = chip_mask(ids_ref, m, q, got.shape[0], chip_rows)
    return norm(jnp.where(own_x, own[...].astype(F32), got[...].astype(F32)), g_ref)


def mid_kernel(chip_rows, c0, b0, c1, t0, w0, t1, ids_ref, g_ref, w_ref, u_in, n_ref, u_ref, ub, usem):
    tl = c0.shape[0]
    r = lax.axis_index("tp")
    for a, (m, q, own, got) in enumerate(((0, r ^ 2, t0, c0), (0, r ^ 3, w0, b0), (1, r ^ 2, t1, c1))):
        n_ref[a * tl:(a + 1) * tl, :] = far_n(ids_ref, m, q, own, got, g_ref, chip_rows)
    for c in umat(n_ref, 0, w_ref, ub, u_ref, ((0, r ^ 2), (0, r ^ 3)), usem):
        c.wait()


def last_kernel(chip_rows, list_ref, xn_ref, nm_ref, c0, b0, c1, b1, w1, dwp_ref, ids_ref, g_ref,
                w_ref, du_ref, u_in, de_in, u_ref, dw_ref, de_ref, xf, n_ref, du2, ub, dwb, usem, wsem, sem):
    d = w_ref.shape[0]
    tl = c0.shape[0]
    r = lax.axis_index("tp")
    h = xn_ref.shape[0]
    order = ((0, r ^ 2), (0, r ^ 3), (1, r ^ 2), (1, r ^ 3))
    take_du(du_ref, du2, tl, order)
    n_ref[0:3 * tl, :] = nm_ref[...]
    n_ref[3 * tl:4 * tl, :] = far_n(ids_ref, 1, r ^ 3, w1, b1, g_ref, chip_rows)
    blk = 256
    for i in range(d // blk):
        rows = slice(i * blk, (i + 1) * blk)
        dwb[rows, :] = dwp_ref[rows, :] + dw_tile(n_ref, du2, i, blk)
        pltpu.make_async_copy(dwb.at[pl.ds(i * blk, blk), :], dw_ref.at[pl.ds(i * blk, blk), :], wsem).start()

    @pl.when(repeats(1, list_ref))
    def _():
        xf[0:h, :] = xn_ref[...]

    for a, ref in enumerate((c0, b0, c1, b1)):
        xf[h + a * tl:h + (a + 1) * tl, :] = ref[...].astype(F32)
    scatter(1, list_ref, xf, de_ref, sem)
    copies = umat(n_ref, 2 * tl, w_ref, ub, u_ref, order[2:], usem)
    scatter_wait(1, list_ref, xf, de_ref, sem)
    pltpu.make_async_copy(dwb, dw_ref, wsem).wait()
    for c in copies:
        c.wait()


def solution(mesh):
    groups = mesh.shape["tp"]
    sib = [(i, i ^ 1) for i in range(groups)]
    cross = [(i, i ^ 2) for i in range(groups)]
    diag = [(i, i ^ 3) for i in range(groups)]

    def local(ids, emb, g, w, du, dres):
        k, t = ids.shape
        vl, d = emb.shape
        fc = w.shape[1]
        tl = t // groups
        n = k * tl
        h = 2 * n
        g2 = g.reshape(1, d)
        S = jax.ShapeDtypeStruct
        D = pltpu.SemaphoreType.DMA

        def perm(v, p):
            return lax.ppermute(v, "tp", p)

        p2, p3, p1, p0 = call(
            pdn_kernel, 60, [S((n, d), BF16)] * 4, [HBM] * 2, [HBM] * 4,
            [pltpu.VMEM((k, t, fc), BF16), pltpu.VMEM((4 * n, fc), BF16), pltpu.VMEM((d, fc), BF16), pltpu.VMEM((4 * n, d), BF16),
             D, D((d // 768,)), D], 8 * n * fc * d, 2 * d * fc + 8 * n * (fc + d))(du, w)
        q2 = perm(p2, cross)
        q3 = perm(p3, diag)
        k0, s0, k1, s1, owned, de = call(
            gather_kernel, 36,
            [S((n, d), BF16)] * 4 + [S((2, 2 * h + 16), jnp.int32), S((vl, d), F32)],
            [SMEM, HBM], [VMEM] * 4 + [SMEM, HBM],
            [pltpu.VMEM((2 * h, 8, d), BF16), pltpu.VMEM((8, 8, d), F32), pltpu.VMEM((2 * h + 8, d), F32), pltpu.VMEM((256, d), F32)]
            + [pltpu.SMEM((2 * h + 8,), jnp.int32), D, D],
            500_000_000, 16 * h * d)(ids, emb)
        y0 = perm(s0, sib)
        y1 = perm(s1, sib)
        q1 = perm(p1, sib)
        own0, oth0, own1, oth1 = call(sum_kernel, 16, [S((tl, d), BF16)] * 4, [VMEM] * 4, [VMEM] * 4, [],
                                      8 * tl * d, 24 * tl * d)(k0, y0, k1, y1)
        z0 = perm(oth0, cross)
        z1 = perm(oth1, cross)
        w0 = perm(oth0, sib)
        w1 = perm(oth1, sib)
        lists, de = call(
            zero_kernel, 8, [S((4, 2 * h + 16), jnp.int32), S((vl, d), F32)], [SMEM, HBM], [SMEM, HBM],
            [pltpu.VMEM((256, d), F32), pltpu.SMEM((2 * h + 8,), jnp.int32), pltpu.SMEM((vl,), jnp.int32), D],
            6_000_000_000, 2 * vl * d, {1: 1})(owned, de)

        def dxk(m, xh, z, tok, more):
            outs = [S((n, d), BF16), S((tl, d), BF16), S((1, d), F32)] + ([S((k, tl, d), BF16)] if m else [])
            return call(functools.partial(dx_kernel, m, 2 * vl), 16, outs,
                        [VMEM] * 9 + [HBM] + [VMEM] * len(more),
                        [VMEM] * len(outs), [], 30 * n * d, 16 * n * d)(
                            xh, z, p0, q1, q2, q3, dres, g2, ids, tok, *more)

        mine0, slot0, dg0 = dxk(0, own0, z0, de, ())
        c0 = perm(slot0, cross)
        next0 = perm(mine0, sib)
        mine1, slot1, dg, x = dxk(1, own1, z1, de, (mine0, dg0))
        c1 = perm(slot1, cross)
        next1 = perm(mine1, sib)
        u, dwp = call(
            u_kernel, 32, [S((k, t, fc), BF16), S((d, fc), F32)], [VMEM] * 8, [HBM, VMEM],
            [pltpu.VMEM((t, d), BF16), pltpu.VMEM((t, fc), BF16), pltpu.VMEM((t, fc), BF16), D],
            4 * t * d * fc, 2 * d * fc)(mine0, next0, mine1, next1, g2, w, du, dg)
        dgs = dg + perm(dg, cross)
        dgs = dgs + perm(dgs, sib)
        dgs = dgs.reshape(d)
        xn, de = call(near_kernel, 8, [S((t, d), F32), S((vl, d), F32)], [SMEM] + [VMEM] * 5 + [HBM], [VMEM, HBM],
                      [D], 8 * h * d, 8 * h * d, {6: 1})(lists, mine0, next0, mine1, next1, dgs, de)
        b0 = perm(c0, sib)
        b1 = perm(c1, sib)

        nm, u = call(
            functools.partial(mid_kernel, 2 * vl), 12, [S((3 * tl, d), BF16), S((k, t, fc), BF16)],
            [VMEM] * 9 + [HBM], [VMEM, HBM], [pltpu.VMEM((2 * tl, fc), BF16), D],
            4 * tl * d * fc, 2 * d * fc, {9: 1})(c0, b0, c1, oth0, w0, oth1, ids, g2, w, u)
        u, dw, de = call(
            functools.partial(last_kernel, 2 * vl), 20, [S((k, t, fc), BF16), S((d, fc), F32), S((vl, d), F32)],
            [SMEM] + [VMEM] * 12 + [HBM] * 2, [HBM] * 3,
            [pltpu.VMEM((2 * h, d), F32), pltpu.VMEM((t, d), BF16), pltpu.VMEM((t, fc), BF16), pltpu.VMEM((2 * tl, fc), BF16),
             pltpu.VMEM((d, fc), F32), D, D, D],
            4 * t * d * fc, 6 * d * fc, {13: 0, 14: 2})(
                lists, xn, nm, c0, b0, c1, b1, w1, dwp, ids, g2, w, du, u, de)
        return u, x, de, dw, dgs

    return jax.shard_map(
        local,
        mesh=mesh,
        in_specs=(P("dp", None), P("tp", None), P(None), P(None, "tp"), P("dp", None, "tp"), P("dp", "tp", None)),
        out_specs=(P("dp", None, "tp"), P("dp", "tp", None), P(("dp", "tp"), None), P(None, ("dp", "tp")), P("dp")),
        check_vma=False,
    )
```

```python
import functools

import jax
import jax.numpy as jnp
from jax import lax
from jax.experimental import pallas as pl
from jax.experimental.pallas import tpu as pltpu
from jax.sharding import PartitionSpec as P


EPS = 1e-6
F32 = jnp.float32
BF16 = jnp.bfloat16
HBM = pl.BlockSpec(memory_space=pltpu.HBM)
VMEM = pl.BlockSpec(memory_space=pltpu.VMEM)
SMEM = pl.BlockSpec(memory_space=pltpu.SMEM)


def call(body, mib, outs, ins, out_specs, scratch, flops, nbytes, aliases=None):
    return pl.pallas_call(
        body,
        out_shape=outs,
        in_specs=ins,
        out_specs=out_specs,
        scratch_shapes=scratch,
        input_output_aliases=aliases or {},
        cost_estimate=pl.CostEstimate(flops=flops, bytes_accessed=nbytes, transcendentals=0),
        compiler_params=pltpu.CompilerParams(vmem_limit_bytes=mib << 20),
    )


def pdn_kernel(du_ref, w_ref, *refs):
    outs = refs[:4]
    dub, dup, wb, ob, dsem, wsem, osem = refs[4:]
    n, d = outs[0].shape
    k, tl = dub.shape[0], dub.shape[1] // 4
    blk = 768
    nb = d // blk
    dc = pltpu.make_async_copy(du_ref, dub, dsem)
    dc.start()
    for i in range(nb):
        pltpu.make_async_copy(w_ref.at[pl.ds(i * blk, blk), :], wb.at[pl.ds(i * blk, blk), :], wsem.at[i]).start()
    r = lax.axis_index("tp")
    dc.wait()
    for a, j in enumerate((2, 3, 1, 0)):
        q = r ^ j
        for m in range(k):
            dup[pl.ds(a * n + m * tl, tl), :] = dub[m, pl.ds(pl.multiple_of(q * tl, tl), tl), :]

    def tile(i, c):
        cols = pl.ds(pl.multiple_of(i * blk, blk), blk)
        pltpu.make_async_copy(w_ref.at[cols, :], wb.at[cols, :], wsem.at[i]).wait()
        p = lax.dot_general(dup[...], wb[cols, :], (((1,), (1,)), ((), ())), preferred_element_type=F32)
        ob[:, cols] = p.astype(BF16)
        for a in range(4):
            pltpu.make_async_copy(ob.at[pl.ds(a * n, n), cols], outs[a].at[:, cols], osem).start()
        return c

    lax.fori_loop(0, nb, tile, 0)
    for a in range(4):
        pltpu.make_async_copy(ob.at[pl.ds(a * n, n), :], outs[a], osem).wait()


FILL = ((0, 3), (3, 6), (6, 16))


def zero_start(z, de_ref, lo, hi, sem):
    step = z.shape[0]
    per = de_ref.shape[0] // 16
    for i in range((hi - lo) * per // step):
        pltpu.make_async_copy(z, de_ref.at[pl.ds(lo * per + i * step, step), :], sem).start()


def zero_wait(z, de_ref, lo, hi, sem):
    step = z.shape[0]
    for _ in range((hi - lo) * (de_ref.shape[0] // 16) // step):
        pltpu.make_async_copy(z, de_ref.at[pl.ds(0, step), :], sem).wait()


def zero_kernel(own_ref, de_in, list_ref, de_ref, z, lnxt, tab, sem):
    z[...] = jnp.zeros_like(z)
    zero_start(z, de_ref, *FILL[2], sem)
    n = own_ref[0, own_ref.shape[1] - 1]
    t = lnxt.shape[0] - 8

    def link(i, c):
        v = own_ref[1, i]
        p = tab[v]
        ok = jnp.logical_and(p >= 0, p < i)
        p = jnp.where(ok, p, 0)
        ok = jnp.logical_and(ok, own_ref[1, p] == v)
        lnxt[i] = -1
        lnxt[jnp.where(ok, p, t)] = i
        tab[v] = i
        return c

    lax.fori_loop(0, n, link, 0)

    def lists(i, c):
        nl, nd, nl0, nd0 = c
        x = lnxt[i]
        end = (x < 0).astype(jnp.int32)
        pos = own_ref[0, i]
        list_ref[0, nl] = pos
        list_ref[1, nl] = own_ref[1, i]
        list_ref[2, nd] = pos
        list_ref[3, nd] = own_ref[0, jnp.maximum(x, 0)]
        to = list_ref[3, nd]
        dup = 1 - end
        return nl + end, nd + dup, nl0 + end * (pos < SEG[1]).astype(jnp.int32), nd0 + dup * (to < SEG[1]).astype(jnp.int32)

    nl, nd, nl0, nd0 = lax.fori_loop(0, n, lists, (0,) * 4)
    e = list_ref.shape[1]
    for a, (v, x) in enumerate(((0, 0), (nl0, nd0), (nl, nd))):
        list_ref[a, e - 1] = v
        list_ref[a, e - 2] = x
    zero_wait(z, de_ref, *FILL[2], sem)


def gather_kernel(ids_ref, emb_ref, k0, s0, k1, s1, own_ref, de_ref, buf, tmp, xf, z, lst, sem, zsem):
    k, t = ids_ref.shape
    vl = emb_ref.shape[0]
    h = k0.shape[0]
    tl = t // 4
    r = lax.axis_index("tp")
    z[...] = jnp.zeros_like(z)
    zero_start(z, de_ref, *FILL[0], zsem)
    n = 0
    for m, q in ((0, r), (0, r ^ 1), (1, r), (1, r ^ 1), (0, r ^ 2), (0, r ^ 3), (1, r ^ 2), (1, r ^ 3)):
        def scan(i, n):
            j = q * tl + i
            lst[n] = m * t + j
            return n + (lax.shift_right_logical(ids_ref[m, j], vl.bit_length() - 1) == r).astype(jnp.int32)

        n = lax.fori_loop(0, tl, scan, n, unroll=16)
    own_ref[0, own_ref.shape[1] - 1] = n

    def start(i, c):
        j = lst[i]
        m = j // t
        v = ids_ref[m, j & (t - 1)] - r * vl
        q = (j & (t - 1)) // tl
        pltpu.make_async_copy(emb_ref.at[pl.ds(pl.multiple_of((v >> 3) << 3, 8), 8), :], buf.at[i], sem).start()
        own_ref[0, i] = ((q ^ r) >> 1) * 2 * h + m * h + ((q ^ r) & 1) * tl + (j & (tl - 1))
        own_ref[1, i] = v
        return c

    lax.fori_loop(0, n, start, 0)
    zero_start(z, de_ref, *FILL[1], zsem)
    for a in range(8):
        own_ref[0, n + a] = k * t
        own_ref[1, n + a] = 0
    xf[...] = jnp.zeros_like(xf)

    def wait(i, c):
        pltpu.make_async_copy(emb_ref.at[pl.ds(0, 8), :], buf.at[0], sem).wait()
        return c

    lax.fori_loop(0, n, wait, 0)

    def take(g, c):
        for a in range(8):
            tmp[a] = buf[g * 8 + a].astype(F32)
        for a in range(8):
            i = g * 8 + a
            xf[pl.ds(own_ref[0, i], 1), :] = tmp[a, pl.ds(own_ref[1, i] & 7, 1), :]
        return c

    lax.fori_loop(0, (n + 7) // 8, take, 0)
    for a, ref in enumerate((k0, s0, k1, s1)):
        for c in range(2):
            ref[c * tl:(c + 1) * tl, :] = xf[c * 2 * h + a * tl:c * 2 * h + (a + 1) * tl, :].astype(BF16)
    zero_wait(z, de_ref, FILL[0][0], FILL[1][1], zsem)


def sum_kernel(k0, y0, k1, y1, a0, t0, a1, t1):
    tl = a0.shape[0]
    for x, y, a, t in ((k0, y0, a0, t0), (k1, y1, a1, t1)):
        a[...] = x[0:tl, :] + y[0:tl, :]
        t[...] = x[tl:2 * tl, :] + y[tl:2 * tl, :]


def chip_mask(ids_ref, m, q, tl, chip_rows):
    t = ids_ref.shape[1]
    row = lax.broadcasted_iota(jnp.int32, (tl, t), 0) + q * tl
    lane = lax.broadcasted_iota(jnp.int32, (tl, t), 1)
    ids = jnp.broadcast_to(ids_ref[m:m + 1, :].astype(F32), (tl, t))
    col = jnp.sum(jnp.where(row == lane, ids, 0.0), axis=1, keepdims=True)
    lo = ((lax.axis_index("tp") >> 1) * chip_rows).astype(F32)
    return jnp.logical_and(col >= lo, col < lo + chip_rows)


def dx_kernel(m, chip_rows, xh_ref, z_ref, p0, p1, p2, p3, dres_ref, g_ref, ids_ref, tok_ref, *refs):
    if m == 1:
        both0_ref, dg0_ref, both_ref, slot_ref, dg_ref, xs_ref = refs
    else:
        both_ref, slot_ref, dg_ref = refs
    tl = slot_ref.shape[0]
    xh = xh_ref[...].astype(F32)
    x = xh + z_ref[...].astype(F32)
    both_ref[0:tl, :] = x.astype(BF16)
    if m == 1:
        xs_ref[0] = both0_ref[0:tl, :]
        xs_ref[1] = x.astype(BF16)
    g = g_ref[...].astype(F32)
    rs = lax.rsqrt(jnp.mean(x * x, axis=-1, keepdims=True) + EPS)
    nh = x * rs
    s = slice(m * tl, (m + 1) * tl)
    dn = (p0[s, :].astype(F32) + p1[s, :].astype(F32)) + (p2[s, :].astype(F32) + p3[s, :].astype(F32))
    gdn = g * dn
    mean = jnp.mean(nh * gdn, axis=-1, keepdims=True)
    dxn = rs * (gdn - nh * mean)
    dx = (dres_ref[m].astype(F32) + dxn).astype(BF16)
    both_ref[tl:2 * tl, :] = dx
    own = chip_mask(ids_ref, m, lax.axis_index("tp"), tl, chip_rows)
    slot_ref[...] = jnp.where(own, xh, dx.astype(F32)).astype(BF16)
    dg = jnp.sum(dn * nh, axis=0, keepdims=True)
    dg_ref[...] = dg if m == 0 else dg + dg0_ref[...]


def norm(x, g_ref):
    rs = lax.rsqrt(jnp.mean(x * x, axis=-1, keepdims=True) + EPS)
    return ((x * rs) * g_ref[...].astype(F32)).astype(BF16)


def umat(n_ref, row, w_ref, ub, u_ref, order, sem):
    blk = 256
    tl = u_ref.shape[1] // 4
    rows = len(order) * tl
    for i in range(ub.shape[1] // blk):
        ub[:, i * blk:(i + 1) * blk] = jnp.dot(
            n_ref[row:row + rows, :], w_ref[:, i * blk:(i + 1) * blk], preferred_element_type=F32).astype(BF16)
    copies = []
    for a, (m, q) in enumerate(order):
        c = pltpu.make_async_copy(ub.at[pl.ds(a * tl, tl), :], u_ref.at[m, pl.ds(pl.multiple_of(q * tl, tl), tl), :], sem)
        c.start()
        copies.append(c)
    return copies


def take_du(du_ref, out_ref, tl, order):
    for a, (m, q) in enumerate(order):
        out_ref[a * tl:(a + 1) * tl, :] = du_ref[m, pl.ds(pl.multiple_of(q * tl, tl), tl), :]


def dw_tile(n_ref, du2, i, blk):
    return lax.dot_general(n_ref[:, i * blk:(i + 1) * blk], du2[...], (((0,), (0,)), ((), ())), preferred_element_type=F32)


def u_kernel(x0, y0, x1, y1, g_ref, w_ref, du_ref, tok_ref, u_ref, dwp_ref, n_ref, du2, ub, usem):
    r = lax.axis_index("tp")
    tl = x0.shape[0] // 2
    for a, x in enumerate((x0, y0, x1, y1)):
        n_ref[a * tl:(a + 1) * tl, :] = norm(x[0:tl, :].astype(F32), g_ref)
    order = ((0, r), (0, r ^ 1), (1, r), (1, r ^ 1))
    take_du(du_ref, du2, tl, order)
    copies = umat(n_ref, 0, w_ref, ub, u_ref, order, usem)
    blk = 256
    for i in range(dwp_ref.shape[0] // blk):
        dwp_ref[i * blk:(i + 1) * blk, :] = dw_tile(n_ref, du2, i, blk)
    for c in copies:
        c.wait()


SEG = (0, 256, 512)


def scatter(p, list_ref, xf, de_ref, sem):
    e = list_ref.shape[1]

    def add(i, c):
        a = list_ref[2, i]
        b = list_ref[3, i]

        @pl.when(jnp.logical_and(b >= SEG[p], b < SEG[p + 1]))
        def _():
            xf[pl.ds(b, 1), :] = xf[pl.ds(b, 1), :] + xf[pl.ds(a, 1), :]

        return c

    @pl.when(repeats(p, list_ref))
    def _():
        lax.fori_loop(0, list_ref[2, e - 2], add, 0)

    def put(i, c):
        pltpu.make_async_copy(xf.at[pl.ds(list_ref[0, i], 1), :], de_ref.at[pl.ds(list_ref[1, i], 1), :], sem).start()
        return c

    lax.fori_loop(list_ref[p, e - 1], list_ref[p + 1, e - 1], put, 0)


def repeats(p, list_ref):
    e = list_ref.shape[1]
    return list_ref[p + 1, e - 2] > list_ref[p, e - 2]


def scatter_wait(p, list_ref, xf, de_ref, sem):
    e = list_ref.shape[1]

    def wait(i, c):
        pltpu.make_async_copy(xf.at[pl.ds(0, 1), :], de_ref.at[pl.ds(0, 1), :], sem).wait()
        return c

    lax.fori_loop(list_ref[p, e - 1], list_ref[p + 1, e - 1], wait, 0)


def near_kernel(list_ref, d0, a0, d1, a1, tok_ref, de_in, xn_ref, de_ref, sem):
    tl = d0.shape[0] // 2
    for a, ref in enumerate((d0, a0, d1, a1)):
        xn_ref[a * tl:(a + 1) * tl, :] = ref[tl:2 * tl, :].astype(F32)
    scatter(0, list_ref, xn_ref, de_ref, sem)
    scatter_wait(0, list_ref, xn_ref, de_ref, sem)


def far_n(ids_ref, m, q, own, got, g_ref, chip_rows):
    own_x = chip_mask(ids_ref, m, q, got.shape[0], chip_rows)
    return norm(jnp.where(own_x, own[...].astype(F32), got[...].astype(F32)), g_ref)


def mid_kernel(chip_rows, c0, b0, c1, t0, w0, t1, ids_ref, g_ref, w_ref, u_in, n_ref, u_ref, ub, usem):
    tl = c0.shape[0]
    r = lax.axis_index("tp")
    for a, (m, q, own, got) in enumerate(((0, r ^ 2, t0, c0), (0, r ^ 3, w0, b0), (1, r ^ 2, t1, c1))):
        n_ref[a * tl:(a + 1) * tl, :] = far_n(ids_ref, m, q, own, got, g_ref, chip_rows)
    for c in umat(n_ref, 0, w_ref, ub, u_ref, ((0, r ^ 2), (0, r ^ 3)), usem):
        c.wait()


def last_kernel(chip_rows, list_ref, xn_ref, nm_ref, c0, b0, c1, b1, w1, dwp_ref, ids_ref, g_ref,
                w_ref, du_ref, u_in, de_in, u_ref, dw_ref, de_ref, xf, n_ref, du2, ub, dwb, usem, wsem, sem):
    d = w_ref.shape[0]
    tl = c0.shape[0]
    r = lax.axis_index("tp")
    h = xn_ref.shape[0]
    order = ((0, r ^ 2), (0, r ^ 3), (1, r ^ 2), (1, r ^ 3))
    take_du(du_ref, du2, tl, order)
    n_ref[0:3 * tl, :] = nm_ref[...]
    n_ref[3 * tl:4 * tl, :] = far_n(ids_ref, 1, r ^ 3, w1, b1, g_ref, chip_rows)
    blk = 256
    for i in range(d // blk):
        rows = slice(i * blk, (i + 1) * blk)
        dwb[rows, :] = dwp_ref[rows, :] + dw_tile(n_ref, du2, i, blk)
        pltpu.make_async_copy(dwb.at[pl.ds(i * blk, blk), :], dw_ref.at[pl.ds(i * blk, blk), :], wsem).start()
    copies = umat(n_ref, 2 * tl, w_ref, ub, u_ref, order[2:], usem)

    @pl.when(repeats(1, list_ref))
    def _():
        xf[0:h, :] = xn_ref[...]

    for a, ref in enumerate((c0, b0, c1, b1)):
        xf[h + a * tl:h + (a + 1) * tl, :] = ref[...].astype(F32)
    scatter(1, list_ref, xf, de_ref, sem)
    scatter_wait(1, list_ref, xf, de_ref, sem)
    pltpu.make_async_copy(dwb, dw_ref, wsem).wait()
    for c in copies:
        c.wait()


def solution(mesh):
    groups = mesh.shape["tp"]
    sib = [(i, i ^ 1) for i in range(groups)]
    cross = [(i, i ^ 2) for i in range(groups)]
    diag = [(i, i ^ 3) for i in range(groups)]

    def local(ids, emb, g, w, du, dres):
        k, t = ids.shape
        vl, d = emb.shape
        fc = w.shape[1]
        tl = t // groups
        n = k * tl
        h = 2 * n
        g2 = g.reshape(1, d)
        S = jax.ShapeDtypeStruct
        D = pltpu.SemaphoreType.DMA

        def perm(v, p):
            return lax.ppermute(v, "tp", p)

        p2, p3, p1, p0 = call(
            pdn_kernel, 60, [S((n, d), BF16)] * 4, [HBM] * 2, [HBM] * 4,
            [pltpu.VMEM((k, t, fc), BF16), pltpu.VMEM((4 * n, fc), BF16), pltpu.VMEM((d, fc), BF16), pltpu.VMEM((4 * n, d), BF16),
             D, D((d // 768,)), D], 8 * n * fc * d, 2 * d * fc + 8 * n * (fc + d))(du, w)
        q2 = perm(p2, cross)
        q3 = perm(p3, diag)
        k0, s0, k1, s1, owned, de = call(
            gather_kernel, 36,
            [S((n, d), BF16)] * 4 + [S((2, 2 * h + 16), jnp.int32), S((vl, d), F32)],
            [SMEM, HBM], [VMEM] * 4 + [SMEM, HBM],
            [pltpu.VMEM((2 * h, 8, d), BF16), pltpu.VMEM((8, 8, d), F32), pltpu.VMEM((2 * h + 8, d), F32), pltpu.VMEM((256, d), F32)]
            + [pltpu.SMEM((2 * h + 8,), jnp.int32), D, D],
            500_000_000, 16 * h * d)(ids, emb)
        y0 = perm(s0, sib)
        y1 = perm(s1, sib)
        q1 = perm(p1, sib)
        own0, oth0, own1, oth1 = call(sum_kernel, 16, [S((tl, d), BF16)] * 4, [VMEM] * 4, [VMEM] * 4, [],
                                      8 * tl * d, 24 * tl * d)(k0, y0, k1, y1)
        z0 = perm(oth0, cross)
        z1 = perm(oth1, cross)
        w0 = perm(oth0, sib)
        w1 = perm(oth1, sib)
        lists, de = call(
            zero_kernel, 8, [S((4, 2 * h + 16), jnp.int32), S((vl, d), F32)], [SMEM, HBM], [SMEM, HBM],
            [pltpu.VMEM((256, d), F32), pltpu.SMEM((2 * h + 8,), jnp.int32), pltpu.SMEM((vl,), jnp.int32), D],
            6_000_000_000, 2 * vl * d, {1: 1})(owned, de)

        def dxk(m, xh, z, tok, more):
            outs = [S((n, d), BF16), S((tl, d), BF16), S((1, d), F32)] + ([S((k, tl, d), BF16)] if m else [])
            return call(functools.partial(dx_kernel, m, 2 * vl), 16, outs,
                        [VMEM] * 9 + [HBM] + [VMEM] * len(more),
                        [VMEM] * len(outs), [], 30 * n * d, 16 * n * d)(
                            xh, z, p0, q1, q2, q3, dres, g2, ids, tok, *more)

        mine0, slot0, dg0 = dxk(0, own0, z0, de, ())
        c0 = perm(slot0, cross)
        next0 = perm(mine0, sib)
        mine1, slot1, dg, x = dxk(1, own1, z1, de, (mine0, dg0))
        c1 = perm(slot1, cross)
        next1 = perm(mine1, sib)
        u, dwp = call(
            u_kernel, 32, [S((k, t, fc), BF16), S((d, fc), F32)], [VMEM] * 8, [HBM, VMEM],
            [pltpu.VMEM((t, d), BF16), pltpu.VMEM((t, fc), BF16), pltpu.VMEM((t, fc), BF16), D],
            4 * t * d * fc, 2 * d * fc)(mine0, next0, mine1, next1, g2, w, du, dg)
        xn, de = call(near_kernel, 8, [S((t, d), F32), S((vl, d), F32)], [SMEM] + [VMEM] * 5 + [HBM], [VMEM, HBM],
                      [D], 8 * h * d, 8 * h * d, {6: 1})(lists, mine0, next0, mine1, next1, dg, de)
        b0 = perm(c0, sib)
        b1 = perm(c1, sib)
        dgs = dg + perm(dg, cross)
        dgs = dgs + perm(dgs, sib)

        nm, u = call(
            functools.partial(mid_kernel, 2 * vl), 12, [S((3 * tl, d), BF16), S((k, t, fc), BF16)],
            [VMEM] * 9 + [HBM], [VMEM, HBM], [pltpu.VMEM((2 * tl, fc), BF16), D],
            4 * tl * d * fc, 2 * d * fc, {9: 1})(c0, b0, c1, oth0, w0, oth1, ids, g2, w, u)
        u, dw, de = call(
            functools.partial(last_kernel, 2 * vl), 20, [S((k, t, fc), BF16), S((d, fc), F32), S((vl, d), F32)],
            [SMEM] + [VMEM] * 12 + [HBM] * 2, [HBM] * 3,
            [pltpu.VMEM((2 * h, d), F32), pltpu.VMEM((t, d), BF16), pltpu.VMEM((t, fc), BF16), pltpu.VMEM((2 * tl, fc), BF16),
             pltpu.VMEM((d, fc), F32), D, D, D],
            4 * t * d * fc, 6 * d * fc, {13: 0, 14: 2})(
                lists, xn, nm, c0, b0, c1, b1, w1, dwp, ids, g2, w, du, u, de)
        return u, x, de, dw, dgs.reshape(d)

    return jax.shard_map(
        local,
        mesh=mesh,
        in_specs=(P("dp", None), P("tp", None), P(None), P(None, "tp"), P("dp", None, "tp"), P("dp", "tp", None)),
        out_specs=(P("dp", None, "tp"), P("dp", "tp", None), P(("dp", "tp"), None), P(None, ("dp", "tp")), P("dp")),
        check_vma=False,
    )
```
